256 devices in a mesh: pitch: 8 (over x, core), span: 32 (over z, y).
Axes of the slice: x: 4, y: 4, z: 8, core: 2. Of those that a mesh axis runs over, the one named last changes fastest.
Arguments:
- residual: float32 [5, 4, 256, 1024], P(None, None, 'span', 'pitch'), may hold values from -0.6 to 0.6
- inverse_diagonal: float32 [5, 5, 4, 256, 1024], P(None, None, None, 'span', 'pitch'), may hold values from -0.1 to 1, as said below
- prior_increment: float32 [5, 4, 256, 1024], P(None, None, 'span', 'pitch'), may hold values from -3 to 3
- coupling: float32 [6, 5, 5], replicated, may hold values from -1 to 1
- characteristic: float32 [2, 2, 512, 5, 5], replicated, may hold values from -6 to 6
- cutoffs: int32 [2], replicated, may hold values from 128 to 512
Outputs:
- update: float32 [5, 4, 256, 1024], P(None, None, 'span', 'pitch')
The draws below stay inside these ranges and needn't reach their ends.
Inputs may be any that keep to these rules, and one draw needn't show every extreme that they name: `inverse_diagonal`: each cell's block is dominated by its diagonal; the sweeps' recurrences are stable.
All inputs are finite; a program needn't handle non-finite values.
Results may differ from the reference program's by a relative error of at most 0.0003.
Values sent between devices are 32-bit elements; how exact they have to be, the bound alone decides.
A program may use at most 64 MiB of HBM per device.

```python
import jax
import jax.numpy as jnp
from jax import lax

VARIABLES = 5
NP = 1024
HARMONICS = 512
AXIAL = 4
SPANWISE_VOLUMES = 256


def draw_inverse_diagonal(key, part):
    first_key, interaction_seed, third_key = jax.random.split(jax.random.fold_in(key, 11), 3)
    shape = (VARIABLES, AXIAL, SPANWISE_VOLUMES, NP)
    spread = jax.random.uniform(first_key, shape, jnp.float32, 0.0, 0.004)
    relaxation_passes = jax.random.randint(interaction_seed, (2,), 0, SPANWISE_VOLUMES)
    spanwise_location = jnp.arange(SPANWISE_VOLUMES, dtype=jnp.int32)
    affected_volumes = jnp.any(spanwise_location[:, None] == relaxation_passes[None, :], axis=1)
    factor = jnp.where(affected_volumes, 0.75, 1.0).astype(jnp.float32)[None, None, :, None]
    diagonal = jnp.exp(-spread) * factor
    full_shape = (VARIABLES, VARIABLES, AXIAL, SPANWISE_VOLUMES, NP)
    offdiag = jnp.clip(0.03 * jax.random.normal(third_key, full_shape, jnp.float32), -0.1, 0.1)
    identity = jnp.eye(VARIABLES, dtype=jnp.float32)[:, :, None, None, None]
    return offdiag * (1.0 - identity) + identity * diagonal[:, None]


def draw_coupling(key, part):
    keys = jax.random.split(jax.random.fold_in(key, 23), 4)
    order = jax.random.permutation(keys[0], VARIABLES)
    slow = order < 3
    rates = jnp.where(slow, 0.998, 0.9).astype(jnp.float32)
    lower_part = jnp.tril(0.05 * jax.random.normal(keys[1], (VARIABLES, VARIABLES), jnp.float32), -1)
    upper_part = jnp.tril(0.05 * jax.random.normal(keys[2], (VARIABLES, VARIABLES), jnp.float32), -1)
    radial_lower = -(jnp.diag(rates) + lower_part)
    radial_upper = jnp.diag(rates) + upper_part
    others = jnp.clip(0.1 * jax.random.normal(keys[3], (4, VARIABLES, VARIABLES), jnp.float32), -0.4, 0.4)
    return jnp.concatenate([radial_lower[None], radial_upper[None], others], axis=0)


def block_scale(rng, shape, pieces, low, high):
    def one(position, parts):
        steps = jax.random.uniform(jax.random.fold_in(jax.random.fold_in(rng, 6), position), (parts,), jnp.float32, low / len(pieces), high / len(pieces))
        return jnp.repeat(jnp.exp(steps), shape[position] // parts).reshape((-1,) + (1,) * (len(shape) - position - 1))

    gain = one(*pieces[0])
    for cut in pieces[1:]:
        gain = gain * one(*cut)
    return gain


def bell_draw(rng, extent, deviation, limit, cuts=(), kind=jnp.bfloat16):
    loudness = block_scale(rng, extent, cuts, -0.22, 0.18) if cuts else 1.0
    values = jax.random.normal(rng, extent, jnp.float32) * deviation * loudness
    return jnp.minimum(jnp.maximum(values, -limit), limit).astype(kind)


def setup_inputs(seed: int = 0) -> dict:
    streams_of = jax.random.split(jax.random.key(seed), 7)
    residual = bell_draw(streams_of[0], (VARIABLES, AXIAL, SPANWISE_VOLUMES, NP), 0.1, 0.6, ((2, 32), (3, 8)), jnp.float32)
    inverse_diagonal = draw_inverse_diagonal(jax.random.fold_in(streams_of[6], 71), 0)
    prior_increment = bell_draw(streams_of[2], (VARIABLES, AXIAL, SPANWISE_VOLUMES, NP), 0.5, 3.0, ((2, 32), (3, 8)), jnp.float32)
    coupling = draw_coupling(jax.random.fold_in(streams_of[6], 71), 0)
    characteristic = bell_draw(streams_of[4], (2, 2, HARMONICS, VARIABLES, VARIABLES), 1.0, 6.0, (), jnp.float32)
    cutoffs = jax.random.randint(streams_of[5], (2,), HARMONICS // 4, HARMONICS + 1).astype(jnp.int32)
    return {"residual": residual, "inverse_diagonal": inverse_diagonal, "prior_increment": prior_increment, "coupling": coupling, "characteristic": characteristic, "cutoffs": cutoffs}


highest = lax.Precision.HIGHEST


def angle_tables(pitch_index, harmonic_index, points):
    product = (pitch_index[:, None] * harmonic_index[None, :]) % points
    angles = product.astype(jnp.float32) * (2.0 * jnp.pi / points)
    return jnp.cos(angles), jnp.sin(angles)


def forward_dft(spanwise_slices, cosine, sine):
    flat = spanwise_slices.reshape(-1, spanwise_slices.shape[-1])
    shape = spanwise_slices.shape[:-1] + (cosine.shape[1],)
    real_part = jnp.dot(flat, cosine, precision=highest).reshape(shape)
    imag_part = -jnp.dot(flat, sine, precision=highest).reshape(shape)
    return real_part, imag_part


def contract(matrix, spectrum):
    return jnp.einsum('pkij,pjrk->pirk', matrix, spectrum, precision=highest)


def apply_harmonics(real_part, imag_part, characteristic, cutoffs, first_harmonic, points):
    char_real = characteristic[:, 0]
    char_imag = characteristic[:, 1]
    result_real_component = contract(char_real, real_part) - contract(char_imag, imag_part)
    out_imag = contract(char_real, imag_part) + contract(char_imag, real_part)
    harmonic = first_harmonic + jnp.arange(real_part.shape[-1], dtype=jnp.int32)
    kept = (harmonic[None, :] < cutoffs[:, None]).astype(jnp.float32)
    weight = jnp.where(harmonic == 0, 1.0, 2.0).astype(jnp.float32) / points
    factor = (kept * weight[None, :])[:, None, None, :]
    return result_real_component * factor, out_imag * factor


def inverse_dft(result_real_component, out_imag, cosine, sine):
    shape = result_real_component.shape[:-1] + (cosine.shape[0],)
    flat_real = result_real_component.reshape(-1, result_real_component.shape[-1])
    flat_imag = out_imag.reshape(-1, out_imag.shape[-1])
    result = jnp.dot(flat_real, cosine.T, precision=highest) - jnp.dot(flat_imag, sine.T, precision=highest)
    return result.reshape(shape)


def mix_field(matrix, field):
    return jnp.einsum('ij,jarp->iarp', matrix, field, precision=highest)


def mix_vector(matrix, vector):
    return jnp.einsum('ij,jap->iap', matrix, vector, precision=highest)


def apply_block(block, vector):
    return jnp.einsum('ijap,jap->iap', block, vector, precision=highest)


def reference(residual, inverse_diagonal, prior_increment, coupling, characteristic, cutoffs):
    spanwise_slices = jnp.stack([residual[:, 0], residual[:, -1]])
    pitch_index = jnp.arange(NP, dtype=jnp.int32)
    harmonic_index = jnp.arange(HARMONICS, dtype=jnp.int32)
    cosine, sine = angle_tables(pitch_index, harmonic_index, NP)
    real_part, imag_part = forward_dft(spanwise_slices, cosine, sine)
    result_real_component, out_imag = apply_harmonics(real_part, imag_part, characteristic, cutoffs, 0, NP)
    correction = inverse_dft(result_real_component, out_imag, cosine, sine)
    corrected = residual.at[:, 0].add(correction[0]).at[:, -1].add(correction[1])
    padded = jnp.concatenate([prior_increment[..., -1:], prior_increment, prior_increment[..., :1]], axis=3)
    axial_pad = jnp.pad(prior_increment, ((0, 0), (1, 1), (0, 0), (0, 0)))
    source = corrected - mix_field(coupling[2], padded[..., :-2]) - mix_field(coupling[3], padded[..., 2:])
    source = source - mix_field(coupling[4], axial_pad[:, :-2]) - mix_field(coupling[5], axial_pad[:, 2:])
    diag_rows = jnp.moveaxis(inverse_diagonal, 3, 0)
    source_rows = jnp.moveaxis(source, 2, 0)
    zeros = jnp.zeros((residual.shape[0], residual.shape[1], residual.shape[3]), jnp.float32)

    def forward_sweep_step(previous, pair):
        block, rhs_row = pair
        current = apply_block(block, rhs_row - mix_vector(coupling[0], previous))
        return current, current

    _, star_rows = lax.scan(forward_sweep_step, zeros, (diag_rows, source_rows))

    def backward_step(following, pair):
        block, star_row = pair
        current = star_row - apply_block(block, mix_vector(coupling[1], following))
        return current, current

    _, final_rows = lax.scan(backward_step, zeros, (diag_rows, star_rows), reverse=True)
    return jnp.moveaxis(final_rows, 0, 2)
```

```python
import jax
import jax.numpy as jnp
import numpy as np
from jax import lax
from jax.experimental import pallas as pl
from jax.experimental.pallas import tpu as pltpu
from jax.sharding import PartitionSpec as P

NP = 1024
PITCH = 8
GROUP = 4
LAYERS = 8
V = 5
LINE = 16
MAPS = 80
VECS = 16
LANES = 128
HIGHEST = lax.Precision.HIGHEST

SPREAD, TWIDDLE, FORWARD, BACK_RE, BACK_IM, GATHER_RE, GATHER_IM = np.cumsum([0, 160, 16, 256, 128, 128, 128]).tolist()


def table():
    two_pi = 2.0 * np.pi
    a = np.arange(8)
    b = np.arange(128)
    k2 = np.arange(64)
    eight = two_pi * (np.outer(a, a) % 8) / 8
    spread = np.zeros((2, 10, 8, 8, LINE))
    for line in range(10):
        spread[0, line, :, :, line] = np.cos(eight)
        spread[1, line, :, :, line] = -np.sin(eight)
    twiddle = two_pi * np.outer(a, b) / NP
    lanes = two_pi * (np.outer(b, k2) % 128) / 128
    cos, sin = np.cos(lanes), np.sin(lanes)
    forward = np.block([[cos, -sin], [sin, cos]])
    back_re = np.concatenate([cos.T, -sin.T], 0)
    back_im = np.concatenate([sin.T, cos.T], 0)
    gather_re = np.zeros((8, LINE, 16, 8))
    gather_im = np.zeros((8, LINE, 16, 8))
    for line in range(10):
        gather_re[:, line, line, :] = np.cos(eight)
        gather_im[:, line, line, :] = -np.sin(eight)
    parts = [
        spread.reshape(160, 128),
        np.cos(twiddle),
        np.sin(twiddle),
        forward,
        back_re,
        back_im,
        gather_re.reshape(128, 128),
        gather_im.reshape(128, 128),
    ]
    return np.concatenate(parts, 0).astype(np.float32)


def every(start, stride):
    return pl.ds(start, 8, stride=stride)


def rows(start, size):
    return pl.ds(pl.multiple_of(start, 8), size)


def product(later, earlier):
    total = later[0][None] * earlier[:, 0][:, None]
    for j in range(1, V):
        total = total + later[j][None] * earlier[:, j][:, None]
    return total


def apply(matrix, vector):
    total = matrix[0] * vector[0][None]
    for j in range(1, V):
        total = total + matrix[j] * vector[j][None]
    return total


def scaled(block, coupling, which):
    columns = []
    for k in range(V):
        total = block[:, 0] * (-coupling[which, k])
        for j in range(1, V):
            total = total + block[:, j] * (-coupling[which, j * V + k])
        columns.append(total)
    return jnp.stack(columns)


def kernel(
    residual, inverse, prior, coupling, characteristic, cutoffs, const, out,
    lower, upper, planes_out, planes_in, corr_out, corr_in,
    maps_out, maps_in, layer_maps, vecs_out, vecs_in, layer_vecs, entry_out, entry_in,
    down, up, first, second, third, source, base, flat, spectra,
    pitch_s, pitch_r, back_s, back_r, side_s, side_r,
    gm_s, gm_r, zm_s, zm_r, gv_s, gv_r, zv_s, zv_r, ge_s, ge_r,
):
    pitch = lax.axis_index("pitch")
    span = lax.axis_index("span")
    layer = span // GROUP
    member = span % GROUP

    def at_pitch(d):
        return {"pitch": lax.rem(pitch + d, PITCH), "span": span}

    def at_member(d):
        return {"pitch": pitch, "span": layer * GROUP + lax.rem(member + d, GROUP)}

    def at_layer(d):
        return {"pitch": pitch, "span": lax.rem(layer + d, LAYERS) * GROUP + member}

    peers = [at_pitch(d) for d in range(1, PITCH)]
    peers += [at_member(d) for d in range(1, GROUP)]
    peers += [at_layer(d) for d in range(1, LAYERS)]
    barrier = pltpu.get_barrier_semaphore()
    for peer in peers:
        pl.semaphore_signal(barrier, inc=1, device_id=peer, device_id_type=pl.DeviceIdType.MESH)

    def send(src, dst, send_sem, recv_sem, peer):
        copy = pltpu.make_async_remote_copy(
            src_ref=src, dst_ref=dst, send_sem=send_sem, recv_sem=recv_sem,
            device_id=peer, device_id_type=pl.DeviceIdType.MESH,
        )
        copy.start()
        return copy

    planes_out[...] = jnp.zeros_like(planes_out)
    for q, axial in enumerate((0, GROUP - 1)):
        for j in range(V):
            planes_out[every(q * V + j, LINE), :] = residual[j, axial * 8 : axial * 8 + 8, :]

    maps_out[...] = jnp.zeros_like(maps_out)
    vecs_out[...] = jnp.zeros_like(vecs_out)
    reach = None
    for s in range(4):
        block = inverse[:, :, every(s, 4), :]
        down[s] = scaled(block, coupling, 0)
        up[s] = scaled(block, coupling, 1)
        reach = down[s] if s == 0 else product(down[s], reach)
        first[s] = reach
    for k in range(V):
        for i in range(V):
            maps_out[every(8 * k + i, MAPS), :] = reach[k, i]
    both = reach
    trail = up[3]
    second[3] = both
    third[3] = trail
    for s in (2, 1, 0):
        both = first[s] + product(up[s], both)
        trail = product(up[s], trail)
        second[s] = both
        third[s] = trail
    for k in range(V):
        for i in range(V):
            maps_out[every(40 + 8 * k + i, MAPS), :] = trail[k, i]
            maps_out[every(8 * k + 5 + i if i < 3 else 40 + 8 * k + 2 + i, MAPS), :] = both[k, i]

    pl.semaphore_wait(barrier, len(peers))

    pitch_copies = []
    for d in range(1, PITCH):
        to = lax.rem(pitch + d, PITCH)
        pitch_copies.append(send(
            planes_out.at[rows(to * LINE, LINE)], planes_in.at[rows(pitch * LINE, LINE)],
            pitch_s.at[d], pitch_r.at[d], at_pitch(d),
        ))
    side_copies = [
        send(prior, lower, side_s.at[0], side_r.at[0], at_pitch(1)),
        send(prior, upper, side_s.at[1], side_r.at[1], at_pitch(PITCH - 1)),
    ]
    map_copies = []
    for d in range(1, GROUP):
        to = lax.rem(member + d, GROUP)
        map_copies.append(send(
            maps_out.at[rows(to * 2 * MAPS, 2 * MAPS)], maps_in.at[rows(member * 2 * MAPS, 2 * MAPS)],
            gm_s.at[d], gm_r.at[d], at_member(d),
        ))
    planes_in[rows(pitch * LINE, LINE), :] = planes_out[rows(pitch * LINE, LINE), :]
    maps_in[rows(member * 2 * MAPS, 2 * MAPS), :] = maps_out[rows(member * 2 * MAPS, 2 * MAPS), :]

    flat[100:104, :] = jnp.zeros((4, 512), jnp.float32)
    for n in range(50):
        flat[2 * n : 2 * n + 2, :] = characteristic[n]
    whole = flat[...]
    high = whole.astype(jnp.bfloat16)
    rest = whole - high.astype(jnp.float32)
    middle = rest.astype(jnp.bfloat16)
    low = (rest - middle.astype(jnp.float32)).astype(jnp.bfloat16)
    harmonic = lax.broadcasted_iota(jnp.int32, (512, LANES), 0)
    lane = lax.broadcasted_iota(jnp.int32, (512, LANES), 1)
    apart = harmonic - 8 * (lane % 64)
    for k1 in range(8):
        pick = jnp.where(apart == k1, 1.0, 0.0).astype(jnp.bfloat16)
        part = jnp.dot(high, pick, preferred_element_type=jnp.float32)
        part = part + jnp.dot(middle, pick, preferred_element_type=jnp.float32)
        part = part + jnp.dot(low, pick, preferred_element_type=jnp.float32)
        spectra[pl.ds(k1, 104, stride=8), :] = part

    for copy in side_copies:
        copy.wait_recv()
    column = lax.broadcasted_iota(jnp.int32, (V, 32, LANES), 2)
    own = prior[...]
    below = pltpu.roll(jnp.where(column == LANES - 1, lower[...], own), 1, 2)
    above = pltpu.roll(jnp.where(column == 0, upper[...], own), LANES - 1, 2)
    zero_row = jnp.zeros((8, LANES), jnp.float32)
    for i in range(V):
        total = residual[i]
        before = after = None
        for j in range(V):
            total = total - coupling[2, i * V + j] * below[j] - coupling[3, i * V + j] * above[j]
            low_term = coupling[4, i * V + j] * own[j]
            high_term = coupling[5, i * V + j] * own[j]
            before = low_term if before is None else before + low_term
            after = high_term if after is None else after + high_term
        total = total - jnp.concatenate([zero_row, before[:24]], 0) - jnp.concatenate([after[8:], zero_row], 0)
        source[i] = total

    for copy in pitch_copies:
        copy.wait_recv()
    spread = jnp.dot(
        const[SPREAD : SPREAD + 160, :], planes_in[...], precision=HIGHEST, preferred_element_type=jnp.float32
    ).reshape(2, 10, 8, LANES)
    turn_re = const[TWIDDLE : TWIDDLE + 8, :][None]
    turn_im = const[TWIDDLE + 8 : TWIDDLE + 16, :][None]
    turned_re = (spread[0] * turn_re + spread[1] * turn_im).reshape(80, LANES)
    turned_im = (spread[1] * turn_re - spread[0] * turn_im).reshape(80, LANES)
    spectrum = jnp.dot(
        jnp.concatenate([turned_re, turned_im], 1), const[FORWARD : FORWARD + 256, :],
        precision=HIGHEST, preferred_element_type=jnp.float32,
    )
    number = lax.broadcasted_iota(jnp.int32, (8, LANES), 0) + 8 * (lax.broadcasted_iota(jnp.int32, (8, LANES), 1) % 64)
    weight = jnp.where(number == 0, 1.0, 2.0) / NP
    sign = jnp.where(lax.broadcasted_iota(jnp.int32, (80, LANES), 1) < 64, -1.0, 1.0)
    crossed = (pltpu.roll(spectrum, 64, 1) * sign).reshape(2, V, 8, LANES)
    spectrum = spectrum.reshape(2, V, 8, LANES)
    corrected = []
    for q in range(2):
        factor = jnp.where(number < cutoffs[q], weight, 0.0)
        for i in range(V):
            total = None
            for j in range(V):
                row = (q * 25 + i * V + j) * 16
                term = spectra[row : row + 8, :] * spectrum[q, j] + spectra[row + 8 : row + 16, :] * crossed[q, j]
                total = term if total is None else total + term
            corrected.append(total * factor)
    corrected = jnp.concatenate(corrected, 0)
    back_re = jnp.dot(
        corrected, const[BACK_RE : BACK_RE + 128, :], precision=HIGHEST, preferred_element_type=jnp.float32
    ).reshape(10, 8, LANES)
    back_im = jnp.dot(
        corrected, const[BACK_IM : BACK_IM + 128, :], precision=HIGHEST, preferred_element_type=jnp.float32
    ).reshape(10, 8, LANES)
    filler = jnp.zeros((48, LANES), jnp.float32)
    lines_re = jnp.concatenate([(back_re * turn_re - back_im * turn_im).reshape(80, LANES), filler], 0)
    lines_im = jnp.concatenate([(back_im * turn_re + back_re * turn_im).reshape(80, LANES), filler], 0)
    corr_out[...] = jnp.dot(
        const[GATHER_RE : GATHER_RE + 128, :], lines_re, precision=HIGHEST, preferred_element_type=jnp.float32
    ) + jnp.dot(
        const[GATHER_IM : GATHER_IM + 128, :], lines_im, precision=HIGHEST, preferred_element_type=jnp.float32
    )
    back_copies = []
    for d in range(1, PITCH):
        to = lax.rem(pitch + d, PITCH)
        back_copies.append(send(
            corr_out.at[rows(to * LINE, LINE)], corr_in.at[rows(pitch * LINE, LINE)],
            back_s.at[d], back_r.at[d], at_pitch(d),
        ))
    corr_in[rows(pitch * LINE, LINE), :] = corr_out[rows(pitch * LINE, LINE), :]

    place = lax.broadcasted_iota(jnp.int32, (8, LANES), 0)

    def tiles(ref, n, second_half):
        start = n * MAPS + (40 if second_half else 0)
        return [ref[start + 8 * j : start + 8 * j + 8, :] for j in range(V)]

    def spread_rows(vector):
        return [jnp.broadcast_to(vector[..., j : j + 1, :], vector.shape) for j in range(V)]

    def mix(matrix, parts):
        total = matrix[0] * parts[0]
        for j in range(1, V):
            total = total + matrix[j] * parts[j]
        return total

    def moved(top, bottom):
        axis = top.ndim - 2
        return jnp.where(place < 3, pltpu.roll(top, 3, axis), pltpu.roll(bottom, 6, axis))

    for copy in map_copies:
        copy.wait_recv()
    top = maps_in[0:40, :].reshape(V, 8, LANES)
    bottom = maps_in[40:80, :].reshape(V, 8, LANES)
    across = [moved(top, bottom)]
    forward = top
    for n in range(1, 8):
        parts = spread_rows(forward)
        forward = mix(tiles(maps_in, n, False), parts)
        across.append(moved(forward, mix(tiles(maps_in, n, True), parts)))
    backward = jnp.concatenate([maps_in[7 * MAPS + 40 : 8 * MAPS, :].reshape(V, 8, LANES), across[7]], 0)
    for n in range(6, -1, -1):
        backward = mix(tiles(maps_in, n, True), spread_rows(backward))
        backward = jnp.concatenate([backward[:V], backward[V:] + across[n]], 0)
    mine = pl.multiple_of(layer * MAPS, 8)
    whole_top = jnp.where(place < V, forward, pltpu.roll(backward[V:], 5, 1))
    whole_bottom = jnp.where(place < V, backward[:V], pltpu.roll(backward[V:], 2, 1))
    layer_maps[pl.ds(mine, 40), :] = whole_top.reshape(40, LANES)
    layer_maps[pl.ds(pl.multiple_of(layer * MAPS + 40, 8), 40), :] = whole_bottom.reshape(40, LANES)
    layer_copies = []
    for d in range(1, LAYERS):
        layer_copies.append(send(
            layer_maps.at[rows(layer * MAPS, MAPS)], layer_maps.at[rows(layer * MAPS, MAPS)],
            zm_s.at[d], zm_r.at[d], at_layer(d),
        ))

    for copy in back_copies:
        copy.wait_recv()
    for j in range(V):
        source[j, 0:8, :] = source[j, 0:8, :] + corr_in[every(j, LINE), :]
        source[j, 24:32, :] = source[j, 24:32, :] + corr_in[every(V + j, LINE), :]
    star = None
    for s in range(4):
        block = inverse[:, :, every(s, 4), :]
        rhs = source[:, every(s, 4), :]
        value = block[:, 0] * rhs[0][None]
        for j in range(1, V):
            value = value + block[:, j] * rhs[j][None]
        star = value if s == 0 else value + apply(down[s], star)
        base[s] = star
    for i in range(V):
        vecs_out[every(i, VECS), :] = star[i]
    update = star
    for s in (2, 1, 0):
        update = base[s] + apply(up[s], update)
        base[s] = update
    for i in range(V):
        vecs_out[every(8 + i, VECS), :] = update[i]
    vec_copies = []
    for d in range(1, GROUP):
        to = lax.rem(member + d, GROUP)
        vec_copies.append(send(
            vecs_out.at[rows(to * 2 * VECS, 2 * VECS)], vecs_in.at[rows(member * 2 * VECS, 2 * VECS)],
            gv_s.at[d], gv_r.at[d], at_member(d),
        ))
    vecs_in[rows(member * 2 * VECS, 2 * VECS), :] = vecs_out[rows(member * 2 * VECS, 2 * VECS), :]

    def chain(maps_ref, vecs_ref, x, y):
        entering_x, entering_y, crossing = [], [None] * 8, []
        for n in range(8):
            entering_x.append(x)
            offset = vecs_ref[n * VECS : n * VECS + 8, :]
            if x is None:
                crossing.append(vecs_ref[n * VECS + 8 : n * VECS + 16, :])
                x = offset
            else:
                parts = spread_rows(x)
                ahead = mix(tiles(maps_ref, n, False), parts)
                aside = mix(tiles(maps_ref, n, True), parts)
                crossing.append(moved(ahead, aside) + vecs_ref[n * VECS + 8 : n * VECS + 16, :])
                x = ahead + offset
        for n in range(7, -1, -1):
            entering_y[n] = y
            y = crossing[n] if y is None else mix(tiles(maps_ref, n, True), spread_rows(y)) + crossing[n]
        return entering_x, entering_y, x, y

    for copy in vec_copies:
        copy.wait_recv()
    _, _, x, y = chain(maps_in, vecs_in, None, None)
    layer_vecs[pl.ds(pl.multiple_of(layer * VECS, 8), 8), :] = x
    layer_vecs[pl.ds(pl.multiple_of(layer * VECS + 8, 8), 8), :] = y
    vec_layer_copies = []
    for d in range(1, LAYERS):
        vec_layer_copies.append(send(
            layer_vecs.at[rows(layer * VECS, VECS)], layer_vecs.at[rows(layer * VECS, VECS)],
            zv_s.at[d], zv_r.at[d], at_layer(d),
        ))
    for copy in layer_copies:
        copy.wait_recv()
    for copy in vec_layer_copies:
        copy.wait_recv()
    entering_x, entering_y, _, _ = chain(layer_maps, layer_vecs, None, None)
    x = jnp.zeros((8, LANES), jnp.float32)
    y = jnp.zeros((8, LANES), jnp.float32)
    for n in range(8):
        if entering_x[n] is not None:
            x = jnp.where(layer == n, entering_x[n], x)
        if entering_y[n] is not None:
            y = jnp.where(layer == n, entering_y[n], y)
    entering_x, entering_y, _, _ = chain(maps_in, vecs_in, x, y)
    for n in range(8):
        entry_out[n * VECS : n * VECS + 8, :] = entering_x[n]
        entry_out[n * VECS + 8 : n * VECS + 16, :] = entering_y[n]
    entry_copies = []
    for d in range(1, GROUP):
        to = lax.rem(member + d, GROUP)
        entry_copies.append(send(
            entry_out.at[rows(to * 2 * VECS, 2 * VECS)], entry_in.at[rows(member * 2 * VECS, 2 * VECS)],
            ge_s.at[d], ge_r.at[d], at_member(d),
        ))
    entry_in[rows(member * 2 * VECS, 2 * VECS), :] = entry_out[rows(member * 2 * VECS, 2 * VECS), :]
    for copy in entry_copies:
        copy.wait_recv()
    x = [entry_in[every(i, VECS), :] for i in range(V)]
    y = [entry_in[every(8 + i, VECS), :] for i in range(V)]
    for s in range(4):
        value = base[s]
        for j in range(V):
            value = value + second[s, j] * x[j][None] + third[s, j] * y[j][None]
        for i in range(V):
            out[i, every(s, 4), :] = value[i]

    for copy in pitch_copies + side_copies + map_copies + back_copies + layer_copies:
        copy.wait_send()
    for copy in vec_copies + vec_layer_copies + entry_copies:
        copy.wait_send()


def body(residual, inverse_diagonal, prior_increment, coupling, characteristic, cutoffs):
    f32 = jnp.float32
    fields = (V, 32, LANES)
    matrices = pltpu.VMEM((4, V, V, 8, LANES), f32)

    def vmem(count):
        return pltpu.VMEM((count, LANES), f32)

    def sems(count):
        return [pltpu.SemaphoreType.DMA((count,))] * 2

    scratch = [
        pltpu.VMEM(fields, f32), pltpu.VMEM(fields, f32),
        vmem(128), vmem(128), vmem(128), vmem(128),
        vmem(8 * MAPS), vmem(8 * MAPS), vmem(8 * MAPS),
        vmem(8 * VECS), vmem(8 * VECS), vmem(8 * VECS), vmem(8 * VECS), vmem(8 * VECS),
        matrices, matrices, matrices, matrices, matrices,
        pltpu.VMEM(fields, f32), pltpu.VMEM((4, V, 8, LANES), f32),
        pltpu.VMEM((104, 512), f32), vmem(104 * 8),
        *sems(PITCH), *sems(PITCH), *sems(2),
        *sems(GROUP), *sems(LAYERS), *sems(GROUP), *sems(LAYERS), *sems(GROUP),
    ]
    inside = pl.BlockSpec(memory_space=pltpu.VMEM)
    scalars = pl.BlockSpec(memory_space=pltpu.SMEM)
    result = pl.pallas_call(
        kernel,
        out_shape=jax.ShapeDtypeStruct(fields, f32),
        in_specs=[inside, inside, inside, scalars, inside, scalars, inside],
        out_specs=inside,
        scratch_shapes=scratch,
        compiler_params=pltpu.CompilerParams(collective_id=0, has_side_effects=True),
    )(
        residual.reshape(fields),
        inverse_diagonal.reshape(V, V, 32, LANES),
        prior_increment.reshape(fields),
        coupling.reshape(6, V * V),
        characteristic.transpose(0, 3, 4, 1, 2).reshape(50, 2, 512),
        cutoffs,
        jnp.asarray(table()),
    )
    return result.reshape(V, GROUP, 8, LANES)


def solution(mesh):
    field = P(None, None, "span", "pitch")
    return jax.shard_map(
        body, mesh=mesh,
        in_specs=(field, P(None, None, None, "span", "pitch"), field, P(), P(), P()),
        out_specs=field, check_vma=False,
    )
```

```python
import jax
import jax.numpy as jnp
import numpy as np
from jax import lax
from jax.experimental import pallas as pl
from jax.experimental.pallas import tpu as pltpu
from jax.sharding import PartitionSpec as P

NP = 1024
PITCH = 8
GROUP = 4
LAYERS = 8
V = 5
LINE = 16
MAPS = 80
VECS = 16
LANES = 128

SPREAD, FORWARD, BACK_RE, BACK_IM, GATHER_RE, GATHER_IM, LOW = np.cumsum([0, 160, 256, 128, 128, 128, 128]).tolist()


def table():
    two_pi = 2.0 * np.pi
    a = np.arange(8)
    b = np.arange(128)
    k2 = np.arange(64)
    eight = two_pi * (np.outer(a, a) % 8) / 8
    spread = np.zeros((2, 10, 8, 8, LINE))
    for line in range(10):
        spread[0, line, :, :, line] = np.cos(eight)
        spread[1, line, :, :, line] = -np.sin(eight)
    twiddle = two_pi * np.outer(a, b) / NP
    lanes = two_pi * (np.outer(b, k2) % 128) / 128
    cos, sin = np.cos(lanes), np.sin(lanes)
    forward = np.block([[cos, -sin], [sin, cos]])
    back_re = np.concatenate([cos.T, -sin.T], 0)
    back_im = np.concatenate([sin.T, cos.T], 0)
    gather_re = np.zeros((8, LINE, 16, 8))
    gather_im = np.zeros((8, LINE, 16, 8))
    for line in range(10):
        gather_re[:, line, line, :] = np.cos(eight)
        gather_im[:, line, line, :] = -np.sin(eight)
    parts = [
        spread.reshape(160, 128),
        forward,
        back_re,
        back_im,
        gather_re.reshape(128, 128),
        gather_im.reshape(128, 128),
    ]
    whole = np.concatenate(parts, 0).astype(np.float32)
    high = whole.astype(jnp.bfloat16)
    low = (whole - high.astype(np.float32)).astype(jnp.bfloat16)
    turns = np.concatenate([np.cos(twiddle), np.sin(twiddle)], 0).astype(np.float32)
    return np.concatenate([high, low], 0), turns


def every(start, stride):
    return pl.ds(start, 8, stride=stride)


def rows(start, size):
    return pl.ds(pl.multiple_of(start, 8), size)


def product(later, earlier):
    total = later[0][None] * earlier[:, 0][:, None]
    for j in range(1, V):
        total = total + later[j][None] * earlier[:, j][:, None]
    return total


def apply(matrix, vector):
    total = matrix[0] * vector[0][None]
    for j in range(1, V):
        total = total + matrix[j] * vector[j][None]
    return total


def scaled(block, coupling, which):
    columns = []
    for k in range(V):
        total = block[:, 0] * (-coupling[0, which, k])
        for j in range(1, V):
            total = total + block[:, j] * (-coupling[j, which, k])
        columns.append(total)
    return jnp.stack(columns)


def times(data, const, start, size, left=False):
    data_high = data.astype(jnp.bfloat16)
    data_low = (data - data_high.astype(jnp.float32)).astype(jnp.bfloat16)
    high = const[start : start + size, :]
    low = const[LOW + start : LOW + start + size, :]
    pairs = ((data_high, high), (data_low, high), (data_high, low))
    total = None
    for x, w in pairs:
        part = jnp.dot(w, x, preferred_element_type=jnp.float32) if left else jnp.dot(x, w, preferred_element_type=jnp.float32)
        total = part if total is None else total + part
    return total


def kernel(
    residual_in, inverse_in, prior_in, coupling, characteristic_in, cutoffs, const_in, turns_in, out,
    residual, inverse, prior, characteristic, const, turns, load_s,
    lower, upper, edge_low, edge_high, planes_out, planes_in, corr_out, corr_in,
    maps_out, maps_in, layer_maps, vecs_out, vecs_in, layer_vecs, entry_out, entry_in,
    down, up, first, second, third, source, base, flat, spectra,
    pitch_s, pitch_r, back_s, back_r, side_s, side_r,
    gm_s, gm_r, zm_s, zm_r, gv_s, gv_r, zv_s, zv_r, ge_s, ge_r,
):
    pitch = lax.axis_index("pitch")
    span = lax.axis_index("span")
    layer = span // GROUP
    member = span % GROUP

    def at_pitch(d):
        return {"pitch": lax.rem(pitch + d, PITCH), "span": span}

    def at_member(d):
        return {"pitch": pitch, "span": layer * GROUP + lax.rem(member + d, GROUP)}

    def at_layer(d):
        return {"pitch": pitch, "span": lax.rem(layer + d, LAYERS) * GROUP + member}

    peers = [at_pitch(d) for d in range(1, PITCH)]
    peers += [at_member(d) for d in range(1, GROUP)]
    peers += [at_layer(d) for d in range(1, LAYERS)]
    barrier = pltpu.get_barrier_semaphore()
    for peer in peers:
        pl.semaphore_signal(barrier, inc=1, device_id=peer, device_id_type=pl.DeviceIdType.MESH)

    loads = []
    for n, (src, dst) in enumerate((
        (residual_in, residual), (prior_in, prior), (inverse_in, inverse),
        (characteristic_in, characteristic), (const_in, const), (turns_in, turns),
    )):
        loads.append(pltpu.make_async_copy(src, dst, load_s.at[n]))
        loads[-1].start()

    def send(src, dst, send_sem, recv_sem, peer):
        copy = pltpu.make_async_remote_copy(
            src_ref=src, dst_ref=dst, send_sem=send_sem, recv_sem=recv_sem,
            device_id=peer, device_id_type=pl.DeviceIdType.MESH,
        )
        copy.start()
        return copy

    planes_out[...] = jnp.zeros_like(planes_out)
    maps_out[...] = jnp.zeros_like(maps_out)
    vecs_out[...] = jnp.zeros_like(vecs_out)
    loads[0].wait()
    for q, axial in enumerate((0, GROUP - 1)):
        for j in range(V):
            planes_out[every(q * V + j, LINE), :] = residual[j, axial * 8 : axial * 8 + 8, :]

    pl.semaphore_wait(barrier, len(peers))

    pitch_copies = []
    for d in range(1, PITCH):
        to = lax.rem(pitch + d, PITCH)
        pitch_copies.append(send(
            planes_out.at[rows(to * LINE, LINE)], planes_in.at[rows(pitch * LINE, LINE)],
            pitch_s.at[d], pitch_r.at[d], at_pitch(d),
        ))
    loads[1].wait()
    column = lax.broadcasted_iota(jnp.int32, (8, LANES), 1)
    last = initial = jnp.zeros((8, LANES), jnp.float32)
    for n in range(V * GROUP):
        tile = prior[n // GROUP, n % GROUP * 8 : n % GROUP * 8 + 8, :]
        last = jnp.where(column == n, pltpu.roll(tile, n + 1, 1), last)
        initial = jnp.where(column == n, pltpu.roll(tile, n, 1) if n else tile, initial)
    edge_high[...] = last
    edge_low[...] = initial
    side_copies = [
        send(edge_high, lower, side_s.at[0], side_r.at[0], at_pitch(1)),
        send(edge_low, upper, side_s.at[1], side_r.at[1], at_pitch(PITCH - 1)),
    ]

    loads[2].wait()
    reach = None
    for s in range(4):
        block = inverse[:, :, every(s, 4), :]
        down[s] = scaled(block, coupling, 0)
        up[s] = scaled(block, coupling, 1)
        reach = down[s] if s == 0 else product(down[s], reach)
        first[s] = reach
    for k in range(V):
        for i in range(V):
            maps_out[every(8 * k + i, MAPS), :] = reach[k, i]
    both = reach
    trail = up[3]
    second[3] = both
    third[3] = trail
    for s in (2, 1, 0):
        both = first[s] + product(up[s], both)
        trail = product(up[s], trail)
        second[s] = both
        third[s] = trail
    for k in range(V):
        for i in range(V):
            maps_out[every(40 + 8 * k + i, MAPS), :] = trail[k, i]
            maps_out[every(8 * k + 5 + i if i < 3 else 40 + 8 * k + 2 + i, MAPS), :] = both[k, i]

    map_copies = []
    for d in range(1, GROUP):
        to = lax.rem(member + d, GROUP)
        map_copies.append(send(
            maps_out.at[rows(to * 2 * MAPS, 2 * MAPS)], maps_in.at[rows(member * 2 * MAPS, 2 * MAPS)],
            gm_s.at[d], gm_r.at[d], at_member(d),
        ))
    planes_in[rows(pitch * LINE, LINE), :] = planes_out[rows(pitch * LINE, LINE), :]
    maps_in[rows(member * 2 * MAPS, 2 * MAPS), :] = maps_out[rows(member * 2 * MAPS, 2 * MAPS), :]

    loads[3].wait()
    flat[100:104, :] = jnp.zeros((4, 512), jnp.float32)
    for n in range(50):
        flat[2 * n : 2 * n + 2, :] = characteristic[n]
    whole = flat[...]
    high = whole.astype(jnp.bfloat16)
    rest = whole - high.astype(jnp.float32)
    middle = rest.astype(jnp.bfloat16)
    low = (rest - middle.astype(jnp.float32)).astype(jnp.bfloat16)
    harmonic = lax.broadcasted_iota(jnp.int32, (512, LANES), 0)
    lane = lax.broadcasted_iota(jnp.int32, (512, LANES), 1)
    apart = harmonic - 8 * (lane % 64)
    for k1 in range(8):
        pick = jnp.where(apart == k1, 1.0, 0.0).astype(jnp.bfloat16)
        part = jnp.dot(high, pick, preferred_element_type=jnp.float32)
        part = part + jnp.dot(middle, pick, preferred_element_type=jnp.float32)
        part = part + jnp.dot(low, pick, preferred_element_type=jnp.float32)
        spectra[pl.ds(k1, 104, stride=8), :] = part

    for copy in pitch_copies:
        copy.wait_recv()
    loads[4].wait()
    loads[5].wait()
    spread = times(planes_in[...], const, SPREAD, 160, True).reshape(2, 10, 8, LANES)
    turn_re = turns[0:8, :][None]
    turn_im = turns[8:16, :][None]
    turned_re = (spread[0] * turn_re + spread[1] * turn_im).reshape(80, LANES)
    turned_im = (spread[1] * turn_re - spread[0] * turn_im).reshape(80, LANES)
    spectrum = times(jnp.concatenate([turned_re, turned_im], 1), const, FORWARD, 256)
    number = lax.broadcasted_iota(jnp.int32, (8, LANES), 0) + 8 * (lax.broadcasted_iota(jnp.int32, (8, LANES), 1) % 64)
    weight = jnp.where(number == 0, 1.0, 2.0) / NP
    sign = jnp.where(lax.broadcasted_iota(jnp.int32, (80, LANES), 1) < 64, -1.0, 1.0)
    crossed = (pltpu.roll(spectrum, 64, 1) * sign).reshape(2, V, 8, LANES)
    spectrum = spectrum.reshape(2, V, 8, LANES)
    corrected = []
    for q in range(2):
        factor = jnp.where(number < cutoffs[q], weight, 0.0)
        for i in range(V):
            total = None
            for j in range(V):
                row = (q * 25 + i * V + j) * 16
                term = spectra[row : row + 8, :] * spectrum[q, j] + spectra[row + 8 : row + 16, :] * crossed[q, j]
                total = term if total is None else total + term
            corrected.append(total * factor)
    corrected = jnp.concatenate(corrected, 0)
    back_re = times(corrected, const, BACK_RE, 128).reshape(10, 8, LANES)
    back_im = times(corrected, const, BACK_IM, 128).reshape(10, 8, LANES)
    filler = jnp.zeros((48, LANES), jnp.float32)
    lines_re = jnp.concatenate([(back_re * turn_re - back_im * turn_im).reshape(80, LANES), filler], 0)
    lines_im = jnp.concatenate([(back_im * turn_re + back_re * turn_im).reshape(80, LANES), filler], 0)
    corr_out[...] = times(lines_re, const, GATHER_RE, 128, True) + times(lines_im, const, GATHER_IM, 128, True)
    back_copies = []
    for d in range(1, PITCH):
        to = lax.rem(pitch + d, PITCH)
        back_copies.append(send(
            corr_out.at[rows(to * LINE, LINE)], corr_in.at[rows(pitch * LINE, LINE)],
            back_s.at[d], back_r.at[d], at_pitch(d),
        ))
    corr_in[rows(pitch * LINE, LINE), :] = corr_out[rows(pitch * LINE, LINE), :]

    place = lax.broadcasted_iota(jnp.int32, (8, LANES), 0)

    def tiles(ref, n, second_half):
        start = n * MAPS + (40 if second_half else 0)
        return [ref[start + 8 * j : start + 8 * j + 8, :] for j in range(V)]

    def spread_rows(vector):
        return [jnp.broadcast_to(vector[..., j : j + 1, :], vector.shape) for j in range(V)]

    def mix(matrix, parts):
        total = matrix[0] * parts[0]
        for j in range(1, V):
            total = total + matrix[j] * parts[j]
        return total

    def moved(top, bottom):
        axis = top.ndim - 2
        return jnp.where(place < 3, pltpu.roll(top, 3, axis), pltpu.roll(bottom, 6, axis))

    for copy in map_copies:
        copy.wait_recv()
    top = maps_in[0:40, :].reshape(V, 8, LANES)
    bottom = maps_in[40:80, :].reshape(V, 8, LANES)
    across = [moved(top, bottom)]
    forward = top
    for n in range(1, 8):
        parts = spread_rows(forward)
        forward = mix(tiles(maps_in, n, False), parts)
        across.append(moved(forward, mix(tiles(maps_in, n, True), parts)))
    backward = jnp.concatenate([maps_in[7 * MAPS + 40 : 8 * MAPS, :].reshape(V, 8, LANES), across[7]], 0)
    for n in range(6, -1, -1):
        backward = mix(tiles(maps_in, n, True), spread_rows(backward))
        backward = jnp.concatenate([backward[:V], backward[V:] + across[n]], 0)
    mine = pl.multiple_of(layer * MAPS, 8)
    whole_top = jnp.where(place < V, forward, pltpu.roll(backward[V:], 5, 1))
    whole_bottom = jnp.where(place < V, backward[:V], pltpu.roll(backward[V:], 2, 1))
    layer_maps[pl.ds(mine, 40), :] = whole_top.reshape(40, LANES)
    layer_maps[pl.ds(pl.multiple_of(layer * MAPS + 40, 8), 40), :] = whole_bottom.reshape(40, LANES)
    layer_copies = []
    for d in range(1, LAYERS):
        layer_copies.append(send(
            layer_maps.at[rows(layer * MAPS, MAPS)], layer_maps.at[rows(layer * MAPS, MAPS)],
            zm_s.at[d], zm_r.at[d], at_layer(d),
        ))

    for copy in side_copies:
        copy.wait_recv()
    own = prior[...]
    below, above = [], []
    for i in range(V):
        low_tiles, high_tiles = [], []
        for a in range(GROUP):
            n = i * GROUP + a
            tile = prior[i, a * 8 : a * 8 + 8, :]
            edge = pltpu.roll(lower[...], LANES - n, 1) if n else lower[...]
            low_tiles.append(jnp.where(column == 0, edge, pltpu.roll(tile, 1, 1)))
            edge = pltpu.roll(upper[...], LANES - 1 - n, 1)
            high_tiles.append(jnp.where(column == LANES - 1, edge, pltpu.roll(tile, LANES - 1, 1)))
        below.append(jnp.concatenate(low_tiles, 0))
        above.append(jnp.concatenate(high_tiles, 0))
    zero_row = jnp.zeros((8, LANES), jnp.float32)
    for i in range(V):
        total = residual[i]
        before = after = None
        for j in range(V):
            total = total - coupling[i, 2, j] * below[j] - coupling[i, 3, j] * above[j]
            low_term = coupling[i, 4, j] * own[j]
            high_term = coupling[i, 5, j] * own[j]
            before = low_term if before is None else before + low_term
            after = high_term if after is None else after + high_term
        total = total - jnp.concatenate([zero_row, before[:24]], 0) - jnp.concatenate([after[8:], zero_row], 0)
        source[i] = total

    for copy in back_copies:
        copy.wait_recv()
    for j in range(V):
        source[j, 0:8, :] = source[j, 0:8, :] + corr_in[every(j, LINE), :]
        source[j, 24:32, :] = source[j, 24:32, :] + corr_in[every(V + j, LINE), :]
    star = None
    for s in range(4):
        block = inverse[:, :, every(s, 4), :]
        rhs = source[:, every(s, 4), :]
        value = block[:, 0] * rhs[0][None]
        for j in range(1, V):
            value = value + block[:, j] * rhs[j][None]
        star = value if s == 0 else value + apply(down[s], star)
        base[s] = star
    for i in range(V):
        vecs_out[every(i, VECS), :] = star[i]
    update = star
    for s in (2, 1, 0):
        update = base[s] + apply(up[s], update)
        base[s] = update
    for i in range(V):
        vecs_out[every(8 + i, VECS), :] = update[i]
    vec_copies = []
    for d in range(1, GROUP):
        to = lax.rem(member + d, GROUP)
        vec_copies.append(send(
            vecs_out.at[rows(to * 2 * VECS, 2 * VECS)], vecs_in.at[rows(member * 2 * VECS, 2 * VECS)],
            gv_s.at[d], gv_r.at[d], at_member(d),
        ))
    vecs_in[rows(member * 2 * VECS, 2 * VECS), :] = vecs_out[rows(member * 2 * VECS, 2 * VECS), :]

    def chain(maps_ref, vecs_ref, x, y):
        entering_x, entering_y, crossing = [], [None] * 8, []
        for n in range(8):
            entering_x.append(x)
            offset = vecs_ref[n * VECS : n * VECS + 8, :]
            if x is None:
                crossing.append(vecs_ref[n * VECS + 8 : n * VECS + 16, :])
                x = offset
            else:
                parts = spread_rows(x)
                ahead = mix(tiles(maps_ref, n, False), parts)
                aside = mix(tiles(maps_ref, n, True), parts)
                crossing.append(moved(ahead, aside) + vecs_ref[n * VECS + 8 : n * VECS + 16, :])
                x = ahead + offset
        for n in range(7, -1, -1):
            entering_y[n] = y
            y = crossing[n] if y is None else mix(tiles(maps_ref, n, True), spread_rows(y)) + crossing[n]
        return entering_x, entering_y, x, y

    for copy in vec_copies:
        copy.wait_recv()
    _, _, x, y = chain(maps_in, vecs_in, None, None)
    layer_vecs[pl.ds(pl.multiple_of(layer * VECS, 8), 8), :] = x
    layer_vecs[pl.ds(pl.multiple_of(layer * VECS + 8, 8), 8), :] = y
    vec_layer_copies = []
    for d in range(1, LAYERS):
        vec_layer_copies.append(send(
            layer_vecs.at[rows(layer * VECS, VECS)], layer_vecs.at[rows(layer * VECS, VECS)],
            zv_s.at[d], zv_r.at[d], at_layer(d),
        ))
    for copy in layer_copies:
        copy.wait_recv()
    for copy in vec_layer_copies:
        copy.wait_recv()
    entering_x, entering_y, _, _ = chain(layer_maps, layer_vecs, None, None)
    x = jnp.zeros((8, LANES), jnp.float32)
    y = jnp.zeros((8, LANES), jnp.float32)
    for n in range(8):
        if entering_x[n] is not None:
            x = jnp.where(layer == n, entering_x[n], x)
        if entering_y[n] is not None:
            y = jnp.where(layer == n, entering_y[n], y)
    entering_x, entering_y, _, _ = chain(maps_in, vecs_in, x, y)
    for n in range(8):
        entry_out[n * VECS : n * VECS + 8, :] = entering_x[n]
        entry_out[n * VECS + 8 : n * VECS + 16, :] = entering_y[n]
    entry_copies = []
    for d in range(1, GROUP):
        to = lax.rem(member + d, GROUP)
        entry_copies.append(send(
            entry_out.at[rows(to * 2 * VECS, 2 * VECS)], entry_in.at[rows(member * 2 * VECS, 2 * VECS)],
            ge_s.at[d], ge_r.at[d], at_member(d),
        ))
    entry_in[rows(member * 2 * VECS, 2 * VECS), :] = entry_out[rows(member * 2 * VECS, 2 * VECS), :]
    for copy in entry_copies:
        copy.wait_recv()
    x = [entry_in[every(i, VECS), :] for i in range(V)]
    y = [entry_in[every(8 + i, VECS), :] for i in range(V)]
    for s in range(4):
        value = base[s]
        for j in range(V):
            value = value + second[s, j] * x[j][None] + third[s, j] * y[j][None]
        for i in range(V):
            out[i, every(s, 4), :] = value[i]

    for copy in pitch_copies + side_copies + map_copies + back_copies + layer_copies:
        copy.wait_send()
    for copy in vec_copies + vec_layer_copies + entry_copies:
        copy.wait_send()


def body(residual, inverse_diagonal, prior_increment, coupling, characteristic, cutoffs):
    f32 = jnp.float32
    fields = (V, 32, LANES)
    matrices = pltpu.VMEM((4, V, V, 8, LANES), f32)

    def vmem(count):
        return pltpu.VMEM((count, LANES), f32)

    def sems(count):
        return [pltpu.SemaphoreType.DMA((count,))] * 2

    scratch = [
        pltpu.VMEM(fields, f32), pltpu.VMEM((V, V, 32, LANES), f32), pltpu.VMEM(fields, f32),
        pltpu.VMEM((50, 2, 512), f32), pltpu.VMEM((2 * LOW, LANES), jnp.bfloat16), vmem(16),
        pltpu.SemaphoreType.DMA((6,)),
        vmem(8), vmem(8), vmem(8), vmem(8),
        vmem(128), vmem(128), vmem(128), vmem(128),
        vmem(8 * MAPS), vmem(8 * MAPS), vmem(8 * MAPS),
        vmem(8 * VECS), vmem(8 * VECS), vmem(8 * VECS), vmem(8 * VECS), vmem(8 * VECS),
        matrices, matrices, matrices, matrices, matrices,
        pltpu.VMEM(fields, f32), pltpu.VMEM((4, V, 8, LANES), f32),
        pltpu.VMEM((104, 512), f32), vmem(104 * 8),
        *sems(PITCH), *sems(PITCH), *sems(2),
        *sems(GROUP), *sems(LAYERS), *sems(GROUP), *sems(LAYERS), *sems(GROUP),
    ]
    inside = pl.BlockSpec(memory_space=pltpu.VMEM)
    outside = pl.BlockSpec(memory_space=pl.ANY)
    high_low, turns = table()
    scalars = pl.BlockSpec(memory_space=pltpu.SMEM)
    result = pl.pallas_call(
        kernel,
        out_shape=jax.ShapeDtypeStruct(fields, f32),
        in_specs=[outside, outside, outside, scalars, outside, scalars, outside, outside],
        out_specs=inside,
        scratch_shapes=scratch,
        compiler_params=pltpu.CompilerParams(collective_id=0, has_side_effects=True),
    )(
        residual.reshape(fields),
        inverse_diagonal.reshape(V, V, 32, LANES),
        prior_increment.reshape(fields),
        coupling.transpose(1, 0, 2),
        characteristic.transpose(0, 3, 4, 1, 2).reshape(50, 2, 512),
        cutoffs,
        jnp.asarray(high_low),
        jnp.asarray(turns),
    )
    return result.reshape(V, GROUP, 8, LANES)


def solution(mesh):
    field = P(None, None, "span", "pitch")
    return jax.shard_map(
        body, mesh=mesh,
        in_specs=(field, P(None, None, None, "span", "pitch"), field, P(), P(), P()),
        out_specs=field, check_vma=False,
    )
```

```python
import jax
import jax.numpy as jnp
import numpy as np
from jax import lax
from jax.experimental import pallas as pl
from jax.experimental.pallas import tpu as pltpu
from jax.sharding import PartitionSpec as P

NP = 1024
PITCH = 8
GROUP = 4
LAYERS = 8
V = 5
LINE = 16
MAPS = 80
VECS = 16
LANES = 128

SPREAD, FORWARD, BACK_RE, BACK_IM, GATHER_RE, GATHER_IM, LOW = np.cumsum([0, 160, 256, 128, 128, 128, 128]).tolist()


def table():
    two_pi = 2.0 * np.pi
    a = np.arange(8)
    b = np.arange(128)
    k2 = np.arange(64)
    eight = two_pi * (np.outer(a, a) % 8) / 8
    spread = np.zeros((2, 10, 8, 8, LINE))
    for line in range(10):
        spread[0, line, :, :, line] = np.cos(eight)
        spread[1, line, :, :, line] = -np.sin(eight)
    twiddle = two_pi * np.outer(a, b) / NP
    lanes = two_pi * (np.outer(b, k2) % 128) / 128
    cos, sin = np.cos(lanes), np.sin(lanes)
    forward = np.block([[cos, -sin], [sin, cos]])
    back_re = np.concatenate([cos.T, -sin.T], 0)
    back_im = np.concatenate([sin.T, cos.T], 0)
    gather_re = np.zeros((8, LINE, 16, 8))
    gather_im = np.zeros((8, LINE, 16, 8))
    for line in range(10):
        gather_re[:, line, line, :] = np.cos(eight)
        gather_im[:, line, line, :] = -np.sin(eight)
    parts = [
        spread.reshape(160, 128),
        forward,
        back_re,
        back_im,
        gather_re.reshape(128, 128),
        gather_im.reshape(128, 128),
    ]
    whole = np.concatenate(parts, 0).astype(np.float32)
    high = whole.astype(jnp.bfloat16)
    low = (whole - high.astype(np.float32)).astype(jnp.bfloat16)
    turns = np.concatenate([np.cos(twiddle), np.sin(twiddle)], 0).astype(np.float32)
    return np.concatenate([high, low], 0), turns


def every(start, stride):
    return pl.ds(start, 8, stride=stride)


def rows(start, size):
    return pl.ds(pl.multiple_of(start, 8), size)


def product(later, earlier):
    total = later[0][None] * earlier[:, 0][:, None]
    for j in range(1, V):
        total = total + later[j][None] * earlier[:, j][:, None]
    return total


def apply(matrix, vector):
    total = matrix[0] * vector[0][None]
    for j in range(1, V):
        total = total + matrix[j] * vector[j][None]
    return total


def scaled(block, coupling, which):
    columns = []
    for k in range(V):
        total = block[:, 0] * (-coupling[0, which, k])
        for j in range(1, V):
            total = total + block[:, j] * (-coupling[j, which, k])
        columns.append(total)
    return jnp.stack(columns)


def times(data, const, start, size, left=False):
    data_high = data.astype(jnp.bfloat16)
    data_low = (data - data_high.astype(jnp.float32)).astype(jnp.bfloat16)
    high = const[start : start + size, :]
    low = const[LOW + start : LOW + start + size, :]
    pairs = ((data_high, high), (data_low, high), (data_high, low))
    total = None
    for x, w in pairs:
        part = jnp.dot(w, x, preferred_element_type=jnp.float32) if left else jnp.dot(x, w, preferred_element_type=jnp.float32)
        total = part if total is None else total + part
    return total


def kernel(
    residual_in, inverse_in, prior_in, coupling_in, characteristic_in, cutoffs_in, const_in, turns_in, out,
    residual, inverse, prior, coupling, cutoffs, characteristic, const, turns, load_s,
    lower, upper, edge_low, edge_high, planes_out, planes_in, corr_out, corr_in,
    maps_out, maps_in, layer_maps, vecs_out, vecs_in, layer_vecs, entry_out, entry_in,
    down, up, first, second, third, next_reach, next_both, source, base, flat, spectra,
    pitch_s, pitch_r, back_s, back_r, side_s, side_r,
    gm_s, gm_r, zm_s, zm_r, zt_s, zt_r, gv_s, gv_r, zv_s, zv_r, ge_s, ge_r,
):
    pitch = lax.axis_index("pitch")
    span = lax.axis_index("span")
    layer = span // GROUP
    member = span % GROUP

    def at_pitch(d):
        return {"pitch": lax.rem(pitch + d, PITCH), "span": span}

    def at_member(d):
        return {"pitch": pitch, "span": layer * GROUP + lax.rem(member + d, GROUP)}

    def at_layer(d):
        return {"pitch": pitch, "span": lax.rem(layer + d, LAYERS) * GROUP + member}

    peers = [at_pitch(d) for d in range(1, PITCH)]
    peers += [at_member(d) for d in range(1, GROUP)]
    peers += [at_layer(d) for d in range(1, LAYERS)]
    barrier = pltpu.get_barrier_semaphore()
    for peer in peers:
        pl.semaphore_signal(barrier, inc=1, device_id=peer, device_id_type=pl.DeviceIdType.MESH)

    loads = []
    for n, (src, dst) in enumerate((
        (residual_in, residual), (prior_in, prior), (inverse_in, inverse),
        (characteristic_in, characteristic), (const_in, const), (turns_in, turns),
        (coupling_in, coupling), (cutoffs_in, cutoffs),
    )):
        loads.append(pltpu.make_async_copy(src, dst, load_s.at[n]))
        loads[-1].start()

    def send(src, dst, send_sem, recv_sem, peer):
        copy = pltpu.make_async_remote_copy(
            src_ref=src, dst_ref=dst, send_sem=send_sem, recv_sem=recv_sem,
            device_id=peer, device_id_type=pl.DeviceIdType.MESH,
        )
        copy.start()
        return copy

    planes_out[...] = jnp.zeros_like(planes_out)
    maps_out[...] = jnp.zeros_like(maps_out)
    vecs_out[...] = jnp.zeros_like(vecs_out)
    loads[0].wait()
    for q, axial in enumerate((0, GROUP - 1)):
        for j in range(V):
            planes_out[every(q * V + j, LINE), :] = residual[j, axial * 8 : axial * 8 + 8, :]

    pl.semaphore_wait(barrier, len(peers))

    pitch_copies = []
    for d in range(1, PITCH):
        to = lax.rem(pitch + d, PITCH)
        pitch_copies.append(send(
            planes_out.at[rows(to * LINE, LINE)], planes_in.at[rows(pitch * LINE, LINE)],
            pitch_s.at[d], pitch_r.at[d], at_pitch(d),
        ))
    loads[1].wait()
    column = lax.broadcasted_iota(jnp.int32, (8, LANES), 1)
    last = initial = jnp.zeros((8, LANES), jnp.float32)
    for n in range(V * GROUP):
        tile = prior[n // GROUP, n % GROUP * 8 : n % GROUP * 8 + 8, :]
        last = jnp.where(column == n, pltpu.roll(tile, n + 1, 1), last)
        initial = jnp.where(column == n, pltpu.roll(tile, n, 1) if n else tile, initial)
    edge_high[...] = last
    edge_low[...] = initial
    side_copies = [
        send(edge_high, lower, side_s.at[0], side_r.at[0], at_pitch(1)),
        send(edge_low, upper, side_s.at[1], side_r.at[1], at_pitch(PITCH - 1)),
    ]

    loads[2].wait()
    loads[6].wait()
    reach = None
    for s in range(4):
        block = inverse[:, :, every(s, 4), :]
        down[s] = scaled(block, coupling, 0)
        up[s] = scaled(block, coupling, 1)
        reach = down[s] if s == 0 else product(down[s], reach)
        first[s] = reach
    both = reach
    trail = up[3]
    second[3] = both
    third[3] = trail
    for s in (2, 1, 0):
        both = first[s] + product(up[s], both)
        trail = product(up[s], trail)
        second[s] = both
        third[s] = trail
    upper_reach = pltpu.roll(reach, 7, 2)
    upper_both = pltpu.roll(both, 7, 2)
    next_reach[...] = upper_reach
    next_both[...] = upper_both
    both = both + product(trail, product(upper_both, reach))
    trail = product(trail, pltpu.roll(trail, 7, 2))
    reach = product(upper_reach, reach)
    for k in range(V):
        for i in range(V):
            maps_out[every(8 * k + i, MAPS), :] = reach[k, i]
            maps_out[every(40 + 8 * k + i, MAPS), :] = trail[k, i]
            maps_out[every(8 * k + 5 + i if i < 3 else 40 + 8 * k + 2 + i, MAPS), :] = both[k, i]

    map_copies = []
    for d in range(1, GROUP):
        to = lax.rem(member + d, GROUP)
        map_copies.append(send(
            maps_out.at[rows(to * 2 * MAPS, MAPS)], maps_in.at[rows(member * MAPS, MAPS)],
            gm_s.at[d], gm_r.at[d], at_member(d),
        ))
    planes_in[rows(pitch * LINE, LINE), :] = planes_out[rows(pitch * LINE, LINE), :]
    maps_in[rows(member * MAPS, MAPS), :] = maps_out[rows(member * 2 * MAPS, MAPS), :]

    loads[3].wait()
    flat[100:104, :] = jnp.zeros((4, 512), jnp.float32)
    for n in range(50):
        flat[2 * n : 2 * n + 2, :] = characteristic[n]
    whole = flat[...]
    high = whole.astype(jnp.bfloat16)
    rest = whole - high.astype(jnp.float32)
    middle = rest.astype(jnp.bfloat16)
    low = (rest - middle.astype(jnp.float32)).astype(jnp.bfloat16)
    harmonic = lax.broadcasted_iota(jnp.int32, (512, LANES), 0)
    lane = lax.broadcasted_iota(jnp.int32, (512, LANES), 1)
    apart = harmonic - 8 * (lane % 64)
    for k1 in range(8):
        pick = jnp.where(apart == k1, 1.0, 0.0).astype(jnp.bfloat16)
        part = jnp.dot(high, pick, preferred_element_type=jnp.float32)
        part = part + jnp.dot(middle, pick, preferred_element_type=jnp.float32)
        part = part + jnp.dot(low, pick, preferred_element_type=jnp.float32)
        spectra[pl.ds(k1, 104, stride=8), :] = part

    for copy in pitch_copies:
        copy.wait_recv()
    for load in (loads[4], loads[5], loads[7]):
        load.wait()
    spread = times(planes_in[...], const, SPREAD, 160, True).reshape(2, 10, 8, LANES)
    turn_re = turns[0:8, :][None]
    turn_im = turns[8:16, :][None]
    turned_re = (spread[0] * turn_re + spread[1] * turn_im).reshape(80, LANES)
    turned_im = (spread[1] * turn_re - spread[0] * turn_im).reshape(80, LANES)
    spectrum = times(jnp.concatenate([turned_re, turned_im], 1), const, FORWARD, 256)
    number = lax.broadcasted_iota(jnp.int32, (8, LANES), 0) + 8 * (lax.broadcasted_iota(jnp.int32, (8, LANES), 1) % 64)
    weight = jnp.where(number == 0, 1.0, 2.0) / NP
    sign = jnp.where(lax.broadcasted_iota(jnp.int32, (80, LANES), 1) < 64, -1.0, 1.0)
    crossed = (pltpu.roll(spectrum, 64, 1) * sign).reshape(2, V, 8, LANES)
    spectrum = spectrum.reshape(2, V, 8, LANES)
    corrected = []
    for q in range(2):
        factor = jnp.where(number < cutoffs[q], weight, 0.0)
        for i in range(V):
            total = None
            for j in range(V):
                row = (q * 25 + i * V + j) * 16
                term = spectra[row : row + 8, :] * spectrum[q, j] + spectra[row + 8 : row + 16, :] * crossed[q, j]
                total = term if total is None else total + term
            corrected.append(total * factor)
    corrected = jnp.concatenate(corrected, 0)
    back_re = times(corrected, const, BACK_RE, 128).reshape(10, 8, LANES)
    back_im = times(corrected, const, BACK_IM, 128).reshape(10, 8, LANES)
    filler = jnp.zeros((48, LANES), jnp.float32)
    lines_re = jnp.concatenate([(back_re * turn_re - back_im * turn_im).reshape(80, LANES), filler], 0)
    lines_im = jnp.concatenate([(back_im * turn_re + back_re * turn_im).reshape(80, LANES), filler], 0)
    corr_out[...] = times(lines_re, const, GATHER_RE, 128, True) + times(lines_im, const, GATHER_IM, 128, True)
    back_copies = []
    for d in range(1, PITCH):
        to = lax.rem(pitch + d, PITCH)
        back_copies.append(send(
            corr_out.at[rows(to * LINE, LINE)], corr_in.at[rows(pitch * LINE, LINE)],
            back_s.at[d], back_r.at[d], at_pitch(d),
        ))
    corr_in[rows(pitch * LINE, LINE), :] = corr_out[rows(pitch * LINE, LINE), :]

    place = lax.broadcasted_iota(jnp.int32, (8, LANES), 0)

    def tiles(ref, n, second_half):
        start = n * MAPS + (40 if second_half else 0)
        return [ref[start + 8 * j : start + 8 * j + 8, :] for j in range(V)]

    def spread_rows(vector):
        return [jnp.broadcast_to(vector[..., j : j + 1, :], vector.shape) for j in range(V)]

    def mix(matrix, parts):
        total = matrix[0] * parts[0]
        for j in range(1, V):
            total = total + matrix[j] * parts[j]
        return total

    def moved(top, bottom):
        axis = top.ndim - 2
        return jnp.where(place < 3, pltpu.roll(top, 3, axis), pltpu.roll(bottom, 6, axis))

    for copy in map_copies:
        copy.wait_recv()
    top = maps_in[0:40, :].reshape(V, 8, LANES)
    bottom = maps_in[40:80, :].reshape(V, 8, LANES)
    across = [moved(top, bottom)]
    forward = top
    for n in range(1, GROUP):
        parts = spread_rows(forward)
        forward = mix(tiles(maps_in, n, False), parts)
        across.append(moved(forward, mix(tiles(maps_in, n, True), parts)))
    backward = jnp.concatenate([maps_in[3 * MAPS + 40 : 4 * MAPS, :].reshape(V, 8, LANES), across[3]], 0)
    for n in range(GROUP - 2, -1, -1):
        backward = mix(tiles(maps_in, n, True), spread_rows(backward))
        backward = jnp.concatenate([backward[:V], backward[V:] + across[n]], 0)
    mine = pl.multiple_of(layer * MAPS, 8)
    whole_top = jnp.where(place < V, forward, pltpu.roll(backward[V:], 5, 1))
    whole_bottom = jnp.where(place < V, backward[:V], pltpu.roll(backward[V:], 2, 1))
    layer_maps[pl.ds(mine, 40), :] = whole_top.reshape(40, LANES)
    layer_maps[pl.ds(pl.multiple_of(layer * MAPS + 40, 8), 40), :] = whole_bottom.reshape(40, LANES)
    layer_copies, lower_copies = [], []
    for d in range(1, LAYERS):
        layer_copies.append(send(
            layer_maps.at[rows(layer * MAPS, 40)], layer_maps.at[rows(layer * MAPS, 40)],
            zm_s.at[d], zm_r.at[d], at_layer(d),
        ))
        copy = pltpu.make_async_remote_copy(
            src_ref=layer_maps.at[rows(layer * MAPS + 40, 40)], dst_ref=layer_maps.at[rows(layer * MAPS + 40, 40)],
            send_sem=zt_s.at[d], recv_sem=zt_r.at[d],
            device_id=at_layer(d), device_id_type=pl.DeviceIdType.MESH,
        )
        lower_copies.append((copy, layer + d >= LAYERS, layer < d))
        pl.when(layer + d >= LAYERS)(copy.start)

    for copy in side_copies:
        copy.wait_recv()
    own = prior[...]
    below, above = [], []
    for i in range(V):
        low_tiles, high_tiles = [], []
        for a in range(GROUP):
            n = i * GROUP + a
            tile = prior[i, a * 8 : a * 8 + 8, :]
            edge = pltpu.roll(lower[...], LANES - n, 1) if n else lower[...]
            low_tiles.append(jnp.where(column == 0, edge, pltpu.roll(tile, 1, 1)))
            edge = pltpu.roll(upper[...], LANES - 1 - n, 1)
            high_tiles.append(jnp.where(column == LANES - 1, edge, pltpu.roll(tile, LANES - 1, 1)))
        below.append(jnp.concatenate(low_tiles, 0))
        above.append(jnp.concatenate(high_tiles, 0))
    zero_row = jnp.zeros((8, LANES), jnp.float32)
    for i in range(V):
        total = residual[i]
        before = after = None
        for j in range(V):
            total = total - coupling[i, 2, j] * below[j] - coupling[i, 3, j] * above[j]
            low_term = coupling[i, 4, j] * own[j]
            high_term = coupling[i, 5, j] * own[j]
            before = low_term if before is None else before + low_term
            after = high_term if after is None else after + high_term
        total = total - jnp.concatenate([zero_row, before[:24]], 0) - jnp.concatenate([after[8:], zero_row], 0)
        source[i] = total

    for copy in back_copies:
        copy.wait_recv()
    for j in range(V):
        source[j, 0:8, :] = source[j, 0:8, :] + corr_in[every(j, LINE), :]
        source[j, 24:32, :] = source[j, 24:32, :] + corr_in[every(V + j, LINE), :]
    star = None
    for s in range(4):
        block = inverse[:, :, every(s, 4), :]
        rhs = source[:, every(s, 4), :]
        value = block[:, 0] * rhs[0][None]
        for j in range(1, V):
            value = value + block[:, j] * rhs[j][None]
        star = value if s == 0 else value + apply(down[s], star)
        base[s] = star
    update = star
    for s in (2, 1, 0):
        update = base[s] + apply(up[s], update)
        base[s] = update
    ahead = pltpu.roll(star, 7, 1) + apply(next_reach, star)
    behind = update + apply(third[0], pltpu.roll(update, 7, 1) + apply(next_both, star))
    for i in range(V):
        vecs_out[every(i, VECS), :] = ahead[i]
        vecs_out[every(8 + i, VECS), :] = behind[i]
    vec_copies = []
    for d in range(1, GROUP):
        to = lax.rem(member + d, GROUP)
        vec_copies.append(send(
            vecs_out.at[rows(to * 2 * VECS, VECS)], vecs_in.at[rows(member * VECS, VECS)],
            gv_s.at[d], gv_r.at[d], at_member(d),
        ))
    vecs_in[rows(member * VECS, VECS), :] = vecs_out[rows(member * 2 * VECS, VECS), :]

    def chain(count, maps_ref, vecs_ref, x, y):
        entering_x, entering_y, crossing = [], [None] * count, []
        for n in range(count):
            entering_x.append(x)
            offset = vecs_ref[n * VECS : n * VECS + 8, :]
            if x is None:
                crossing.append(vecs_ref[n * VECS + 8 : n * VECS + 16, :])
                x = offset
            else:
                parts = spread_rows(x)
                ahead = mix(tiles(maps_ref, n, False), parts)
                aside = mix(tiles(maps_ref, n, True), parts)
                crossing.append(moved(ahead, aside) + vecs_ref[n * VECS + 8 : n * VECS + 16, :])
                x = ahead + offset
        for n in range(count - 1, -1, -1):
            entering_y[n] = y
            y = crossing[n] if y is None else mix(tiles(maps_ref, n, True), spread_rows(y)) + crossing[n]
        return entering_x, entering_y, x, y

    for copy in vec_copies:
        copy.wait_recv()
    _, _, x, y = chain(GROUP, maps_in, vecs_in, None, None)
    layer_vecs[pl.ds(pl.multiple_of(layer * VECS, 8), 8), :] = x
    layer_vecs[pl.ds(pl.multiple_of(layer * VECS + 8, 8), 8), :] = y
    vec_layer_copies = []
    for d in range(1, LAYERS):
        vec_layer_copies.append(send(
            layer_vecs.at[rows(layer * VECS, VECS)], layer_vecs.at[rows(layer * VECS, VECS)],
            zv_s.at[d], zv_r.at[d], at_layer(d),
        ))
    for copy in layer_copies:
        copy.wait_recv()
    for copy, _, comes in lower_copies:
        pl.when(comes)(copy.wait_recv)
    for copy in vec_layer_copies:
        copy.wait_recv()
    entering_x, entering_y, _, _ = chain(LAYERS, layer_maps, layer_vecs, None, None)
    x = jnp.zeros((8, LANES), jnp.float32)
    y = jnp.zeros((8, LANES), jnp.float32)
    for n in range(8):
        if entering_x[n] is not None:
            x = jnp.where(layer == n, entering_x[n], x)
        if entering_y[n] is not None:
            y = jnp.where(layer == n, entering_y[n], y)
    entering_x, entering_y, _, _ = chain(GROUP, maps_in, vecs_in, x, y)
    for n in range(8):
        entry_out[n * VECS : n * VECS + 8, :] = entering_x[n // 2]
        entry_out[n * VECS + 8 : n * VECS + 16, :] = entering_y[n // 2]
    entry_copies = []
    for d in range(1, GROUP):
        to = lax.rem(member + d, GROUP)
        entry_copies.append(send(
            entry_out.at[rows(to * 2 * VECS, 2 * VECS)], entry_in.at[rows(member * 2 * VECS, 2 * VECS)],
            ge_s.at[d], ge_r.at[d], at_member(d),
        ))
    entry_in[rows(member * 2 * VECS, 2 * VECS), :] = entry_out[rows(member * 2 * VECS, 2 * VECS), :]
    for copy in entry_copies:
        copy.wait_recv()
    x = jnp.stack([entry_in[every(i, VECS), :] for i in range(V)])
    y = jnp.stack([entry_in[every(8 + i, VECS), :] for i in range(V)])
    odd = place % 2 == 1
    x = jnp.where(odd, pltpu.roll(apply(first[3], x) + base[3], 1, 1), x)
    y = jnp.where(odd, y, pltpu.roll(apply(third[0], y) + apply(second[0], x) + base[0], 7, 1))
    for s in range(4):
        value = base[s]
        for j in range(V):
            value = value + second[s, j] * x[j][None] + third[s, j] * y[j][None]
        for i in range(V):
            out[i, every(s, 4), :] = value[i]

    for copy in pitch_copies + side_copies + map_copies + back_copies + layer_copies:
        copy.wait_send()
    for copy in vec_copies + vec_layer_copies + entry_copies:
        copy.wait_send()
    for copy, goes, _ in lower_copies:
        pl.when(goes)(copy.wait_send)


def body(residual, inverse_diagonal, prior_increment, coupling, characteristic, cutoffs):
    f32 = jnp.float32
    fields = (V, 32, LANES)
    matrices = pltpu.VMEM((4, V, V, 8, LANES), f32)

    def vmem(count):
        return pltpu.VMEM((count, LANES), f32)

    def sems(count):
        return [pltpu.SemaphoreType.DMA((count,))] * 2

    scratch = [
        pltpu.VMEM(fields, f32), pltpu.VMEM((V, V, 32, LANES), f32), pltpu.VMEM(fields, f32),
        pltpu.SMEM((V, 6, V), f32), pltpu.SMEM((2,), jnp.int32),
        pltpu.VMEM((50, 2, 512), f32), pltpu.VMEM((2 * LOW, LANES), jnp.bfloat16), vmem(16),
        pltpu.SemaphoreType.DMA((8,)),
        vmem(8), vmem(8), vmem(8), vmem(8),
        vmem(128), vmem(128), vmem(128), vmem(128),
        vmem(8 * MAPS), vmem(8 * MAPS), vmem(8 * MAPS),
        vmem(8 * VECS), vmem(8 * VECS), vmem(8 * VECS), vmem(8 * VECS), vmem(8 * VECS),
        matrices, matrices, matrices, matrices, matrices,
        pltpu.VMEM((V, V, 8, LANES), f32), pltpu.VMEM((V, V, 8, LANES), f32),
        pltpu.VMEM(fields, f32), pltpu.VMEM((4, V, 8, LANES), f32),
        pltpu.VMEM((104, 512), f32), vmem(104 * 8),
        *sems(PITCH), *sems(PITCH), *sems(2),
        *sems(GROUP), *sems(LAYERS), *sems(LAYERS), *sems(GROUP), *sems(LAYERS), *sems(GROUP),
    ]
    inside = pl.BlockSpec(memory_space=pltpu.VMEM)
    outside = pl.BlockSpec(memory_space=pl.ANY)
    high_low, turns = table()
    result = pl.pallas_call(
        kernel,
        out_shape=pltpu.VMEM(fields, f32),
        in_specs=[outside] * 8,
        out_specs=inside,
        scratch_shapes=scratch,
        compiler_params=pltpu.CompilerParams(collective_id=0, has_side_effects=True),
    )(
        residual.reshape(fields),
        inverse_diagonal.reshape(V, V, 32, LANES),
        prior_increment.reshape(fields),
        coupling.transpose(1, 0, 2),
        characteristic.transpose(0, 3, 4, 1, 2).reshape(50, 2, 512),
        cutoffs,
        jnp.asarray(high_low),
        jnp.asarray(turns),
    )
    return result.reshape(V, GROUP, 8, LANES)


def solution(mesh):
    field = P(None, None, "span", "pitch")
    return jax.shard_map(
        body, mesh=mesh,
        in_specs=(field, P(None, None, None, "span", "pitch"), field, P(), P(), P()),
        out_specs=field, check_vma=False,
    )
```

```python
import jax
import jax.numpy as jnp
import numpy as np
from jax import lax
from jax.experimental import pallas as pl
from jax.experimental.pallas import tpu as pltpu
from jax.sharding import PartitionSpec as P

NP = 1024
PITCH = 8
GROUP = 4
LAYERS = 8
V = 5
LINE = 16
MAPS = 80
A, B, C, USED = 0, 25, 50, 75
VECS = 16
SENT = 10
LANES = 128

SPREAD, FORWARD, BACK_RE, BACK_IM, GATHER_RE, GATHER_IM, LOW = np.cumsum([0, 160, 256, 128, 128, 128, 128]).tolist()


def table():
    two_pi = 2.0 * np.pi
    a = np.arange(8)
    b = np.arange(128)
    k2 = np.arange(64)
    eight = two_pi * (np.outer(a, a) % 8) / 8
    spread = np.zeros((2, 10, 8, 8, LINE))
    for line in range(10):
        spread[0, line, :, :, line] = np.cos(eight)
        spread[1, line, :, :, line] = -np.sin(eight)
    twiddle = two_pi * np.outer(a, b) / NP
    lanes = two_pi * (np.outer(b, k2) % 128) / 128
    cos, sin = np.cos(lanes), np.sin(lanes)
    forward = np.block([[cos, -sin], [sin, cos]])
    back_re = np.concatenate([cos.T, -sin.T], 0)
    back_im = np.concatenate([sin.T, cos.T], 0)
    gather_re = np.zeros((8, LINE, 16, 8))
    gather_im = np.zeros((8, LINE, 16, 8))
    for line in range(10):
        gather_re[:, line, line, :] = np.cos(eight)
        gather_im[:, line, line, :] = -np.sin(eight)
    parts = [
        spread.reshape(160, 128),
        forward,
        back_re,
        back_im,
        gather_re.reshape(128, 128),
        gather_im.reshape(128, 128),
    ]
    whole = np.concatenate(parts, 0).astype(np.float32)
    high = whole.astype(jnp.bfloat16)
    low = (whole - high.astype(np.float32)).astype(jnp.bfloat16)
    turns = np.concatenate([np.cos(twiddle), np.sin(twiddle)], 0).astype(np.float32)
    return np.concatenate([high, low], 0), turns


FAR_FIRST = (4, 3, 5, 2, 6, 1, 7)
MEMBERS = (2, 1, 3)


def every(start, stride):
    return pl.ds(start, 8, stride=stride)


def rows(start, size):
    return pl.ds(pl.multiple_of(start, 8), size)


def product(later, earlier):
    total = later[0][None] * earlier[:, 0][:, None]
    for j in range(1, V):
        total = total + later[j][None] * earlier[:, j][:, None]
    return total


def apply(matrix, vector):
    total = matrix[0] * vector[0][None]
    for j in range(1, V):
        total = total + matrix[j] * vector[j][None]
    return total


def scaled(block, coupling, which):
    columns = []
    for k in range(V):
        total = block[:, 0] * (-coupling[0, which, k])
        for j in range(1, V):
            total = total + block[:, j] * (-coupling[j, which, k])
        columns.append(total)
    return jnp.stack(columns)


def times(data, const, start, size, left=False):
    data_high = data.astype(jnp.bfloat16)
    data_low = (data - data_high.astype(jnp.float32)).astype(jnp.bfloat16)
    high = const[start : start + size, :]
    low = const[LOW + start : LOW + start + size, :]
    pairs = ((data_high, high), (data_low, high), (data_high, low))
    total = None
    for x, w in pairs:
        part = jnp.dot(w, x, preferred_element_type=jnp.float32) if left else jnp.dot(x, w, preferred_element_type=jnp.float32)
        total = part if total is None else total + part
    return total


def kernel(
    residual_in, inverse_in, prior_in, coupling_in, characteristic_in, cutoffs_in, const_in, turns_in, out,
    residual, inverse, prior, coupling, cutoffs, characteristic, const, turns, load_s,
    lower, upper, edge_low, edge_high, planes_out, planes_in, corr_out, corr_in,
    maps_out, maps_in, packed, layer_maps, vecs_out, vecs_in, layer_vecs, entry_out, entry_in,
    down, up, first, second, third, next_reach, next_both, source, base, flat, spectra,
    pitch_s, pitch_r, back_s, back_r, side_s, side_r,
    gm_s, gm_r, gv_s, gv_r, zv_s, zv_r, ge_s, ge_r, zt_s, zt_r,
):
    pitch = lax.axis_index("pitch")
    span = lax.axis_index("span")
    layer = span // GROUP
    member = span % GROUP

    def at_pitch(d):
        return {"pitch": lax.rem(pitch + d, PITCH), "span": span}

    def at_member(d):
        return {"pitch": pitch, "span": layer * GROUP + lax.rem(member + d, GROUP)}

    def at_layer(d):
        return {"pitch": pitch, "span": lax.rem(layer + d, LAYERS) * GROUP + member}

    peers = [at_pitch(d) for d in range(1, PITCH)]
    peers += [at_member(d) for d in range(1, GROUP)]
    peers += [at_layer(d) for d in range(1, LAYERS)]
    for area in (planes_in, maps_in, layer_maps, vecs_in, layer_vecs, entry_in):
        area[...] = jnp.zeros_like(area)
    barrier = pltpu.get_barrier_semaphore()
    for peer in peers:
        pl.semaphore_signal(barrier, inc=1, device_id=peer, device_id_type=pl.DeviceIdType.MESH)

    loads = []
    for n, (src, dst) in enumerate((
        (residual_in, residual), (prior_in, prior), (inverse_in, inverse),
        (characteristic_in, characteristic), (const_in, const), (turns_in, turns),
        (coupling_in, coupling), (cutoffs_in, cutoffs),
    )):
        loads.append(pltpu.make_async_copy(src, dst, load_s.at[n]))
        loads[-1].start()

    def send(src, dst, send_sem, recv_sem, peer):
        copy = pltpu.make_async_remote_copy(
            src_ref=src, dst_ref=dst, send_sem=send_sem, recv_sem=recv_sem,
            device_id=peer, device_id_type=pl.DeviceIdType.MESH,
        )
        copy.start()

    def finish(sem, count):
        area = maps_out.at[pl.ds(0, count)]
        pltpu.make_async_copy(area, area, sem).wait()

    planes_out[...] = jnp.zeros_like(planes_out)
    maps_out[...] = jnp.zeros_like(maps_out)
    vecs_out[...] = jnp.zeros_like(vecs_out)
    loads[0].wait()
    for q, axial in enumerate((0, GROUP - 1)):
        for j in range(V):
            planes_out[every(q * V + j, LINE), :] = residual[j, axial * 8 : axial * 8 + 8, :]

    pl.semaphore_wait(barrier, len(peers))

    for d in FAR_FIRST:
        to = lax.rem(pitch + d, PITCH)
        send(
            planes_out.at[rows(to * LINE, SENT)], planes_in.at[rows(pitch * LINE, SENT)],
            pitch_s, pitch_r, at_pitch(d),
        )
    loads[1].wait()
    column = lax.broadcasted_iota(jnp.int32, (8, LANES), 1)
    last = initial = jnp.zeros((8, LANES), jnp.float32)
    for n in range(V * GROUP):
        tile = prior[n // GROUP, n % GROUP * 8 : n % GROUP * 8 + 8, :]
        last = jnp.where(column == n, pltpu.roll(tile, n + 1, 1), last)
        initial = jnp.where(column == n, pltpu.roll(tile, n, 1) if n else tile, initial)
    edge_high[...] = last
    edge_low[...] = initial
    send(edge_high, lower, side_s, side_r, at_pitch(1))
    send(edge_low, upper, side_s, side_r, at_pitch(PITCH - 1))

    loads[2].wait()
    loads[6].wait()
    reach = None
    for s in range(4):
        block = inverse[:, :, every(s, 4), :]
        down[s] = scaled(block, coupling, 0)
        up[s] = scaled(block, coupling, 1)
        reach = down[s] if s == 0 else product(down[s], reach)
        first[s] = reach
    both = reach
    trail = up[3]
    second[3] = both
    third[3] = trail
    for s in (2, 1, 0):
        both = first[s] + product(up[s], both)
        trail = product(up[s], trail)
        second[s] = both
        third[s] = trail
    upper_reach = pltpu.roll(reach, 7, 2)
    upper_both = pltpu.roll(both, 7, 2)
    next_reach[...] = upper_reach
    next_both[...] = upper_both
    both = both + product(trail, product(upper_both, reach))
    trail = product(trail, pltpu.roll(trail, 7, 2))
    reach = product(upper_reach, reach)
    for k in range(V):
        for i in range(V):
            maps_out[every(A + V * k + i, MAPS), :] = reach[k, i]
            maps_out[every(B + V * k + i, MAPS), :] = trail[k, i]
            maps_out[every(C + V * k + i, MAPS), :] = both[k, i]

    for d in MEMBERS:
        to = lax.rem(member + d, GROUP)
        send(
            maps_out.at[rows(to * 2 * MAPS, USED)], maps_in.at[rows(member * MAPS, USED)],
            gm_s, gm_r, at_member(d),
        )
    planes_in[rows(pitch * LINE, LINE), :] = planes_out[rows(pitch * LINE, LINE), :]
    maps_in[rows(member * MAPS, MAPS), :] = maps_out[rows(member * 2 * MAPS, MAPS), :]

    loads[3].wait()
    flat[100:104, :] = jnp.zeros((4, 512), jnp.float32)
    for n in range(50):
        flat[2 * n : 2 * n + 2, :] = characteristic[n]
    whole = flat[...]
    high = whole.astype(jnp.bfloat16)
    rest = whole - high.astype(jnp.float32)
    middle = rest.astype(jnp.bfloat16)
    low = (rest - middle.astype(jnp.float32)).astype(jnp.bfloat16)
    harmonic = lax.broadcasted_iota(jnp.int32, (512, LANES), 0)
    lane = lax.broadcasted_iota(jnp.int32, (512, LANES), 1)
    apart = harmonic - 8 * (lane % 64)
    for k1 in range(8):
        pick = jnp.where(apart == k1, 1.0, 0.0).astype(jnp.bfloat16)
        part = jnp.dot(high, pick, preferred_element_type=jnp.float32)
        part = part + jnp.dot(middle, pick, preferred_element_type=jnp.float32)
        part = part + jnp.dot(low, pick, preferred_element_type=jnp.float32)
        spectra[pl.ds(k1, 104, stride=8), :] = part

    finish(pitch_r, (PITCH - 1) * SENT)
    for load in (loads[4], loads[5], loads[7]):
        load.wait()
    spread = times(planes_in[...], const, SPREAD, 160, True).reshape(2, 10, 8, LANES)
    turn_re = turns[0:8, :][None]
    turn_im = turns[8:16, :][None]
    turned_re = (spread[0] * turn_re + spread[1] * turn_im).reshape(80, LANES)
    turned_im = (spread[1] * turn_re - spread[0] * turn_im).reshape(80, LANES)
    spectrum = times(jnp.concatenate([turned_re, turned_im], 1), const, FORWARD, 256)
    number = lax.broadcasted_iota(jnp.int32, (8, LANES), 0) + 8 * (lax.broadcasted_iota(jnp.int32, (8, LANES), 1) % 64)
    weight = jnp.where(number == 0, 1.0, 2.0) / NP
    sign = jnp.where(lax.broadcasted_iota(jnp.int32, (80, LANES), 1) < 64, -1.0, 1.0)
    crossed = (pltpu.roll(spectrum, 64, 1) * sign).reshape(2, V, 8, LANES)
    spectrum = spectrum.reshape(2, V, 8, LANES)
    corrected = []
    for q in range(2):
        factor = jnp.where(number < cutoffs[q], weight, 0.0)
        for i in range(V):
            total = None
            for j in range(V):
                row = (q * 25 + i * V + j) * 16
                term = spectra[row : row + 8, :] * spectrum[q, j] + spectra[row + 8 : row + 16, :] * crossed[q, j]
                total = term if total is None else total + term
            corrected.append(total * factor)
    corrected = jnp.concatenate(corrected, 0)
    back_re = times(corrected, const, BACK_RE, 128).reshape(10, 8, LANES)
    back_im = times(corrected, const, BACK_IM, 128).reshape(10, 8, LANES)
    filler = jnp.zeros((48, LANES), jnp.float32)
    lines_re = jnp.concatenate([(back_re * turn_re - back_im * turn_im).reshape(80, LANES), filler], 0)
    lines_im = jnp.concatenate([(back_im * turn_re + back_re * turn_im).reshape(80, LANES), filler], 0)
    corr_out[...] = times(lines_re, const, GATHER_RE, 128, True) + times(lines_im, const, GATHER_IM, 128, True)
    for d in FAR_FIRST:
        to = lax.rem(pitch + d, PITCH)
        send(
            corr_out.at[rows(to * LINE, SENT)], corr_in.at[rows(pitch * LINE, SENT)],
            back_s, back_r, at_pitch(d),
        )
    corr_in[rows(pitch * LINE, LINE), :] = corr_out[rows(pitch * LINE, LINE), :]

    place = lax.broadcasted_iota(jnp.int32, (8, LANES), 0)

    def tiles(ref, n, which):
        start = n * MAPS + which
        return [ref[start + V * j : start + V * j + 8, :] for j in range(V)]

    def spread_rows(vector):
        return [jnp.broadcast_to(vector[..., j : j + 1, :], vector.shape) for j in range(V)]

    def mix(matrix, parts):
        total = matrix[0] * parts[0]
        for j in range(1, V):
            total = total + matrix[j] * parts[j]
        return total

    finish(gm_r, (GROUP - 1) * USED)
    forward = jnp.stack(tiles(maps_in, 0, A))
    across = [jnp.stack(tiles(maps_in, 0, C))]
    for n in range(1, GROUP):
        parts = spread_rows(forward)
        forward = mix(tiles(maps_in, n, A), parts)
        across.append(mix(tiles(maps_in, n, C), parts))
    backward = jnp.concatenate([jnp.stack(tiles(maps_in, GROUP - 1, B)), across[GROUP - 1]], 0)
    for n in range(GROUP - 2, -1, -1):
        backward = mix(tiles(maps_in, n, B), spread_rows(backward))
        backward = jnp.concatenate([backward[:V], backward[V:] + across[n]], 0)
    columns = jnp.concatenate([forward, backward], 0)
    for n in range(3 * V):
        packed[V * n : V * n + 8, :] = columns[n]
    layer_maps[rows(layer * MAPS, MAPS), :] = packed[0:MAPS, :]
    lower_copies = []
    for d in FAR_FIRST:
        wraps = layer + d >= LAYERS
        pieces = []
        for size, n in ((USED, d - 1), (B, LAYERS - 2 + d)):
            pieces.append(pltpu.make_async_remote_copy(
                src_ref=layer_maps.at[rows(layer * MAPS, size)], dst_ref=layer_maps.at[rows(layer * MAPS, size)],
                send_sem=zt_s.at[n], recv_sem=zt_r.at[n],
                device_id=at_layer(d), device_id_type=pl.DeviceIdType.MESH,
            ))
        lower_copies.append((pieces, wraps, layer < d))
        pl.when(wraps)(pieces[0].start)
        pl.when(jnp.logical_not(wraps))(pieces[1].start)

    finish(side_r, 16)
    own = prior[...]
    below, above = [], []
    for i in range(V):
        low_tiles, high_tiles = [], []
        for a in range(GROUP):
            n = i * GROUP + a
            tile = prior[i, a * 8 : a * 8 + 8, :]
            edge = pltpu.roll(lower[...], LANES - n, 1) if n else lower[...]
            low_tiles.append(jnp.where(column == 0, edge, pltpu.roll(tile, 1, 1)))
            edge = pltpu.roll(upper[...], LANES - 1 - n, 1)
            high_tiles.append(jnp.where(column == LANES - 1, edge, pltpu.roll(tile, LANES - 1, 1)))
        below.append(jnp.concatenate(low_tiles, 0))
        above.append(jnp.concatenate(high_tiles, 0))
    zero_row = jnp.zeros((8, LANES), jnp.float32)
    for i in range(V):
        total = residual[i]
        before = after = None
        for j in range(V):
            total = total - coupling[i, 2, j] * below[j] - coupling[i, 3, j] * above[j]
            low_term = coupling[i, 4, j] * own[j]
            high_term = coupling[i, 5, j] * own[j]
            before = low_term if before is None else before + low_term
            after = high_term if after is None else after + high_term
        total = total - jnp.concatenate([zero_row, before[:24]], 0) - jnp.concatenate([after[8:], zero_row], 0)
        source[i] = total

    finish(back_r, (PITCH - 1) * SENT)
    for j in range(V):
        source[j, 0:8, :] = source[j, 0:8, :] + corr_in[every(j, LINE), :]
        source[j, 24:32, :] = source[j, 24:32, :] + corr_in[every(V + j, LINE), :]
    star = None
    for s in range(4):
        block = inverse[:, :, every(s, 4), :]
        rhs = source[:, every(s, 4), :]
        value = block[:, 0] * rhs[0][None]
        for j in range(1, V):
            value = value + block[:, j] * rhs[j][None]
        star = value if s == 0 else value + apply(down[s], star)
        base[s] = star
    update = star
    for s in (2, 1, 0):
        update = base[s] + apply(up[s], update)
        base[s] = update
    ahead = pltpu.roll(star, 7, 1) + apply(next_reach, star)
    behind = update + apply(third[0], pltpu.roll(update, 7, 1) + apply(next_both, star))
    for i in range(V):
        vecs_out[every(i, VECS), :] = ahead[i]
        vecs_out[every(V + i, VECS), :] = behind[i]
    for d in MEMBERS:
        to = lax.rem(member + d, GROUP)
        send(
            vecs_out.at[rows(to * 2 * VECS, SENT)], vecs_in.at[rows(member * VECS, SENT)],
            gv_s, gv_r, at_member(d),
        )
    vecs_in[rows(member * VECS, VECS), :] = vecs_out[rows(member * 2 * VECS, VECS), :]

    def chain(count, maps_ref, vecs_ref, x, y):
        entering_x, entering_y, crossing = [], [None] * count, []
        for n in range(count):
            entering_x.append(x)
            offset = vecs_ref[n * VECS : n * VECS + 8, :]
            if x is None:
                crossing.append(vecs_ref[n * VECS + V : n * VECS + V + 8, :])
                x = offset
            else:
                parts = spread_rows(x)
                ahead = mix(tiles(maps_ref, n, A), parts)
                crossing.append(mix(tiles(maps_ref, n, C), parts) + vecs_ref[n * VECS + V : n * VECS + V + 8, :])
                x = ahead + offset
        for n in range(count - 1, -1, -1):
            entering_y[n] = y
            y = crossing[n] if y is None else mix(tiles(maps_ref, n, B), spread_rows(y)) + crossing[n]
        return entering_x, entering_y, x, y

    finish(gv_r, (GROUP - 1) * SENT)
    _, _, x, y = chain(GROUP, maps_in, vecs_in, None, None)
    tail = pltpu.roll(y, V, 0)
    layer_vecs[rows(layer * VECS, 8), :] = jnp.where(place < V, x, tail)
    layer_vecs[rows(layer * VECS + 8, 8), :] = tail
    for d in FAR_FIRST:
        send(
            layer_vecs.at[rows(layer * VECS, SENT)], layer_vecs.at[rows(layer * VECS, SENT)],
            zv_s, zv_r, at_layer(d),
        )
    for pieces, _, from_above in lower_copies:
        pl.when(from_above)(pieces[0].wait_recv)
        pl.when(jnp.logical_not(from_above))(pieces[1].wait_recv)
    finish(zv_r, (LAYERS - 1) * SENT)
    entering_x, entering_y, _, _ = chain(LAYERS, layer_maps, layer_vecs, None, None)
    x = jnp.zeros((8, LANES), jnp.float32)
    y = jnp.zeros((8, LANES), jnp.float32)
    for n in range(8):
        if entering_x[n] is not None:
            x = jnp.where(layer == n, entering_x[n], x)
        if entering_y[n] is not None:
            y = jnp.where(layer == n, entering_y[n], y)
    entering_x, entering_y, _, _ = chain(GROUP, maps_in, vecs_in, x, y)
    for n in range(GROUP):
        tail = pltpu.roll(entering_y[n], V, 0)
        entry_out[n * VECS : n * VECS + 8, :] = jnp.where(place < V, entering_x[n], tail)
        entry_out[n * VECS + 8 : n * VECS + 16, :] = tail
    for d in MEMBERS:
        to = lax.rem(member + d, GROUP)
        send(
            entry_out.at[rows(to * VECS, SENT)], entry_in.at[rows(member * 2 * VECS, SENT)],
            ge_s, ge_r, at_member(d),
        )
    entry_in[rows(member * 2 * VECS, VECS), :] = entry_out[rows(member * VECS, VECS), :]
    finish(ge_r, (GROUP - 1) * SENT)
    x = jnp.stack([entry_in[every(i, VECS), :] for i in range(V)])
    y = jnp.stack([entry_in[every(V + i, VECS), :] for i in range(V)])
    odd = place % 2 == 1
    x = jnp.where(odd, pltpu.roll(apply(first[3], x) + base[3], 1, 1), x)
    y = jnp.where(odd, pltpu.roll(y, 1, 1), y)
    y = jnp.where(odd, y, pltpu.roll(apply(third[0], y) + apply(second[0], x) + base[0], 7, 1))
    for s in range(4):
        value = base[s]
        for j in range(V):
            value = value + second[s, j] * x[j][None] + third[s, j] * y[j][None]
        for i in range(V):
            out[i, every(s, 4), :] = value[i]

    finish(pitch_s, (PITCH - 1) * SENT)
    finish(side_s, 16)
    finish(gm_s, (GROUP - 1) * USED)
    finish(back_s, (PITCH - 1) * SENT)
    finish(gv_s, (GROUP - 1) * SENT)
    finish(zv_s, (LAYERS - 1) * SENT)
    finish(ge_s, (GROUP - 1) * SENT)
    for pieces, wraps, _ in lower_copies:
        pl.when(wraps)(pieces[0].wait_send)
        pl.when(jnp.logical_not(wraps))(pieces[1].wait_send)


def body(residual, inverse_diagonal, prior_increment, coupling, characteristic, cutoffs):
    f32 = jnp.float32
    fields = (V, 32, LANES)
    matrices = pltpu.VMEM((4, V, V, 8, LANES), f32)

    def vmem(count):
        return pltpu.VMEM((count, LANES), f32)

    scratch = [
        pltpu.VMEM(fields, f32), pltpu.VMEM((V, V, 32, LANES), f32), pltpu.VMEM(fields, f32),
        pltpu.SMEM((V, 6, V), f32), pltpu.SMEM((2,), jnp.int32),
        pltpu.VMEM((50, 2, 512), f32), pltpu.VMEM((2 * LOW, LANES), jnp.bfloat16), vmem(16),
        pltpu.SemaphoreType.DMA((8,)),
        vmem(8), vmem(8), vmem(8), vmem(8),
        vmem(128), vmem(128), vmem(128), vmem(128),
        vmem(8 * MAPS), vmem(GROUP * MAPS), vmem(MAPS), vmem(LAYERS * MAPS),
        vmem(8 * VECS), vmem(GROUP * VECS), vmem(LAYERS * VECS), vmem(GROUP * VECS), vmem(8 * VECS),
        matrices, matrices, matrices, matrices, matrices,
        pltpu.VMEM((V, V, 8, LANES), f32), pltpu.VMEM((V, V, 8, LANES), f32),
        pltpu.VMEM(fields, f32), pltpu.VMEM((4, V, 8, LANES), f32),
        pltpu.VMEM((104, 512), f32), vmem(104 * 8),
        *[pltpu.SemaphoreType.DMA] * 14, *[pltpu.SemaphoreType.DMA((2 * (LAYERS - 1),))] * 2,
    ]
    inside = pl.BlockSpec(memory_space=pltpu.VMEM)
    outside = pl.BlockSpec(memory_space=pl.ANY)
    high_low, turns = table()
    result = pl.pallas_call(
        kernel,
        out_shape=pltpu.VMEM(fields, f32),
        in_specs=[outside] * 8,
        out_specs=inside,
        scratch_shapes=scratch,
        compiler_params=pltpu.CompilerParams(collective_id=0, has_side_effects=True),
    )(
        residual.reshape(fields),
        inverse_diagonal.reshape(V, V, 32, LANES),
        prior_increment.reshape(fields),
        coupling.transpose(1, 0, 2),
        characteristic.transpose(0, 3, 4, 1, 2).reshape(50, 2, 512),
        cutoffs,
        jnp.asarray(high_low),
        jnp.asarray(turns),
    )
    return result.reshape(V, GROUP, 8, LANES)


def solution(mesh):
    field = P(None, None, "span", "pitch")
    return jax.shard_map(
        body, mesh=mesh,
        in_specs=(field, P(None, None, None, "span", "pitch"), field, P(), P(), P()),
        out_specs=field, check_vma=False,
    )
```

```python
import jax
import jax.numpy as jnp
import numpy as np
from jax import lax
from jax.experimental import pallas as pl
from jax.experimental.pallas import tpu as pltpu
from jax.sharding import PartitionSpec as P

NP = 1024
PITCH = 8
GROUP = 4
LAYERS = 8
V = 5
LINE = 16
MAPS = 88
B, C, A = 0, 25, 56
PAIR, SINGLE, USED = 50, 25, 81
VECS = 16
SENT = 10
LANES = 128

FORWARD, BACK_RE, BACK_IM, LOW = 0, 256, 384, 512
HALF = float(np.sqrt(0.5))


def table():
    two_pi = 2.0 * np.pi
    a = np.arange(8)
    b = np.arange(128)
    k2 = np.arange(64)
    twiddle = two_pi * np.outer(a, b) / NP
    lanes = two_pi * (np.outer(b, k2) % 128) / 128
    cos, sin = np.cos(lanes), np.sin(lanes)
    forward = np.block([[cos, -sin], [sin, cos]])
    back_re = np.concatenate([cos.T, -sin.T], 0)
    back_im = np.concatenate([sin.T, cos.T], 0)
    parts = [forward, back_re, back_im]
    whole = np.concatenate(parts, 0).astype(np.float32)
    high = whole.astype(jnp.bfloat16)
    low = (whole - high.astype(np.float32)).astype(jnp.bfloat16)
    turns = np.concatenate([np.cos(twiddle), np.sin(twiddle)], 0).astype(np.float32)
    return np.concatenate([high, low], 0), turns


FAR_FIRST = (4, 3, 5, 2, 6, 1, 7)
MEMBERS = (2, 1, 3)


def every(start, stride):
    return pl.ds(start, 8, stride=stride)


def rows(start, size):
    return pl.ds(pl.multiple_of(start, 8), size)


def product(later, earlier):
    total = later[0][None] * earlier[:, 0][:, None]
    for j in range(1, V):
        total = total + later[j][None] * earlier[:, j][:, None]
    return total


def apply(matrix, vector):
    total = matrix[0] * vector[0][None]
    for j in range(1, V):
        total = total + matrix[j] * vector[j][None]
    return total


def scaled(block, coupling, which):
    columns = []
    for k in range(V):
        total = block[:, 0] * (-coupling[0, which, k])
        for j in range(1, V):
            total = total + block[:, j] * (-coupling[j, which, k])
        columns.append(total)
    return jnp.stack(columns)


def times(data, const, start, size):
    data_high = data.astype(jnp.bfloat16)
    data_low = (data - data_high.astype(jnp.float32)).astype(jnp.bfloat16)
    high = const[start : start + size, :]
    low = const[LOW + start : LOW + start + size, :]
    total = jnp.dot(data_high, high, preferred_element_type=jnp.float32)
    total = total + jnp.dot(data_low, high, preferred_element_type=jnp.float32)
    return total + jnp.dot(data_high, low, preferred_element_type=jnp.float32)


def eight_forward(x):
    s0, d0, s2, d2 = x[0] + x[4], x[0] - x[4], x[2] + x[6], x[2] - x[6]
    s1, d1, s3, d3 = x[1] + x[5], x[1] - x[5], x[3] + x[7], x[3] - x[7]
    even, odd = s0 + s2, s1 + s3
    real, imag = s0 - s2, s3 - s1
    near, far = HALF * (d1 - d3), HALF * (d1 + d3)
    zero = jnp.zeros_like(even)
    first = (d0 + near, -(d2 + far))
    third = (d0 - near, d2 - far)
    return [
        (even + odd, zero), first, (real, imag), third,
        (even - odd, zero), (third[0], -third[1]), (real, -imag), (first[0], -first[1]),
    ]


def eight_back(re, im):
    p1, p2, p3 = re[1] + re[7], re[2] + re[6], re[3] + re[5]
    q1, q2, q3 = im[1] - im[7], im[2] - im[6], im[3] - im[5]
    total, gap = re[0] + re[4], re[0] - re[4]
    both, part = p1 + p3, HALF * (p1 - p3)
    cross, lean = q1 - q3, HALF * (q1 + q3)
    return [
        total + p2 + both, gap - q2 + part - lean, total - p2 - cross, gap + q2 - part - lean,
        total + p2 - both, gap - q2 - part + lean, total - p2 + cross, gap + q2 + part + lean,
    ]


def kernel(
    residual_in, inverse_in, prior_in, coupling_in, characteristic_in, cutoffs_in, const_in, turns_in, out,
    residual, inverse, prior, coupling, cutoffs, characteristic, const, turns, load_s,
    lower, upper, edge_low, edge_high, planes_out, planes_in, ordered, corr_out, corr_in,
    maps_out, maps_in, packed, layer_maps, vecs_out, vecs_in, layer_vecs, entry_out, entry_in,
    down, up, first, second, third, next_reach, next_both, source, base, flat, spectra,
    pitch_s, pitch_r, back_s, back_r, side_s, side_r,
    gm_s, gm_r, zm_s, zm_r, gv_s, gv_r, zv_s, zv_r, ge_s, ge_r, zt_s, zt_r,
):
    pitch = lax.axis_index("pitch")
    span = lax.axis_index("span")
    layer = span // GROUP
    member = span % GROUP

    def at_pitch(d):
        return {"pitch": lax.rem(pitch + d, PITCH), "span": span}

    def at_member(d):
        return {"pitch": pitch, "span": layer * GROUP + lax.rem(member + d, GROUP)}

    def at_layer(d):
        return {"pitch": pitch, "span": lax.rem(layer + d, LAYERS) * GROUP + member}

    peers = [at_pitch(d) for d in range(1, PITCH)]
    peers += [at_member(d) for d in range(1, GROUP)]
    peers += [at_layer(d) for d in range(1, LAYERS)]
    packed[...] = jnp.zeros_like(packed)
    for area in (planes_in, maps_in, layer_maps, vecs_in, layer_vecs, entry_in):
        area[...] = jnp.zeros_like(area)
    barrier = pltpu.get_barrier_semaphore()
    for peer in peers:
        pl.semaphore_signal(barrier, inc=1, device_id=peer, device_id_type=pl.DeviceIdType.MESH)

    loads = []
    for n, (src, dst) in enumerate((
        (residual_in, residual), (prior_in, prior), (inverse_in, inverse),
        (characteristic_in, characteristic), (const_in, const), (turns_in, turns),
        (coupling_in, coupling), (cutoffs_in, cutoffs),
    )):
        loads.append(pltpu.make_async_copy(src, dst, load_s.at[n]))
        loads[-1].start()

    def send(src, dst, send_sem, recv_sem, peer):
        copy = pltpu.make_async_remote_copy(
            src_ref=src, dst_ref=dst, send_sem=send_sem, recv_sem=recv_sem,
            device_id=peer, device_id_type=pl.DeviceIdType.MESH,
        )
        copy.start()

    def finish(sem, count):
        area = maps_out.at[pl.ds(0, count)]
        pltpu.make_async_copy(area, area, sem).wait()

    planes_out[...] = jnp.zeros_like(planes_out)
    maps_out[...] = jnp.zeros_like(maps_out)
    vecs_out[...] = jnp.zeros_like(vecs_out)
    loads[0].wait()
    for q, axial in enumerate((0, GROUP - 1)):
        for j in range(V):
            planes_out[every(q * V + j, LINE), :] = residual[j, axial * 8 : axial * 8 + 8, :]

    pl.semaphore_wait(barrier, len(peers))

    for d in FAR_FIRST:
        to = lax.rem(pitch + d, PITCH)
        send(
            planes_out.at[rows(to * LINE, SENT)], planes_in.at[rows(pitch * LINE, SENT)],
            pitch_s, pitch_r, at_pitch(d),
        )
    loads[1].wait()
    column = lax.broadcasted_iota(jnp.int32, (8, LANES), 1)
    last = initial = jnp.zeros((8, LANES), jnp.float32)
    for n in range(V * GROUP):
        tile = prior[n // GROUP, n % GROUP * 8 : n % GROUP * 8 + 8, :]
        last = jnp.where(column == n, pltpu.roll(tile, n + 1, 1), last)
        initial = jnp.where(column == n, pltpu.roll(tile, n, 1) if n else tile, initial)
    edge_high[...] = last
    edge_low[...] = initial
    send(edge_high, lower, side_s, side_r, at_pitch(1))
    send(edge_low, upper, side_s, side_r, at_pitch(PITCH - 1))

    loads[2].wait()
    loads[6].wait()
    reach = None
    for s in range(4):
        block = inverse[:, :, every(s, 4), :]
        down[s] = scaled(block, coupling, 0)
        up[s] = scaled(block, coupling, 1)
        reach = down[s] if s == 0 else product(down[s], reach)
        first[s] = reach
    both = reach
    trail = up[3]
    second[3] = both
    third[3] = trail
    for s in (2, 1, 0):
        both = first[s] + product(up[s], both)
        trail = product(up[s], trail)
        second[s] = both
        third[s] = trail
    upper_reach = pltpu.roll(reach, 7, 2)
    upper_both = pltpu.roll(both, 7, 2)
    next_reach[...] = upper_reach
    next_both[...] = upper_both
    both = both + product(trail, product(upper_both, reach))
    trail = product(trail, pltpu.roll(trail, 7, 2))
    reach = product(upper_reach, reach)
    for k in range(V):
        for i in range(V):
            maps_out[every(A + V * k + i, MAPS), :] = reach[k, i]
            maps_out[every(B + V * k + i, MAPS), :] = trail[k, i]
            maps_out[every(C + V * k + i, MAPS), :] = both[k, i]

    for d in MEMBERS:
        to = lax.rem(member + d, GROUP)
        send(
            maps_out.at[rows(to * 2 * MAPS, USED)], maps_in.at[rows(member * MAPS, USED)],
            gm_s, gm_r, at_member(d),
        )
    planes_in[rows(pitch * LINE, LINE), :] = planes_out[rows(pitch * LINE, LINE), :]
    maps_in[rows(member * MAPS, MAPS), :] = maps_out[rows(member * 2 * MAPS, MAPS), :]

    loads[3].wait()
    flat[100:104, :] = jnp.zeros((4, 512), jnp.float32)
    for n in range(50):
        flat[2 * n : 2 * n + 2, :] = characteristic[n]
    whole = flat[...]
    high = whole.astype(jnp.bfloat16)
    rest = whole - high.astype(jnp.float32)
    middle = rest.astype(jnp.bfloat16)
    low = (rest - middle.astype(jnp.float32)).astype(jnp.bfloat16)
    harmonic = lax.broadcasted_iota(jnp.int32, (512, LANES), 0)
    lane = lax.broadcasted_iota(jnp.int32, (512, LANES), 1)
    apart = harmonic - 8 * (lane % 64)
    for k1 in range(8):
        pick = jnp.where(apart == k1, 1.0, 0.0).astype(jnp.bfloat16)
        part = jnp.dot(high, pick, preferred_element_type=jnp.float32)
        part = part + jnp.dot(middle, pick, preferred_element_type=jnp.float32)
        part = part + jnp.dot(low, pick, preferred_element_type=jnp.float32)
        spectra[pl.ds(k1, 104, stride=8), :] = part

    finish(pitch_r, (PITCH - 1) * SENT)
    for load in (loads[4], loads[5], loads[7]):
        load.wait()
    turned_re, turned_im = [], []
    parts = eight_forward([planes_in[a * LINE : a * LINE + LINE, :] for a in range(8)])
    for k1, (re, im) in enumerate(parts):
        turn_re, turn_im = turns[k1 : k1 + 1, :], turns[8 + k1 : 9 + k1, :]
        turned_re.append(re * turn_re + im * turn_im)
        turned_im.append(im * turn_re - re * turn_im)
    turned = jnp.concatenate([jnp.concatenate(turned_re, 0), jnp.concatenate(turned_im, 0)], 1)
    ordered[...] = times(turned, const, FORWARD, 256)
    spectrum = jnp.concatenate([ordered[every(line, LINE), :] for line in range(2 * V)], 0)
    number = lax.broadcasted_iota(jnp.int32, (8, LANES), 0) + 8 * (lax.broadcasted_iota(jnp.int32, (8, LANES), 1) % 64)
    weight = jnp.where(number == 0, 1.0, 2.0) / NP
    sign = jnp.where(lax.broadcasted_iota(jnp.int32, (80, LANES), 1) < 64, -1.0, 1.0)
    crossed = (pltpu.roll(spectrum, 64, 1) * sign).reshape(2, V, 8, LANES)
    spectrum = spectrum.reshape(2, V, 8, LANES)
    for q in range(2):
        factor = jnp.where(number < cutoffs[q], weight, 0.0)
        for i in range(V):
            total = None
            for j in range(V):
                row = (q * 25 + i * V + j) * 16
                term = spectra[row : row + 8, :] * spectrum[q, j] + spectra[row + 8 : row + 16, :] * crossed[q, j]
                total = term if total is None else total + term
            ordered[every(q * V + i, LINE), :] = total * factor
    corrected = ordered[...]
    back_re = times(corrected, const, BACK_RE, 128)
    back_im = times(corrected, const, BACK_IM, 128)
    lines_re, lines_im = [], []
    for k1 in range(8):
        turn_re, turn_im = turns[k1 : k1 + 1, :], turns[8 + k1 : 9 + k1, :]
        re, im = back_re[k1 * LINE : k1 * LINE + LINE], back_im[k1 * LINE : k1 * LINE + LINE]
        lines_re.append(re * turn_re - im * turn_im)
        lines_im.append(im * turn_re + re * turn_im)
    for a, value in enumerate(eight_back(lines_re, lines_im)):
        corr_out[a * LINE : a * LINE + LINE, :] = value
    for d in FAR_FIRST:
        to = lax.rem(pitch + d, PITCH)
        send(
            corr_out.at[rows(to * LINE, SENT)], corr_in.at[rows(pitch * LINE, SENT)],
            back_s, back_r, at_pitch(d),
        )
    corr_in[rows(pitch * LINE, LINE), :] = corr_out[rows(pitch * LINE, LINE), :]

    place = lax.broadcasted_iota(jnp.int32, (8, LANES), 0)

    def tiles(ref, n, which):
        start = n * MAPS + which
        return [ref[start + V * j : start + V * j + 8, :] for j in range(V)]

    def spread_rows(vector):
        return [jnp.broadcast_to(vector[..., j : j + 1, :], vector.shape) for j in range(V)]

    def mix(matrix, parts):
        total = matrix[0] * parts[0]
        for j in range(1, V):
            total = total + matrix[j] * parts[j]
        return total

    finish(gm_r, (GROUP - 1) * USED)
    forward = jnp.stack(tiles(maps_in, 0, A))
    across = [jnp.stack(tiles(maps_in, 0, C))]
    for n in range(1, GROUP):
        parts = spread_rows(forward)
        forward = mix(tiles(maps_in, n, A), parts)
        across.append(mix(tiles(maps_in, n, C), parts))
    backward = jnp.concatenate([jnp.stack(tiles(maps_in, GROUP - 1, B)), across[GROUP - 1]], 0)
    for n in range(GROUP - 2, -1, -1):
        backward = mix(tiles(maps_in, n, B), spread_rows(backward))
        backward = jnp.concatenate([backward[:V], backward[V:] + across[n]], 0)
    columns = jnp.concatenate([forward, backward], 0)
    for n in range(3 * V):
        start = A + V * n if n < V else V * n - 25
        packed[start : start + 8, :] = columns[n]
    layer_maps[rows(layer * MAPS, MAPS), :] = packed[...]
    lower_copies = []
    for d in FAR_FIRST:
        send(
            layer_maps.at[rows(layer * MAPS + A, SINGLE)], layer_maps.at[rows(layer * MAPS + A, SINGLE)],
            zm_s, zm_r, at_layer(d),
        )
        copy = pltpu.make_async_remote_copy(
            src_ref=layer_maps.at[rows(layer * MAPS, PAIR)], dst_ref=layer_maps.at[rows(layer * MAPS, PAIR)],
            send_sem=zt_s.at[d - 1], recv_sem=zt_r.at[d - 1],
            device_id=at_layer(d), device_id_type=pl.DeviceIdType.MESH,
        )
        lower_copies.append((copy, layer + d >= LAYERS, layer < d))
        pl.when(layer + d >= LAYERS)(copy.start)

    finish(side_r, 16)
    own = prior[...]
    below, above = [], []
    for i in range(V):
        low_tiles, high_tiles = [], []
        for a in range(GROUP):
            n = i * GROUP + a
            tile = prior[i, a * 8 : a * 8 + 8, :]
            edge = pltpu.roll(lower[...], LANES - n, 1) if n else lower[...]
            low_tiles.append(jnp.where(column == 0, edge, pltpu.roll(tile, 1, 1)))
            edge = pltpu.roll(upper[...], LANES - 1 - n, 1)
            high_tiles.append(jnp.where(column == LANES - 1, edge, pltpu.roll(tile, LANES - 1, 1)))
        below.append(jnp.concatenate(low_tiles, 0))
        above.append(jnp.concatenate(high_tiles, 0))
    zero_row = jnp.zeros((8, LANES), jnp.float32)
    for i in range(V):
        total = residual[i]
        before = after = None
        for j in range(V):
            total = total - coupling[i, 2, j] * below[j] - coupling[i, 3, j] * above[j]
            low_term = coupling[i, 4, j] * own[j]
            high_term = coupling[i, 5, j] * own[j]
            before = low_term if before is None else before + low_term
            after = high_term if after is None else after + high_term
        total = total - jnp.concatenate([zero_row, before[:24]], 0) - jnp.concatenate([after[8:], zero_row], 0)
        source[i] = total

    finish(back_r, (PITCH - 1) * SENT)
    for j in range(V):
        source[j, 0:8, :] = source[j, 0:8, :] + corr_in[every(j, LINE), :]
        source[j, 24:32, :] = source[j, 24:32, :] + corr_in[every(V + j, LINE), :]
    star = None
    for s in range(4):
        block = inverse[:, :, every(s, 4), :]
        rhs = source[:, every(s, 4), :]
        value = block[:, 0] * rhs[0][None]
        for j in range(1, V):
            value = value + block[:, j] * rhs[j][None]
        star = value if s == 0 else value + apply(down[s], star)
        base[s] = star
    update = star
    for s in (2, 1, 0):
        update = base[s] + apply(up[s], update)
        base[s] = update
    ahead = pltpu.roll(star, 7, 1) + apply(next_reach, star)
    behind = update + apply(third[0], pltpu.roll(update, 7, 1) + apply(next_both, star))
    for i in range(V):
        vecs_out[every(i, VECS), :] = ahead[i]
        vecs_out[every(V + i, VECS), :] = behind[i]
    for d in MEMBERS:
        to = lax.rem(member + d, GROUP)
        send(
            vecs_out.at[rows(to * 2 * VECS, SENT)], vecs_in.at[rows(member * VECS, SENT)],
            gv_s, gv_r, at_member(d),
        )
    vecs_in[rows(member * VECS, VECS), :] = vecs_out[rows(member * 2 * VECS, VECS), :]

    def chain(count, maps_ref, vecs_ref, x, y):
        entering_x, entering_y, crossing = [], [None] * count, []
        for n in range(count):
            entering_x.append(x)
            offset = vecs_ref[n * VECS : n * VECS + 8, :]
            if x is None:
                crossing.append(vecs_ref[n * VECS + V : n * VECS + V + 8, :])
                x = offset
            else:
                parts = spread_rows(x)
                ahead = mix(tiles(maps_ref, n, A), parts)
                crossing.append(mix(tiles(maps_ref, n, C), parts) + vecs_ref[n * VECS + V : n * VECS + V + 8, :])
                x = ahead + offset
        for n in range(count - 1, -1, -1):
            entering_y[n] = y
            y = crossing[n] if y is None else mix(tiles(maps_ref, n, B), spread_rows(y)) + crossing[n]
        return entering_x, entering_y, x, y

    finish(gv_r, (GROUP - 1) * SENT)
    _, _, x, y = chain(GROUP, maps_in, vecs_in, None, None)
    tail = pltpu.roll(y, V, 0)
    layer_vecs[rows(layer * VECS, 8), :] = jnp.where(place < V, x, tail)
    layer_vecs[rows(layer * VECS + 8, 8), :] = tail
    for d in FAR_FIRST:
        send(
            layer_vecs.at[rows(layer * VECS, SENT)], layer_vecs.at[rows(layer * VECS, SENT)],
            zv_s, zv_r, at_layer(d),
        )
    finish(zm_r, (LAYERS - 1) * SINGLE)
    for copy, _, from_above in lower_copies:
        pl.when(from_above)(copy.wait_recv)
    finish(zv_r, (LAYERS - 1) * SENT)
    entering_x, entering_y, _, _ = chain(LAYERS, layer_maps, layer_vecs, None, None)
    x = jnp.zeros((8, LANES), jnp.float32)
    y = jnp.zeros((8, LANES), jnp.float32)
    for n in range(8):
        if entering_x[n] is not None:
            x = jnp.where(layer == n, entering_x[n], x)
        if entering_y[n] is not None:
            y = jnp.where(layer == n, entering_y[n], y)
    entering_x, entering_y, _, _ = chain(GROUP, maps_in, vecs_in, x, y)
    for n in range(GROUP):
        tail = pltpu.roll(entering_y[n], V, 0)
        entry_out[n * VECS : n * VECS + 8, :] = jnp.where(place < V, entering_x[n], tail)
        entry_out[n * VECS + 8 : n * VECS + 16, :] = tail
    for d in MEMBERS:
        to = lax.rem(member + d, GROUP)
        send(
            entry_out.at[rows(to * VECS, SENT)], entry_in.at[rows(member * 2 * VECS, SENT)],
            ge_s, ge_r, at_member(d),
        )
    entry_in[rows(member * 2 * VECS, VECS), :] = entry_out[rows(member * VECS, VECS), :]
    finish(ge_r, (GROUP - 1) * SENT)
    x = jnp.stack([entry_in[every(i, VECS), :] for i in range(V)])
    y = jnp.stack([entry_in[every(V + i, VECS), :] for i in range(V)])
    odd = place % 2 == 1
    x = jnp.where(odd, pltpu.roll(apply(first[3], x) + base[3], 1, 1), x)
    y = jnp.where(odd, pltpu.roll(y, 1, 1), y)
    y = jnp.where(odd, y, pltpu.roll(apply(third[0], y) + apply(second[0], x) + base[0], 7, 1))
    for s in range(4):
        value = base[s]
        for j in range(V):
            value = value + second[s, j] * x[j][None] + third[s, j] * y[j][None]
        for i in range(V):
            out[i, every(s, 4), :] = value[i]

    finish(pitch_s, (PITCH - 1) * SENT)
    finish(side_s, 16)
    finish(gm_s, (GROUP - 1) * USED)
    finish(back_s, (PITCH - 1) * SENT)
    finish(gv_s, (GROUP - 1) * SENT)
    finish(zv_s, (LAYERS - 1) * SENT)
    finish(ge_s, (GROUP - 1) * SENT)
    finish(zm_s, (LAYERS - 1) * SINGLE)
    for copy, wraps, _ in lower_copies:
        pl.when(wraps)(copy.wait_send)


def body(residual, inverse_diagonal, prior_increment, coupling, characteristic, cutoffs):
    f32 = jnp.float32
    fields = (V, 32, LANES)
    matrices = pltpu.VMEM((4, V, V, 8, LANES), f32)

    def vmem(count):
        return pltpu.VMEM((count, LANES), f32)

    scratch = [
        pltpu.VMEM(fields, f32), pltpu.VMEM((V, V, 32, LANES), f32), pltpu.VMEM(fields, f32),
        pltpu.SMEM((V, 6, V), f32), pltpu.SMEM((2,), jnp.int32),
        pltpu.VMEM((50, 2, 512), f32), pltpu.VMEM((2 * LOW, LANES), jnp.bfloat16), vmem(16),
        pltpu.SemaphoreType.DMA((8,)),
        vmem(8), vmem(8), vmem(8), vmem(8),
        vmem(128), vmem(128), vmem(128), vmem(128), vmem(128),
        vmem(8 * MAPS), vmem(GROUP * MAPS), vmem(MAPS), vmem(LAYERS * MAPS),
        vmem(8 * VECS), vmem(GROUP * VECS), vmem(LAYERS * VECS), vmem(GROUP * VECS), vmem(8 * VECS),
        matrices, matrices, matrices, matrices, matrices,
        pltpu.VMEM((V, V, 8, LANES), f32), pltpu.VMEM((V, V, 8, LANES), f32),
        pltpu.VMEM(fields, f32), pltpu.VMEM((4, V, 8, LANES), f32),
        pltpu.VMEM((104, 512), f32), vmem(104 * 8),
        *[pltpu.SemaphoreType.DMA] * 16, *[pltpu.SemaphoreType.DMA((LAYERS - 1,))] * 2,
    ]
    inside = pl.BlockSpec(memory_space=pltpu.VMEM)
    outside = pl.BlockSpec(memory_space=pl.ANY)
    high_low, turns = table()
    result = pl.pallas_call(
        kernel,
        out_shape=pltpu.VMEM(fields, f32),
        in_specs=[outside] * 8,
        out_specs=inside,
        scratch_shapes=scratch,
        compiler_params=pltpu.CompilerParams(collective_id=0, has_side_effects=True),
    )(
        residual.reshape(fields),
        inverse_diagonal.reshape(V, V, 32, LANES),
        prior_increment.reshape(fields),
        coupling.transpose(1, 0, 2),
        characteristic.transpose(0, 3, 4, 1, 2).reshape(50, 2, 512),
        cutoffs,
        jnp.asarray(high_low),
        jnp.asarray(turns),
    )
    return result.reshape(V, GROUP, 8, LANES)


def solution(mesh):
    field = P(None, None, "span", "pitch")
    return jax.shard_map(
        body, mesh=mesh,
        in_specs=(field, P(None, None, None, "span", "pitch"), field, P(), P(), P()),
        out_specs=field, check_vma=False,
    )
```

```python
import jax
import jax.numpy as jnp
import numpy as np
from jax import lax
from jax.experimental import pallas as pl
from jax.experimental.pallas import tpu as pltpu
from jax.sharding import PartitionSpec as P

NP = 1024
PITCH = 8
GROUP = 4
LAYERS = 8
V = 5
LINE = 16
MAPS = 88
B, C, A = 0, 25, 56
PAIR, SINGLE, USED = 50, 25, 81
VECS = 16
SENT = 10
LANES = 128

FORWARD, BACK_RE, BACK_IM, LOW = 0, 256, 384, 512
HALF = float(np.sqrt(0.5))


def table():
    two_pi = 2.0 * np.pi
    a = np.arange(8)
    b = np.arange(128)
    k2 = np.arange(64)
    twiddle = two_pi * np.outer(a, b) / NP
    lanes = two_pi * (np.outer(b, k2) % 128) / 128
    cos, sin = np.cos(lanes), np.sin(lanes)
    forward = np.block([[cos, -sin], [sin, cos]])
    back_re = np.concatenate([cos.T, -sin.T], 0)
    back_im = np.concatenate([sin.T, cos.T], 0)
    parts = [forward, back_re, back_im]
    whole = np.concatenate(parts, 0).astype(np.float32)
    high = whole.astype(jnp.bfloat16)
    low = (whole - high.astype(np.float32)).astype(jnp.bfloat16)
    turns = np.concatenate([np.cos(twiddle), np.sin(twiddle)], 0).astype(np.float32)
    return np.concatenate([high, low], 0), turns


FAR_FIRST = (4, 3, 5, 2, 6, 1, 7)
MEMBERS = (2, 1, 3)


def every(start, stride):
    return pl.ds(start, 8, stride=stride)


def rows(start, size):
    return pl.ds(pl.multiple_of(start, 8), size)


def product(later, earlier):
    total = later[0][None] * earlier[:, 0][:, None]
    for j in range(1, V):
        total = total + later[j][None] * earlier[:, j][:, None]
    return total


def apply(matrix, vector):
    total = matrix[0] * vector[0][None]
    for j in range(1, V):
        total = total + matrix[j] * vector[j][None]
    return total


def scaled(block, coupling, which):
    columns = []
    for k in range(V):
        total = block[:, 0] * (-coupling[0, which, k])
        for j in range(1, V):
            total = total + block[:, j] * (-coupling[j, which, k])
        columns.append(total)
    return jnp.stack(columns)


def times(data, const, start, size):
    data_high = data.astype(jnp.bfloat16)
    data_low = (data - data_high.astype(jnp.float32)).astype(jnp.bfloat16)
    high = const[start : start + size, :]
    low = const[LOW + start : LOW + start + size, :]
    total = jnp.dot(data_high, high, preferred_element_type=jnp.float32)
    total = total + jnp.dot(data_low, high, preferred_element_type=jnp.float32)
    return total + jnp.dot(data_high, low, preferred_element_type=jnp.float32)


def eight_forward(x):
    s0, d0, s2, d2 = x[0] + x[4], x[0] - x[4], x[2] + x[6], x[2] - x[6]
    s1, d1, s3, d3 = x[1] + x[5], x[1] - x[5], x[3] + x[7], x[3] - x[7]
    even, odd = s0 + s2, s1 + s3
    real, imag = s0 - s2, s3 - s1
    near, far = HALF * (d1 - d3), HALF * (d1 + d3)
    zero = jnp.zeros_like(even)
    first = (d0 + near, -(d2 + far))
    third = (d0 - near, d2 - far)
    return [
        (even + odd, zero), first, (real, imag), third,
        (even - odd, zero), (third[0], -third[1]), (real, -imag), (first[0], -first[1]),
    ]


def eight_back(re, im):
    p1, p2, p3 = re[1] + re[7], re[2] + re[6], re[3] + re[5]
    q1, q2, q3 = im[1] - im[7], im[2] - im[6], im[3] - im[5]
    total, gap = re[0] + re[4], re[0] - re[4]
    both, part = p1 + p3, HALF * (p1 - p3)
    cross, lean = q1 - q3, HALF * (q1 + q3)
    return [
        total + p2 + both, gap - q2 + part - lean, total - p2 - cross, gap + q2 - part - lean,
        total + p2 - both, gap - q2 - part + lean, total - p2 + cross, gap + q2 + part + lean,
    ]


def kernel(
    residual_in, inverse_in, prior_in, coupling_in, characteristic_in, cutoffs_in, const_in, turns_in, out,
    residual, inverse, prior, coupling, cutoffs, characteristic, const, turns, load_s,
    lower, upper, edge_low, edge_high, planes_out, planes_in, ordered, corr_out, corr_in,
    maps_out, maps_in, packed, layer_maps, vecs_early, vecs_out, vecs_in, layer_vecs, entry_out, entry_in,
    down, up, first, second, third, next_reach, next_both, source, base, flat, spectra,
    pitch_s, pitch_r, back_s, back_r, side_s, side_r,
    gm_s, gm_r, zm_s, zm_r, gv_s, gv_r, zv_s, zv_r, ge_s, ge_r, zt_s, zt_r,
):
    pitch = lax.axis_index("pitch")
    span = lax.axis_index("span")
    layer = span // GROUP
    member = span % GROUP

    def cell(m):
        return (1 - m // 2) * (1 - m) + m // 2 * m

    def at_pitch(d):
        return {"pitch": lax.rem(pitch + d, PITCH), "span": span}

    def at_member(d):
        return {"pitch": pitch, "span": layer * GROUP + lax.rem(member + d, GROUP)}

    def at_layer(d):
        return {"pitch": pitch, "span": lax.rem(layer + d, LAYERS) * GROUP + member}

    peers = [at_pitch(d) for d in range(1, PITCH)]
    peers += [at_member(d) for d in range(1, GROUP)]
    peers += [at_layer(d) for d in range(1, LAYERS)]
    loads = [pltpu.make_async_copy(residual_in, residual, load_s.at[0])]
    loads[0].start()
    barrier = pltpu.get_barrier_semaphore()
    for peer in peers:
        pl.semaphore_signal(barrier, inc=1, device_id=peer, device_id_type=pl.DeviceIdType.MESH)

    for n, (src, dst) in enumerate((
        (prior_in, prior), (inverse_in, inverse),
        (characteristic_in, characteristic), (const_in, const), (turns_in, turns),
        (coupling_in, coupling), (cutoffs_in, cutoffs),
    )):
        loads.append(pltpu.make_async_copy(src, dst, load_s.at[n + 1]))
        loads[-1].start()

    def send(src, dst, send_sem, recv_sem, peer):
        copy = pltpu.make_async_remote_copy(
            src_ref=src, dst_ref=dst, send_sem=send_sem, recv_sem=recv_sem,
            device_id=peer, device_id_type=pl.DeviceIdType.MESH,
        )
        copy.start()

    def to_layer(src, dst, send_sem, recv_sem, t):
        return pltpu.make_async_remote_copy(
            src_ref=src, dst_ref=dst, send_sem=send_sem, recv_sem=recv_sem,
            device_id={"pitch": pitch, "span": t * GROUP + member}, device_id_type=pl.DeviceIdType.MESH,
        )

    def finish(sem, count):
        area = maps_out.at[pl.ds(0, count)]
        pltpu.make_async_copy(area, area, sem).wait()

    loads[0].wait()
    for q, axial in enumerate((0, GROUP - 1)):
        for j in range(V):
            planes_out[every(q * V + j, LINE), :] = residual[j, axial * 8 : axial * 8 + 8, :]

    loads[2].wait()
    loads[6].wait()
    reach = None
    for s in range(4):
        block = inverse[:, :, every(s, 4), :]
        down[s] = scaled(block, coupling, 0)
        up[s] = scaled(block, coupling, 1)
        reach = down[s] if s == 0 else product(down[s], reach)
        first[s] = reach

    pl.semaphore_wait(barrier, len(peers))

    for d in FAR_FIRST:
        to = lax.rem(pitch + d, PITCH)
        send(
            planes_out.at[rows(to * LINE, SENT)], planes_in.at[rows(pitch * LINE, SENT)],
            pitch_s, pitch_r, at_pitch(d),
        )
    reach = first[3]
    both = reach
    trail = up[3]
    second[3] = both
    third[3] = trail
    for s in (2, 1, 0):
        both = first[s] + product(up[s], both)
        trail = product(up[s], trail)
        second[s] = both
        third[s] = trail
    upper_reach = pltpu.roll(reach, 7, 2)
    upper_both = pltpu.roll(both, 7, 2)
    next_reach[...] = upper_reach
    next_both[...] = upper_both
    both = both + product(trail, product(upper_both, reach))
    trail = product(trail, pltpu.roll(trail, 7, 2))
    reach = product(upper_reach, reach)
    for k in range(V):
        for i in range(V):
            maps_out[every(A + V * k + i, MAPS), :] = reach[k, i]
            maps_out[every(B + V * k + i, MAPS), :] = trail[k, i]
            maps_out[every(C + V * k + i, MAPS), :] = both[k, i]
    for d in MEMBERS:
        to = lax.rem(member + d, GROUP)
        send(
            maps_out.at[rows(cell(to) * 2 * MAPS, USED)], maps_in.at[rows(member * MAPS, USED)],
            gm_s, gm_r, at_member(d),
        )
    loads[1].wait()
    column = lax.broadcasted_iota(jnp.int32, (8, LANES), 1)
    last = initial = jnp.zeros((8, LANES), jnp.float32)
    for n in range(V * GROUP):
        tile = prior[n // GROUP, n % GROUP * 8 : n % GROUP * 8 + 8, :]
        last = jnp.where(column == n, pltpu.roll(tile, n + 1, 1), last)
        initial = jnp.where(column == n, pltpu.roll(tile, n, 1) if n else tile, initial)
    edge_high[...] = last
    edge_low[...] = initial
    send(edge_high, lower, side_s, side_r, at_pitch(1))
    send(edge_low, upper, side_s, side_r, at_pitch(PITCH - 1))

    planes_in[rows(pitch * LINE, LINE), :] = planes_out[rows(pitch * LINE, LINE), :]
    maps_in[rows(member * MAPS, MAPS), :] = maps_out[rows(cell(member) * 2 * MAPS, MAPS), :]

    loads[3].wait()
    flat[100:104, :] = jnp.zeros((4, 512), jnp.float32)
    for n in range(50):
        flat[2 * n : 2 * n + 2, :] = characteristic[n]
    whole = flat[...]
    high = whole.astype(jnp.bfloat16)
    rest = whole - high.astype(jnp.float32)
    middle = rest.astype(jnp.bfloat16)
    low = (rest - middle.astype(jnp.float32)).astype(jnp.bfloat16)
    harmonic = lax.broadcasted_iota(jnp.int32, (512, LANES), 0)
    lane = lax.broadcasted_iota(jnp.int32, (512, LANES), 1)
    apart = harmonic - 8 * (lane % 64)
    for k1 in range(8):
        pick = jnp.where(apart == k1, 1.0, 0.0).astype(jnp.bfloat16)
        part = jnp.dot(high, pick, preferred_element_type=jnp.float32)
        part = part + jnp.dot(middle, pick, preferred_element_type=jnp.float32)
        part = part + jnp.dot(low, pick, preferred_element_type=jnp.float32)
        spectra[pl.ds(k1, 104, stride=8), :] = part

    finish(pitch_r, (PITCH - 1) * SENT)
    for load in (loads[4], loads[5], loads[7]):
        load.wait()
    turned_re, turned_im = [], []
    parts = eight_forward([planes_in[a * LINE : a * LINE + LINE, :] for a in range(8)])
    for k1, (re, im) in enumerate(parts):
        turn_re, turn_im = turns[k1 : k1 + 1, :], turns[8 + k1 : 9 + k1, :]
        turned_re.append(re * turn_re + im * turn_im)
        turned_im.append(im * turn_re - re * turn_im)
    turned = jnp.concatenate([jnp.concatenate(turned_re, 0), jnp.concatenate(turned_im, 0)], 1)
    ordered[...] = times(turned, const, FORWARD, 256)
    spectrum = jnp.concatenate([ordered[every(line, LINE), :] for line in range(2 * V)], 0)
    number = lax.broadcasted_iota(jnp.int32, (8, LANES), 0) + 8 * (lax.broadcasted_iota(jnp.int32, (8, LANES), 1) % 64)
    weight = jnp.where(number == 0, 1.0, 2.0) / NP
    sign = jnp.where(lax.broadcasted_iota(jnp.int32, (80, LANES), 1) < 64, -1.0, 1.0)
    crossed = (pltpu.roll(spectrum, 64, 1) * sign).reshape(2, V, 8, LANES)
    spectrum = spectrum.reshape(2, V, 8, LANES)
    for q in range(2):
        factor = jnp.where(number < cutoffs[q], weight, 0.0)
        for i in range(V):
            total = None
            for j in range(V):
                row = (q * 25 + i * V + j) * 16
                term = spectra[row : row + 8, :] * spectrum[q, j] + spectra[row + 8 : row + 16, :] * crossed[q, j]
                total = term if total is None else total + term
            ordered[every(q * V + i, LINE), :] = total * factor
    corrected = ordered[...]
    back_re = times(corrected, const, BACK_RE, 128)
    back_im = times(corrected, const, BACK_IM, 128)
    lines_re, lines_im = [], []
    for k1 in range(8):
        turn_re, turn_im = turns[k1 : k1 + 1, :], turns[8 + k1 : 9 + k1, :]
        re, im = back_re[k1 * LINE : k1 * LINE + LINE], back_im[k1 * LINE : k1 * LINE + LINE]
        lines_re.append(re * turn_re - im * turn_im)
        lines_im.append(im * turn_re + re * turn_im)
    for a, value in enumerate(eight_back(lines_re, lines_im)):
        corr_out[a * LINE : a * LINE + LINE, :] = value
    for d in FAR_FIRST:
        to = lax.rem(pitch + d, PITCH)
        send(
            corr_out.at[rows(to * LINE, SENT)], corr_in.at[rows(pitch * LINE, SENT)],
            back_s, back_r, at_pitch(d),
        )
    corr_in[rows(pitch * LINE, LINE), :] = corr_out[rows(pitch * LINE, LINE), :]

    place = lax.broadcasted_iota(jnp.int32, (8, LANES), 0)

    def tiles(ref, n, which):
        start = n * MAPS + which
        return [ref[start + V * j : start + V * j + 8, :] for j in range(V)]

    def spread_rows(vector):
        return [jnp.broadcast_to(vector[..., j : j + 1, :], vector.shape) for j in range(V)]

    def mix(matrix, parts):
        total = matrix[0] * parts[0]
        for j in range(1, V):
            total = total + matrix[j] * parts[j]
        return total

    finish(gm_r, (GROUP - 1) * USED)
    forward = jnp.stack(tiles(maps_in, 0, A))
    across = [jnp.stack(tiles(maps_in, 0, C))]
    for n in range(1, GROUP):
        parts = spread_rows(forward)
        forward = mix(tiles(maps_in, n, A), parts)
        across.append(mix(tiles(maps_in, n, C), parts))
    backward = jnp.concatenate([jnp.stack(tiles(maps_in, GROUP - 1, B)), across[GROUP - 1]], 0)
    for n in range(GROUP - 2, -1, -1):
        backward = mix(tiles(maps_in, n, B), spread_rows(backward))
        backward = jnp.concatenate([backward[:V], backward[V:] + across[n]], 0)
    columns = jnp.concatenate([forward, backward], 0)
    for n in range(3 * V):
        start = A + V * n if n < V else V * n - 25
        packed[start : start + 8, :] = columns[n]
    layer_maps[rows(layer * MAPS, MAPS), :] = packed[...]
    lower_copies = []
    for t in range(LAYERS):
        single = to_layer(
            layer_maps.at[rows(layer * MAPS + A, SINGLE)], layer_maps.at[rows(layer * MAPS + A, SINGLE)], zm_s, zm_r, t,
        )
        pl.when(layer != t)(single.start)
        pair = to_layer(
            layer_maps.at[rows(layer * MAPS, PAIR)], layer_maps.at[rows(layer * MAPS, PAIR)], zt_s.at[t], zt_r.at[layer], t,
        )
        pl.when(layer > t)(pair.start)
        lower_copies.append(pair)

    finish(side_r, 16)
    own = prior[...]
    below, above = [], []
    for i in range(V):
        low_tiles, high_tiles = [], []
        for a in range(GROUP):
            n = i * GROUP + a
            tile = prior[i, a * 8 : a * 8 + 8, :]
            edge = pltpu.roll(lower[...], LANES - n, 1) if n else lower[...]
            low_tiles.append(jnp.where(column == 0, edge, pltpu.roll(tile, 1, 1)))
            edge = pltpu.roll(upper[...], LANES - 1 - n, 1)
            high_tiles.append(jnp.where(column == LANES - 1, edge, pltpu.roll(tile, LANES - 1, 1)))
        below.append(jnp.concatenate(low_tiles, 0))
        above.append(jnp.concatenate(high_tiles, 0))
    zero_row = jnp.zeros((8, LANES), jnp.float32)
    for i in range(V):
        total = residual[i]
        before = after = None
        for j in range(V):
            total = total - coupling[i, 2, j] * below[j] - coupling[i, 3, j] * above[j]
            low_term = coupling[i, 4, j] * own[j]
            high_term = coupling[i, 5, j] * own[j]
            before = low_term if before is None else before + low_term
            after = high_term if after is None else after + high_term
        total = total - jnp.concatenate([zero_row, before[:24]], 0) - jnp.concatenate([after[8:], zero_row], 0)
        source[i] = total

    def sweep(offsets, parity):
        star = None
        for s in range(4):
            block = inverse[:, :, every(s, 4), :]
            rhs = source[:, every(s, 4), :]
            value = block[:, 0] * rhs[0][None]
            for j in range(1, V):
                value = value + block[:, j] * rhs[j][None]
            star = value if s == 0 else value + apply(down[s], star)
            base[s] = star
        update = star
        for s in (2, 1, 0):
            update = base[s] + apply(up[s], update)
            base[s] = update
        ahead = pltpu.roll(star, 7, 1) + apply(next_reach, star)
        behind = update + apply(third[0], pltpu.roll(update, 7, 1) + apply(next_both, star))
        for i in range(V):
            offsets[every(i, VECS), :] = ahead[i]
            offsets[every(V + i, VECS), :] = behind[i]
        for d in MEMBERS:
            to = lax.rem(member + d, GROUP)
            copy = pltpu.make_async_remote_copy(
                src_ref=offsets.at[rows(cell(to) * 2 * VECS, SENT)], dst_ref=vecs_in.at[rows(member * VECS, SENT)],
                send_sem=gv_s, recv_sem=gv_r,
                device_id=at_member(d), device_id_type=pl.DeviceIdType.MESH,
            )
            pl.when(lax.rem(to, 2) == parity)(copy.start)

    sweep(vecs_early, 0)

    finish(back_r, (PITCH - 1) * SENT)
    for j in range(V):
        source[j, 0:8, :] = source[j, 0:8, :] + corr_in[every(j, LINE), :]
        source[j, 24:32, :] = source[j, 24:32, :] + corr_in[every(V + j, LINE), :]
    sweep(vecs_out, 1)
    vecs_in[rows(member * VECS, VECS), :] = vecs_out[rows(cell(member) * 2 * VECS, VECS), :]

    def chain(count, maps_ref, vecs_ref, x, y):
        entering_x, entering_y, crossing = [], [None] * count, []
        for n in range(count):
            entering_x.append(x)
            offset = vecs_ref[n * VECS : n * VECS + 8, :]
            if x is None:
                crossing.append(vecs_ref[n * VECS + V : n * VECS + V + 8, :])
                x = offset
            else:
                parts = spread_rows(x)
                ahead = mix(tiles(maps_ref, n, A), parts)
                crossing.append(mix(tiles(maps_ref, n, C), parts) + vecs_ref[n * VECS + V : n * VECS + V + 8, :])
                x = ahead + offset
        for n in range(count - 1, -1, -1):
            entering_y[n] = y
            y = crossing[n] if y is None else mix(tiles(maps_ref, n, B), spread_rows(y)) + crossing[n]
        return entering_x, entering_y, x, y

    finish(gv_r, (GROUP - 1) * SENT)
    _, _, x, y = chain(GROUP, maps_in, vecs_in, None, None)
    tail = pltpu.roll(y, V, 0)
    layer_vecs[rows(layer * VECS, 8), :] = jnp.where(place < V, x, tail)
    layer_vecs[rows(layer * VECS + 8, 8), :] = tail
    for t in range(LAYERS):
        pl.when(layer != t)(to_layer(
            layer_vecs.at[rows(layer * VECS, SENT)], layer_vecs.at[rows(layer * VECS, SENT)], zv_s, zv_r, t,
        ).start)
    finish(zm_r, (LAYERS - 1) * SINGLE)
    for t in range(LAYERS):
        above = layer_maps.at[pl.ds(t * MAPS, PAIR)]
        pl.when(layer < t)(to_layer(above, above, zt_s.at[t], zt_r.at[t], t).wait_recv)
    finish(zv_r, (LAYERS - 1) * SENT)
    entering_x, entering_y, _, _ = chain(LAYERS, layer_maps, layer_vecs, None, None)
    x = jnp.zeros((8, LANES), jnp.float32)
    y = jnp.zeros((8, LANES), jnp.float32)
    for n in range(8):
        if entering_x[n] is not None:
            x = jnp.where(layer == n, entering_x[n], x)
        if entering_y[n] is not None:
            y = jnp.where(layer == n, entering_y[n], y)
    entering_x, entering_y, _, _ = chain(GROUP, maps_in, vecs_in, x, y)
    for n in range(GROUP):
        tail = pltpu.roll(entering_y[n], V, 0)
        entry_out[n * VECS : n * VECS + 8, :] = jnp.where(place < V, entering_x[n], tail)
        entry_out[n * VECS + 8 : n * VECS + 16, :] = tail
    for d in MEMBERS:
        to = lax.rem(member + d, GROUP)
        send(
            entry_out.at[rows(to * VECS, SENT)], entry_in.at[rows(cell(member) * 2 * VECS, SENT)],
            ge_s, ge_r, at_member(d),
        )
    entry_in[rows(cell(member) * 2 * VECS, VECS), :] = entry_out[rows(member * VECS, VECS), :]
    finish(ge_r, (GROUP - 1) * SENT)
    x = jnp.stack([entry_in[every(i, VECS), :] for i in range(V)])
    y = jnp.stack([entry_in[every(V + i, VECS), :] for i in range(V)])
    odd = place % 2 == 1
    x = jnp.where(odd, pltpu.roll(apply(first[3], x) + base[3], 1, 1), x)
    y = jnp.where(odd, pltpu.roll(y, 1, 1), y)
    y = jnp.where(odd, y, pltpu.roll(apply(third[0], y) + apply(second[0], x) + base[0], 7, 1))
    for s in range(4):
        value = base[s]
        for j in range(V):
            value = value + second[s, j] * x[j][None] + third[s, j] * y[j][None]
        for i in range(V):
            out[i, every(s, 4), :] = value[i]

    finish(pitch_s, (PITCH - 1) * SENT)
    finish(side_s, 16)
    finish(gm_s, (GROUP - 1) * USED)
    finish(back_s, (PITCH - 1) * SENT)
    finish(gv_s, (GROUP - 1) * SENT)
    finish(zv_s, (LAYERS - 1) * SENT)
    finish(ge_s, (GROUP - 1) * SENT)
    finish(zm_s, (LAYERS - 1) * SINGLE)
    for t, pair in enumerate(lower_copies):
        pl.when(layer > t)(pair.wait_send)


def body(residual, inverse_diagonal, prior_increment, coupling, characteristic, cutoffs):
    f32 = jnp.float32
    fields = (V, 32, LANES)
    matrices = pltpu.VMEM((4, V, V, 8, LANES), f32)

    def vmem(count):
        return pltpu.VMEM((count, LANES), f32)

    scratch = [
        pltpu.VMEM(fields, f32), pltpu.VMEM((V, V, 32, LANES), f32), pltpu.VMEM(fields, f32),
        pltpu.SMEM((V, 6, V), f32), pltpu.SMEM((2,), jnp.int32),
        pltpu.VMEM((50, 2, 512), f32), pltpu.VMEM((2 * LOW, LANES), jnp.bfloat16), vmem(16),
        pltpu.SemaphoreType.DMA((8,)),
        vmem(8), vmem(8), vmem(8), vmem(8),
        vmem(128), vmem(128), vmem(128), vmem(128), vmem(128),
        vmem(8 * MAPS), vmem(GROUP * MAPS), vmem(MAPS), vmem(LAYERS * MAPS),
        vmem(8 * VECS), vmem(8 * VECS), vmem(GROUP * VECS), vmem(LAYERS * VECS), vmem(GROUP * VECS), vmem(8 * VECS),
        matrices, matrices, matrices, matrices, matrices,
        pltpu.VMEM((V, V, 8, LANES), f32), pltpu.VMEM((V, V, 8, LANES), f32),
        pltpu.VMEM(fields, f32), pltpu.VMEM((4, V, 8, LANES), f32),
        pltpu.VMEM((104, 512), f32), vmem(104 * 8),
        *[pltpu.SemaphoreType.DMA] * 16, *[pltpu.SemaphoreType.DMA((LAYERS,))] * 2,
    ]
    inside = pl.BlockSpec(memory_space=pltpu.VMEM)
    outside = pl.BlockSpec(memory_space=pl.ANY)
    high_low, turns = table()
    result = pl.pallas_call(
        kernel,
        out_shape=pltpu.VMEM(fields, f32),
        in_specs=[outside] * 8,
        out_specs=inside,
        scratch_shapes=scratch,
        compiler_params=pltpu.CompilerParams(collective_id=0, has_side_effects=True),
    )(
        residual.reshape(fields),
        inverse_diagonal.reshape(V, V, 32, LANES),
        prior_increment.reshape(fields),
        coupling.transpose(1, 0, 2),
        characteristic.transpose(0, 3, 4, 1, 2).reshape(50, 2, 512),
        cutoffs,
        jnp.asarray(high_low),
        jnp.asarray(turns),
    )
    return result.reshape(V, GROUP, 8, LANES)


def solution(mesh):
    field = P(None, None, "span", "pitch")
    return jax.shard_map(
        body, mesh=mesh,
        in_specs=(field, P(None, None, None, "span", "pitch"), field, P(), P(), P()),
        out_specs=field, check_vma=False,
    )
```

```python
import functools

import jax
import jax.numpy as jnp
import numpy as np
from jax import lax
from jax.experimental import pallas as pl
from jax.experimental.pallas import tpu as pltpu
from jax.sharding import PartitionSpec as P

NP = 1024
PITCH = 8
GROUP = 4
LAYERS = 8
V = 5
LINE = 16
MAPS = 88
B, C, A = 0, 25, 56
PAIR, SINGLE, USED = 50, 25, 81
VECS = 16
SENT = 10
LANES = 128

FORWARD, BACK_RE, BACK_IM, LOW = 0, 256, 384, 512
HALF = float(np.sqrt(0.5))


def table():
    two_pi = 2.0 * np.pi
    a = np.arange(8)
    b = np.arange(128)
    k2 = np.arange(64)
    twiddle = two_pi * np.outer(a, b) / NP
    lanes = two_pi * (np.outer(b, k2) % 128) / 128
    cos, sin = np.cos(lanes), np.sin(lanes)
    forward = np.block([[cos, -sin], [sin, cos]])
    back_re = np.concatenate([cos.T, -sin.T], 0)
    back_im = np.concatenate([sin.T, cos.T], 0)
    parts = [forward, back_re, back_im]
    whole = np.concatenate(parts, 0).astype(np.float32)
    high = whole.astype(jnp.bfloat16)
    low = (whole - high.astype(np.float32)).astype(jnp.bfloat16)
    turns = np.concatenate([np.cos(twiddle), np.sin(twiddle)], 0).astype(np.float32)
    return np.concatenate([high, low], 0), turns


FAR_FIRST = (4, 3, 5, 2, 6, 1, 7)
MEMBERS = (2, 1, 3)


def every(start, stride):
    return pl.ds(start, 8, stride=stride)


def rows(start, size):
    return pl.ds(pl.multiple_of(start, 8), size)


def product(later, earlier):
    total = later[0][None] * earlier[:, 0][:, None]
    for j in range(1, V):
        total = total + later[j][None] * earlier[:, j][:, None]
    return total


def apply(matrix, vector):
    total = matrix[0] * vector[0][None]
    for j in range(1, V):
        total = total + matrix[j] * vector[j][None]
    return total


def scaled(block, coupling, which):
    columns = []
    for k in range(V):
        total = block[:, 0] * (-coupling[0, which, k])
        for j in range(1, V):
            total = total + block[:, j] * (-coupling[j, which, k])
        columns.append(total)
    return jnp.stack(columns)


def times(data, const, start, size):
    data_high = data.astype(jnp.bfloat16)
    data_low = (data - data_high.astype(jnp.float32)).astype(jnp.bfloat16)
    high = const[start : start + size, :]
    low = const[LOW + start : LOW + start + size, :]
    total = jnp.dot(data_high, high, preferred_element_type=jnp.float32)
    total = total + jnp.dot(data_low, high, preferred_element_type=jnp.float32)
    return total + jnp.dot(data_high, low, preferred_element_type=jnp.float32)


def eight_forward(x):
    s0, d0, s2, d2 = x[0] + x[4], x[0] - x[4], x[2] + x[6], x[2] - x[6]
    s1, d1, s3, d3 = x[1] + x[5], x[1] - x[5], x[3] + x[7], x[3] - x[7]
    even, odd = s0 + s2, s1 + s3
    real, imag = s0 - s2, s3 - s1
    near, far = HALF * (d1 - d3), HALF * (d1 + d3)
    zero = jnp.zeros_like(even)
    first = (d0 + near, -(d2 + far))
    third = (d0 - near, d2 - far)
    return [
        (even + odd, zero), first, (real, imag), third,
        (even - odd, zero), (third[0], -third[1]), (real, -imag), (first[0], -first[1]),
    ]


def eight_back(re, im):
    p1, p2, p3 = re[1] + re[7], re[2] + re[6], re[3] + re[5]
    q1, q2, q3 = im[1] - im[7], im[2] - im[6], im[3] - im[5]
    total, gap = re[0] + re[4], re[0] - re[4]
    both, part = p1 + p3, HALF * (p1 - p3)
    cross, lean = q1 - q3, HALF * (q1 + q3)
    return [
        total + p2 + both, gap - q2 + part - lean, total - p2 - cross, gap + q2 - part - lean,
        total + p2 - both, gap - q2 - part + lean, total - p2 + cross, gap + q2 + part + lean,
    ]


def kernel(
    residual_in, inverse_in, prior_in, coupling_in, characteristic_in, cutoffs_in, const_in, turns_in, out,
    residual, inverse, prior, coupling, cutoffs, characteristic, const, turns, load_s,
    lower, upper, edge_low, edge_high, planes_out, planes_in, ordered, corr_out, corr_in,
    maps_out, maps_in, packed, layer_maps, vecs_early, vecs_out, vecs_in, layer_vecs, entry_out, entry_in,
    down, up, first, second, third, next_reach, next_both, source, base, flat, spectra,
    pitch_s, pitch_r, back_s, back_r, side_s, side_r,
    gm_s, gm_r, zm_s, zm_r, gv_s, gv_r, zv_s, zv_r, ge_s, ge_r, zt_s, zt_r,
):
    pitch = lax.axis_index("pitch")
    span = lax.axis_index("span")
    layer = span // GROUP
    member = span % GROUP

    def cell(m):
        return (1 - m // 2) * (1 - m) + m // 2 * m

    def at_pitch(d):
        return {"pitch": lax.rem(pitch + d, PITCH), "span": span}

    def at_member(d):
        return {"pitch": pitch, "span": layer * GROUP + lax.rem(member + d, GROUP)}

    def at_layer(d):
        return {"pitch": pitch, "span": lax.rem(layer + d, LAYERS) * GROUP + member}

    peers = [at_pitch(d) for d in range(1, PITCH)]
    peers += [at_member(d) for d in range(1, GROUP)]
    peers += [at_layer(d) for d in range(1, LAYERS)]
    loads = [pltpu.make_async_copy(residual_in, residual, load_s.at[0])]
    loads[0].start()
    barrier = pltpu.get_barrier_semaphore()
    for peer in peers:
        pl.semaphore_signal(barrier, inc=1, device_id=peer, device_id_type=pl.DeviceIdType.MESH)

    for n, (src, dst) in enumerate((
        (prior_in, prior), (inverse_in, inverse),
        (characteristic_in, characteristic), (const_in, const), (turns_in, turns),
        (coupling_in, coupling), (cutoffs_in, cutoffs),
    )):
        loads.append(pltpu.make_async_copy(src, dst, load_s.at[n + 1]))
        loads[-1].start()

    def send(src, dst, send_sem, recv_sem, peer):
        copy = pltpu.make_async_remote_copy(
            src_ref=src, dst_ref=dst, send_sem=send_sem, recv_sem=recv_sem,
            device_id=peer, device_id_type=pl.DeviceIdType.MESH,
        )
        copy.start()

    def to_layer(src, dst, send_sem, recv_sem, t):
        return pltpu.make_async_remote_copy(
            src_ref=src, dst_ref=dst, send_sem=send_sem, recv_sem=recv_sem,
            device_id={"pitch": pitch, "span": t * GROUP + member}, device_id_type=pl.DeviceIdType.MESH,
        )

    def finish(sem, count):
        area = maps_out.at[pl.ds(0, count)]
        pltpu.make_async_copy(area, area, sem).wait()

    loads[0].wait()
    for q, axial in enumerate((0, GROUP - 1)):
        for j in range(V):
            planes_out[every(q * V + j, LINE), :] = residual[j, axial * 8 : axial * 8 + 8, :]

    loads[2].wait()
    loads[6].wait()
    reach = None
    for s in range(4):
        block = inverse[:, :, every(s, 4), :]
        down[s] = scaled(block, coupling, 0)
        up[s] = scaled(block, coupling, 1)
        reach = down[s] if s == 0 else product(down[s], reach)
        first[s] = reach

    pl.semaphore_wait(barrier, len(peers))

    for d in FAR_FIRST:
        to = lax.rem(pitch + d, PITCH)
        send(
            planes_out.at[rows(to * LINE, SENT)], planes_in.at[rows(pitch * LINE, SENT)],
            pitch_s, pitch_r, at_pitch(d),
        )
    reach = first[3]
    both = reach
    trail = up[3]
    second[3] = both
    third[3] = trail
    for s in (2, 1, 0):
        both = first[s] + product(up[s], both)
        trail = product(up[s], trail)
        second[s] = both
        third[s] = trail
    upper_reach = pltpu.roll(reach, 7, 2)
    upper_both = pltpu.roll(both, 7, 2)
    next_reach[...] = upper_reach
    next_both[...] = upper_both
    both = both + product(trail, product(upper_both, reach))
    trail = product(trail, pltpu.roll(trail, 7, 2))
    reach = product(upper_reach, reach)
    for k in range(V):
        for i in range(V):
            maps_out[every(A + V * k + i, MAPS), :] = reach[k, i]
            maps_out[every(B + V * k + i, MAPS), :] = trail[k, i]
            maps_out[every(C + V * k + i, MAPS), :] = both[k, i]
    for d in MEMBERS:
        to = lax.rem(member + d, GROUP)
        send(
            maps_out.at[rows(cell(to) * 2 * MAPS, USED)], maps_in.at[rows(member * MAPS, USED)],
            gm_s, gm_r, at_member(d),
        )
    loads[1].wait()
    column = lax.broadcasted_iota(jnp.int32, (8, LANES), 1)
    last = initial = jnp.zeros((8, LANES), jnp.float32)
    for n in range(V * GROUP):
        tile = prior[n // GROUP, n % GROUP * 8 : n % GROUP * 8 + 8, :]
        last = jnp.where(column == n, pltpu.roll(tile, n + 1, 1), last)
        initial = jnp.where(column == n, pltpu.roll(tile, n, 1) if n else tile, initial)
    edge_high[...] = last
    edge_low[...] = initial
    send(edge_high, lower, side_s, side_r, at_pitch(1))
    send(edge_low, upper, side_s, side_r, at_pitch(PITCH - 1))

    planes_in[rows(pitch * LINE, LINE), :] = planes_out[rows(pitch * LINE, LINE), :]
    maps_in[rows(member * MAPS, MAPS), :] = maps_out[rows(cell(member) * 2 * MAPS, MAPS), :]

    loads[3].wait()
    flat[100:104, :] = jnp.zeros((4, 512), jnp.float32)
    for n in range(50):
        flat[2 * n : 2 * n + 2, :] = characteristic[n]
    whole = flat[...]
    high = whole.astype(jnp.bfloat16)
    rest = whole - high.astype(jnp.float32)
    middle = rest.astype(jnp.bfloat16)
    low = (rest - middle.astype(jnp.float32)).astype(jnp.bfloat16)
    harmonic = lax.broadcasted_iota(jnp.int32, (512, LANES), 0)
    lane = lax.broadcasted_iota(jnp.int32, (512, LANES), 1)
    apart = harmonic - 8 * (lane % 64)
    for k1 in range(8):
        pick = jnp.where(apart == k1, 1.0, 0.0).astype(jnp.bfloat16)
        part = jnp.dot(high, pick, preferred_element_type=jnp.float32)
        part = part + jnp.dot(middle, pick, preferred_element_type=jnp.float32)
        part = part + jnp.dot(low, pick, preferred_element_type=jnp.float32)
        spectra[pl.ds(k1, 104, stride=8), :] = part

    finish(pitch_r, (PITCH - 1) * SENT)
    for load in (loads[4], loads[5], loads[7]):
        load.wait()
    turned_re, turned_im = [], []
    parts = eight_forward([planes_in[a * LINE : a * LINE + LINE, :] for a in range(8)])
    for k1, (re, im) in enumerate(parts):
        turn_re, turn_im = turns[k1 : k1 + 1, :], turns[8 + k1 : 9 + k1, :]
        turned_re.append(re * turn_re + im * turn_im)
        turned_im.append(im * turn_re - re * turn_im)
    turned = jnp.concatenate([jnp.concatenate(turned_re, 0), jnp.concatenate(turned_im, 0)], 1)
    ordered[...] = times(turned, const, FORWARD, 256)
    spectrum = jnp.concatenate([ordered[every(line, LINE), :] for line in range(2 * V)], 0)
    number = lax.broadcasted_iota(jnp.int32, (8, LANES), 0) + 8 * (lax.broadcasted_iota(jnp.int32, (8, LANES), 1) % 64)
    weight = jnp.where(number == 0, 1.0, 2.0) / NP
    sign = jnp.where(lax.broadcasted_iota(jnp.int32, (80, LANES), 1) < 64, -1.0, 1.0)
    crossed = (pltpu.roll(spectrum, 64, 1) * sign).reshape(2, V, 8, LANES)
    spectrum = spectrum.reshape(2, V, 8, LANES)
    for q in range(2):
        factor = jnp.where(number < cutoffs[q], weight, 0.0)
        for i in range(V):
            total = None
            for j in range(V):
                row = (q * 25 + i * V + j) * 16
                term = spectra[row : row + 8, :] * spectrum[q, j] + spectra[row + 8 : row + 16, :] * crossed[q, j]
                total = term if total is None else total + term
            ordered[every(q * V + i, LINE), :] = total * factor
    corrected = ordered[...]
    back_re = times(corrected, const, BACK_RE, 128)
    back_im = times(corrected, const, BACK_IM, 128)
    lines_re, lines_im = [], []
    for k1 in range(8):
        turn_re, turn_im = turns[k1 : k1 + 1, :], turns[8 + k1 : 9 + k1, :]
        re, im = back_re[k1 * LINE : k1 * LINE + LINE], back_im[k1 * LINE : k1 * LINE + LINE]
        lines_re.append(re * turn_re - im * turn_im)
        lines_im.append(im * turn_re + re * turn_im)
    for a, value in enumerate(eight_back(lines_re, lines_im)):
        corr_out[a * LINE : a * LINE + LINE, :] = value
    for d in FAR_FIRST:
        to = lax.rem(pitch + d, PITCH)
        send(
            corr_out.at[rows(to * LINE, SENT)], corr_in.at[rows(pitch * LINE, SENT)],
            back_s, back_r, at_pitch(d),
        )
    corr_in[rows(pitch * LINE, LINE), :] = corr_out[rows(pitch * LINE, LINE), :]

    place = lax.broadcasted_iota(jnp.int32, (8, LANES), 0)

    def tiles(ref, n, which):
        start = n * MAPS + which
        return [ref[start + V * j : start + V * j + 8, :] for j in range(V)]

    def spread_rows(vector):
        return [jnp.broadcast_to(vector[..., j : j + 1, :], vector.shape) for j in range(V)]

    def mix(matrix, parts):
        total = matrix[0] * parts[0]
        for j in range(1, V):
            total = total + matrix[j] * parts[j]
        return total

    finish(gm_r, (GROUP - 1) * USED)
    forward = jnp.stack(tiles(maps_in, 0, A))
    across = [jnp.stack(tiles(maps_in, 0, C))]
    for n in range(1, GROUP):
        parts = spread_rows(forward)
        forward = mix(tiles(maps_in, n, A), parts)
        across.append(mix(tiles(maps_in, n, C), parts))
    backward = jnp.concatenate([jnp.stack(tiles(maps_in, GROUP - 1, B)), across[GROUP - 1]], 0)
    for n in range(GROUP - 2, -1, -1):
        backward = mix(tiles(maps_in, n, B), spread_rows(backward))
        backward = jnp.concatenate([backward[:V], backward[V:] + across[n]], 0)
    columns = jnp.concatenate([forward, backward], 0)
    for n in range(3 * V):
        start = A + V * n if n < V else V * n - 25
        packed[start : start + 8, :] = columns[n]
    layer_maps[rows(layer * MAPS, MAPS), :] = packed[...]
    for t in range(LAYERS):
        single = to_layer(
            layer_maps.at[rows(layer * MAPS + A, SINGLE)], layer_maps.at[rows(layer * MAPS + A, SINGLE)], zm_s, zm_r, t,
        )
        pl.when(layer != t)(single.start)
        pair = to_layer(
            layer_maps.at[rows(layer * MAPS, PAIR)], layer_maps.at[rows(layer * MAPS, PAIR)], zt_s, zt_r, t,
        )
        pl.when(layer > t)(pair.start)

    finish(side_r, 16)
    own = prior[...]
    below, above = [], []
    for i in range(V):
        low_tiles, high_tiles = [], []
        for a in range(GROUP):
            n = i * GROUP + a
            tile = prior[i, a * 8 : a * 8 + 8, :]
            edge = pltpu.roll(lower[...], LANES - n, 1) if n else lower[...]
            low_tiles.append(jnp.where(column == 0, edge, pltpu.roll(tile, 1, 1)))
            edge = pltpu.roll(upper[...], LANES - 1 - n, 1)
            high_tiles.append(jnp.where(column == LANES - 1, edge, pltpu.roll(tile, LANES - 1, 1)))
        below.append(jnp.concatenate(low_tiles, 0))
        above.append(jnp.concatenate(high_tiles, 0))
    zero_row = jnp.zeros((8, LANES), jnp.float32)
    for i in range(V):
        total = residual[i]
        before = after = None
        for j in range(V):
            total = total - coupling[i, 2, j] * below[j] - coupling[i, 3, j] * above[j]
            low_term = coupling[i, 4, j] * own[j]
            high_term = coupling[i, 5, j] * own[j]
            before = low_term if before is None else before + low_term
            after = high_term if after is None else after + high_term
        total = total - jnp.concatenate([zero_row, before[:24]], 0) - jnp.concatenate([after[8:], zero_row], 0)
        source[i] = total

    def sweep(offsets, parity):
        star = None
        for s in range(4):
            block = inverse[:, :, every(s, 4), :]
            rhs = source[:, every(s, 4), :]
            value = block[:, 0] * rhs[0][None]
            for j in range(1, V):
                value = value + block[:, j] * rhs[j][None]
            star = value if s == 0 else value + apply(down[s], star)
            base[s] = star
        update = star
        for s in (2, 1, 0):
            update = base[s] + apply(up[s], update)
            base[s] = update
        ahead = pltpu.roll(star, 7, 1) + apply(next_reach, star)
        behind = update + apply(third[0], pltpu.roll(update, 7, 1) + apply(next_both, star))
        for i in range(V):
            offsets[every(i, VECS), :] = ahead[i]
            offsets[every(V + i, VECS), :] = behind[i]
        for d in MEMBERS:
            to = lax.rem(member + d, GROUP)
            copy = pltpu.make_async_remote_copy(
                src_ref=offsets.at[rows(cell(to) * 2 * VECS, SENT)], dst_ref=vecs_in.at[rows(member * VECS, SENT)],
                send_sem=gv_s, recv_sem=gv_r,
                device_id=at_member(d), device_id_type=pl.DeviceIdType.MESH,
            )
            pl.when(lax.rem(to, 2) == parity)(copy.start)

    sweep(vecs_early, 0)

    finish(back_r, (PITCH - 1) * SENT)
    for j in range(V):
        source[j, 0:8, :] = source[j, 0:8, :] + corr_in[every(j, LINE), :]
        source[j, 24:32, :] = source[j, 24:32, :] + corr_in[every(V + j, LINE), :]
    sweep(vecs_out, 1)
    vecs_in[rows(member * VECS, VECS), :] = vecs_out[rows(cell(member) * 2 * VECS, VECS), :]

    def chain(count, maps_ref, vecs_ref, x, y):
        entering_x, entering_y, crossing = [], [None] * count, []
        for n in range(count):
            entering_x.append(x)
            offset = vecs_ref[n * VECS : n * VECS + 8, :]
            if x is None:
                crossing.append(vecs_ref[n * VECS + V : n * VECS + V + 8, :])
                x = offset
            else:
                parts = spread_rows(x)
                ahead = mix(tiles(maps_ref, n, A), parts)
                crossing.append(mix(tiles(maps_ref, n, C), parts) + vecs_ref[n * VECS + V : n * VECS + V + 8, :])
                x = ahead + offset
        for n in range(count - 1, -1, -1):
            entering_y[n] = y
            y = crossing[n] if y is None else mix(tiles(maps_ref, n, B), spread_rows(y)) + crossing[n]
        return entering_x, entering_y, x, y

    finish(gv_r, (GROUP - 1) * SENT)
    _, _, x, y = chain(GROUP, maps_in, vecs_in, None, None)
    tail = pltpu.roll(y, V, 0)
    layer_vecs[rows(layer * VECS, 8), :] = jnp.where(place < V, x, tail)
    layer_vecs[rows(layer * VECS + 8, 8), :] = tail
    for t in range(LAYERS):
        pl.when(layer != t)(to_layer(
            layer_vecs.at[rows(layer * VECS, SENT)], layer_vecs.at[rows(layer * VECS, SENT)], zv_s, zv_r, t,
        ).start)
    finish(zm_r, (LAYERS - 1) * SINGLE)
    for t in range(LAYERS - 1):
        pl.when(layer == t)(functools.partial(finish, zt_r, (LAYERS - 1 - t) * PAIR))
    finish(zv_r, (LAYERS - 1) * SENT)
    entering_x, entering_y, _, _ = chain(LAYERS, layer_maps, layer_vecs, None, None)
    x = jnp.zeros((8, LANES), jnp.float32)
    y = jnp.zeros((8, LANES), jnp.float32)
    for n in range(8):
        if entering_x[n] is not None:
            x = jnp.where(layer == n, entering_x[n], x)
        if entering_y[n] is not None:
            y = jnp.where(layer == n, entering_y[n], y)
    entering_x, entering_y, _, _ = chain(GROUP, maps_in, vecs_in, x, y)
    for n in range(GROUP):
        tail = pltpu.roll(entering_y[n], V, 0)
        entry_out[n * VECS : n * VECS + 8, :] = jnp.where(place < V, entering_x[n], tail)
        entry_out[n * VECS + 8 : n * VECS + 16, :] = tail
    for d in MEMBERS:
        to = lax.rem(member + d, GROUP)
        send(
            entry_out.at[rows(to * VECS, SENT)], entry_in.at[rows(cell(member) * 2 * VECS, SENT)],
            ge_s, ge_r, at_member(d),
        )
    entry_in[rows(cell(member) * 2 * VECS, VECS), :] = entry_out[rows(member * VECS, VECS), :]
    finish(ge_r, (GROUP - 1) * SENT)
    x = jnp.stack([entry_in[every(i, VECS), :] for i in range(V)])
    y = jnp.stack([entry_in[every(V + i, VECS), :] for i in range(V)])
    odd = place % 2 == 1
    x = jnp.where(odd, pltpu.roll(apply(first[3], x) + base[3], 1, 1), x)
    y = jnp.where(odd, pltpu.roll(y, 1, 1), y)
    y = jnp.where(odd, y, pltpu.roll(apply(third[0], y) + apply(second[0], x) + base[0], 7, 1))
    for s in range(4):
        value = base[s]
        for j in range(V):
            value = value + second[s, j] * x[j][None] + third[s, j] * y[j][None]
        for i in range(V):
            out[i, every(s, 4), :] = value[i]

    finish(pitch_s, (PITCH - 1) * SENT)
    finish(side_s, 16)
    finish(gm_s, (GROUP - 1) * USED)
    finish(back_s, (PITCH - 1) * SENT)
    finish(gv_s, (GROUP - 1) * SENT)
    finish(zv_s, (LAYERS - 1) * SENT)
    finish(ge_s, (GROUP - 1) * SENT)
    finish(zm_s, (LAYERS - 1) * SINGLE)
    for t in range(1, LAYERS):
        pl.when(layer == t)(functools.partial(finish, zt_s, t * PAIR))


def body(residual, inverse_diagonal, prior_increment, coupling, characteristic, cutoffs):
    f32 = jnp.float32
    fields = (V, 32, LANES)
    matrices = pltpu.VMEM((4, V, V, 8, LANES), f32)

    def vmem(count):
        return pltpu.VMEM((count, LANES), f32)

    scratch = [
        pltpu.VMEM(fields, f32), pltpu.VMEM((V, V, 32, LANES), f32), pltpu.VMEM(fields, f32),
        pltpu.SMEM((V, 6, V), f32), pltpu.SMEM((2,), jnp.int32),
        pltpu.VMEM((50, 2, 512), f32), pltpu.VMEM((2 * LOW, LANES), jnp.bfloat16), vmem(16),
        pltpu.SemaphoreType.DMA((8,)),
        vmem(8), vmem(8), vmem(8), vmem(8),
        vmem(128), vmem(128), vmem(128), vmem(128), vmem(128),
        vmem(8 * MAPS), vmem(GROUP * MAPS), vmem(MAPS), vmem(LAYERS * MAPS),
        vmem(8 * VECS), vmem(8 * VECS), vmem(GROUP * VECS), vmem(LAYERS * VECS), vmem(GROUP * VECS), vmem(8 * VECS),
        matrices, matrices, matrices, matrices, matrices,
        pltpu.VMEM((V, V, 8, LANES), f32), pltpu.VMEM((V, V, 8, LANES), f32),
        pltpu.VMEM(fields, f32), pltpu.VMEM((4, V, 8, LANES), f32),
        pltpu.VMEM((104, 512), f32), vmem(104 * 8),
        *[pltpu.SemaphoreType.DMA] * 18,
    ]
    inside = pl.BlockSpec(memory_space=pltpu.VMEM)
    outside = pl.BlockSpec(memory_space=pl.ANY)
    high_low, turns = table()
    result = pl.pallas_call(
        kernel,
        out_shape=pltpu.VMEM(fields, f32),
        in_specs=[outside] * 8,
        out_specs=inside,
        scratch_shapes=scratch,
        compiler_params=pltpu.CompilerParams(collective_id=0, has_side_effects=True),
    )(
        residual.reshape(fields),
        inverse_diagonal.reshape(V, V, 32, LANES),
        prior_increment.reshape(fields),
        coupling.transpose(1, 0, 2),
        characteristic.transpose(0, 3, 4, 1, 2).reshape(50, 2, 512),
        cutoffs,
        jnp.asarray(high_low),
        jnp.asarray(turns),
    )
    return result.reshape(V, GROUP, 8, LANES)


def solution(mesh):
    field = P(None, None, "span", "pitch")
    return jax.shard_map(
        body, mesh=mesh,
        in_specs=(field, P(None, None, None, "span", "pitch"), field, P(), P(), P()),
        out_specs=field, check_vma=False,
    )
```

```python
import functools

import jax
import jax.numpy as jnp
import numpy as np
from jax import lax
from jax.experimental import pallas as pl
from jax.experimental.pallas import tpu as pltpu
from jax.sharding import PartitionSpec as P

NP = 1024
PITCH = 8
GROUP = 4
LAYERS = 8
V = 5
LINE = 16
MAPS = 88
B, C, A = 0, 25, 56
PAIR, SINGLE, USED = 50, 25, 81
VECS = 16
SENT = 10
LANES = 128

FORWARD, BACK_RE, BACK_IM, LOW = 0, 256, 384, 512
HALF = float(np.sqrt(0.5))


def table():
    two_pi = 2.0 * np.pi
    a = np.arange(8)
    b = np.arange(128)
    k2 = np.arange(64)
    twiddle = two_pi * np.outer(a, b) / NP
    lanes = two_pi * (np.outer(b, k2) % 128) / 128
    cos, sin = np.cos(lanes), np.sin(lanes)
    forward = np.block([[cos, -sin], [sin, cos]])
    back_re = np.concatenate([cos.T, -sin.T], 0)
    back_im = np.concatenate([sin.T, cos.T], 0)
    parts = [forward, back_re, back_im]
    whole = np.concatenate(parts, 0).astype(np.float32)
    high = whole.astype(jnp.bfloat16)
    low = (whole - high.astype(np.float32)).astype(jnp.bfloat16)
    turns = np.concatenate([np.cos(twiddle), np.sin(twiddle)], 0).astype(np.float32)
    return np.concatenate([high, low], 0), turns


FAR_FIRST = (4, 3, 5, 2, 6, 1, 7)
MEMBERS = (2, 1, 3)


def every(start, stride):
    return pl.ds(start, 8, stride=stride)


def rows(start, size):
    return pl.ds(pl.multiple_of(start, 8), size)


def product(later, earlier):
    total = later[0][None] * earlier[:, 0][:, None]
    for j in range(1, V):
        total = total + later[j][None] * earlier[:, j][:, None]
    return total


def apply(matrix, vector):
    total = matrix[0] * vector[0][None]
    for j in range(1, V):
        total = total + matrix[j] * vector[j][None]
    return total


def scaled(block, coupling, which):
    columns = []
    for k in range(V):
        total = block[:, 0] * (-coupling[0, which, k])
        for j in range(1, V):
            total = total + block[:, j] * (-coupling[j, which, k])
        columns.append(total)
    return jnp.stack(columns)


def times(data, const, start, size):
    data_high = data.astype(jnp.bfloat16)
    data_low = (data - data_high.astype(jnp.float32)).astype(jnp.bfloat16)
    high = const[start : start + size, :]
    low = const[LOW + start : LOW + start + size, :]
    total = jnp.dot(data_high, high, preferred_element_type=jnp.float32)
    total = total + jnp.dot(data_low, high, preferred_element_type=jnp.float32)
    return total + jnp.dot(data_high, low, preferred_element_type=jnp.float32)


def eight_forward(x):
    s0, d0, s2, d2 = x[0] + x[4], x[0] - x[4], x[2] + x[6], x[2] - x[6]
    s1, d1, s3, d3 = x[1] + x[5], x[1] - x[5], x[3] + x[7], x[3] - x[7]
    even, odd = s0 + s2, s1 + s3
    real, imag = s0 - s2, s3 - s1
    near, far = HALF * (d1 - d3), HALF * (d1 + d3)
    zero = jnp.zeros_like(even)
    first = (d0 + near, -(d2 + far))
    third = (d0 - near, d2 - far)
    return [
        (even + odd, zero), first, (real, imag), third,
        (even - odd, zero), (third[0], -third[1]), (real, -imag), (first[0], -first[1]),
    ]


def eight_back(re, im):
    p1, p2, p3 = re[1] + re[7], re[2] + re[6], re[3] + re[5]
    q1, q2, q3 = im[1] - im[7], im[2] - im[6], im[3] - im[5]
    total, gap = re[0] + re[4], re[0] - re[4]
    both, part = p1 + p3, HALF * (p1 - p3)
    cross, lean = q1 - q3, HALF * (q1 + q3)
    return [
        total + p2 + both, gap - q2 + part - lean, total - p2 - cross, gap + q2 - part - lean,
        total + p2 - both, gap - q2 - part + lean, total - p2 + cross, gap + q2 + part + lean,
    ]


def kernel(
    residual_in, inverse_in, prior_in, coupling_in, characteristic_in, cutoffs_in, const_in, turns_in, out,
    residual, inverse, prior, coupling, cutoffs, characteristic, const, turns, load_s,
    lower, upper, edge_low, edge_high, planes_out, planes_in, ordered, corr_out, corr_in,
    maps_out, maps_in, packed, layer_maps, vecs_early, vecs_out, vecs_in, layer_vecs, entry_out, entry_in,
    down, up, first, second, third, next_reach, next_both, source, base, flat, spectra,
    pitch_s, pitch_r, back_s, back_r, side_s, side_r,
    gm_s, gm_r, zm_s, zm_r, gv_s, gv_r, zv_s, zv_r, ge_s, ge_r, zt_s, zt_r, ready,
):
    pitch = lax.axis_index("pitch")
    span = lax.axis_index("span")
    layer = span // GROUP
    member = span % GROUP

    def cell(m):
        return (1 - m // 2) * (1 - m) + m // 2 * m

    def at_pitch(d):
        return {"pitch": lax.rem(pitch + d, PITCH), "span": span}

    def at_member(d):
        return {"pitch": pitch, "span": layer * GROUP + lax.rem(member + d, GROUP)}

    def at_layer(d):
        return {"pitch": pitch, "span": lax.rem(layer + d, LAYERS) * GROUP + member}

    peers = [at_pitch(d) for d in range(1, PITCH)]
    peers += [at_member(d) for d in range(1, GROUP)]
    near = [at_layer(d) for d in (1, 2, LAYERS - 2, LAYERS - 1)]
    peers += near
    loads = [pltpu.make_async_copy(residual_in, residual, load_s.at[0])]
    loads[0].start()
    barrier = pltpu.get_barrier_semaphore()
    for peer in peers:
        pl.semaphore_signal(barrier, inc=1, device_id=peer, device_id_type=pl.DeviceIdType.MESH)

    for n, (src, dst) in enumerate((
        (prior_in, prior), (inverse_in, inverse),
        (characteristic_in, characteristic), (const_in, const), (turns_in, turns),
        (coupling_in, coupling), (cutoffs_in, cutoffs),
    )):
        loads.append(pltpu.make_async_copy(src, dst, load_s.at[n + 1]))
        loads[-1].start()

    def send(src, dst, send_sem, recv_sem, peer):
        copy = pltpu.make_async_remote_copy(
            src_ref=src, dst_ref=dst, send_sem=send_sem, recv_sem=recv_sem,
            device_id=peer, device_id_type=pl.DeviceIdType.MESH,
        )
        copy.start()

    def to_layer(src, dst, send_sem, recv_sem, t):
        return pltpu.make_async_remote_copy(
            src_ref=src, dst_ref=dst, send_sem=send_sem, recv_sem=recv_sem,
            device_id={"pitch": pitch, "span": t * GROUP + member}, device_id_type=pl.DeviceIdType.MESH,
        )

    def finish(sem, count):
        area = maps_out.at[pl.ds(0, count)]
        pltpu.make_async_copy(area, area, sem).wait()

    loads[0].wait()
    for q, axial in enumerate((0, GROUP - 1)):
        for j in range(V):
            planes_out[every(q * V + j, LINE), :] = residual[j, axial * 8 : axial * 8 + 8, :]

    loads[2].wait()
    loads[6].wait()
    reach = None
    for s in range(4):
        block = inverse[:, :, every(s, 4), :]
        down[s] = scaled(block, coupling, 0)
        up[s] = scaled(block, coupling, 1)
        reach = down[s] if s == 0 else product(down[s], reach)
        first[s] = reach

    pl.semaphore_wait(barrier, len(peers))

    for d in FAR_FIRST:
        to = lax.rem(pitch + d, PITCH)
        send(
            planes_out.at[rows(to * LINE, SENT)], planes_in.at[rows(pitch * LINE, SENT)],
            pitch_s, pitch_r, at_pitch(d),
        )
    reach = first[3]
    both = reach
    trail = up[3]
    second[3] = both
    third[3] = trail
    for s in (2, 1, 0):
        both = first[s] + product(up[s], both)
        trail = product(up[s], trail)
        second[s] = both
        third[s] = trail
    upper_reach = pltpu.roll(reach, 7, 2)
    upper_both = pltpu.roll(both, 7, 2)
    next_reach[...] = upper_reach
    next_both[...] = upper_both
    both = both + product(trail, product(upper_both, reach))
    trail = product(trail, pltpu.roll(trail, 7, 2))
    reach = product(upper_reach, reach)
    for k in range(V):
        for i in range(V):
            maps_out[every(A + V * k + i, MAPS), :] = reach[k, i]
            maps_out[every(B + V * k + i, MAPS), :] = trail[k, i]
            maps_out[every(C + V * k + i, MAPS), :] = both[k, i]
    for d in MEMBERS:
        to = lax.rem(member + d, GROUP)
        send(
            maps_out.at[rows(cell(to) * 2 * MAPS, USED)], maps_in.at[rows(member * MAPS, USED)],
            gm_s, gm_r, at_member(d),
        )
    for peer in near:
        pl.semaphore_signal(ready, inc=1, device_id=peer, device_id_type=pl.DeviceIdType.MESH)
    loads[1].wait()
    column = lax.broadcasted_iota(jnp.int32, (8, LANES), 1)
    last = initial = jnp.zeros((8, LANES), jnp.float32)
    for n in range(V * GROUP):
        tile = prior[n // GROUP, n % GROUP * 8 : n % GROUP * 8 + 8, :]
        last = jnp.where(column == n, pltpu.roll(tile, n + 1, 1), last)
        initial = jnp.where(column == n, pltpu.roll(tile, n, 1) if n else tile, initial)
    edge_high[...] = last
    edge_low[...] = initial
    send(edge_high, lower, side_s, side_r, at_pitch(1))
    send(edge_low, upper, side_s, side_r, at_pitch(PITCH - 1))

    planes_in[rows(pitch * LINE, LINE), :] = planes_out[rows(pitch * LINE, LINE), :]
    maps_in[rows(member * MAPS, MAPS), :] = maps_out[rows(cell(member) * 2 * MAPS, MAPS), :]

    loads[3].wait()
    flat[100:104, :] = jnp.zeros((4, 512), jnp.float32)
    for n in range(50):
        flat[2 * n : 2 * n + 2, :] = characteristic[n]
    whole = flat[...]
    high = whole.astype(jnp.bfloat16)
    rest = whole - high.astype(jnp.float32)
    middle = rest.astype(jnp.bfloat16)
    low = (rest - middle.astype(jnp.float32)).astype(jnp.bfloat16)
    harmonic = lax.broadcasted_iota(jnp.int32, (512, LANES), 0)
    lane = lax.broadcasted_iota(jnp.int32, (512, LANES), 1)
    apart = harmonic - 8 * (lane % 64)
    for k1 in range(8):
        pick = jnp.where(apart == k1, 1.0, 0.0).astype(jnp.bfloat16)
        part = jnp.dot(high, pick, preferred_element_type=jnp.float32)
        part = part + jnp.dot(middle, pick, preferred_element_type=jnp.float32)
        part = part + jnp.dot(low, pick, preferred_element_type=jnp.float32)
        spectra[pl.ds(k1, 104, stride=8), :] = part

    finish(pitch_r, (PITCH - 1) * SENT)
    for load in (loads[4], loads[5], loads[7]):
        load.wait()
    turned_re, turned_im = [], []
    parts = eight_forward([planes_in[a * LINE : a * LINE + LINE, :] for a in range(8)])
    for k1, (re, im) in enumerate(parts):
        turn_re, turn_im = turns[k1 : k1 + 1, :], turns[8 + k1 : 9 + k1, :]
        turned_re.append(re * turn_re + im * turn_im)
        turned_im.append(im * turn_re - re * turn_im)
    turned = jnp.concatenate([jnp.concatenate(turned_re, 0), jnp.concatenate(turned_im, 0)], 1)
    ordered[...] = times(turned, const, FORWARD, 256)
    spectrum = jnp.concatenate([ordered[every(line, LINE), :] for line in range(2 * V)], 0)
    number = lax.broadcasted_iota(jnp.int32, (8, LANES), 0) + 8 * (lax.broadcasted_iota(jnp.int32, (8, LANES), 1) % 64)
    weight = jnp.where(number == 0, 1.0, 2.0) / NP
    sign = jnp.where(lax.broadcasted_iota(jnp.int32, (80, LANES), 1) < 64, -1.0, 1.0)
    crossed = (pltpu.roll(spectrum, 64, 1) * sign).reshape(2, V, 8, LANES)
    spectrum = spectrum.reshape(2, V, 8, LANES)
    for q in range(2):
        factor = jnp.where(number < cutoffs[q], weight, 0.0)
        for i in range(V):
            total = None
            for j in range(V):
                row = (q * 25 + i * V + j) * 16
                term = spectra[row : row + 8, :] * spectrum[q, j] + spectra[row + 8 : row + 16, :] * crossed[q, j]
                total = term if total is None else total + term
            ordered[every(q * V + i, LINE), :] = total * factor
    corrected = ordered[...]
    back_re = times(corrected, const, BACK_RE, 128)
    back_im = times(corrected, const, BACK_IM, 128)
    lines_re, lines_im = [], []
    for k1 in range(8):
        turn_re, turn_im = turns[k1 : k1 + 1, :], turns[8 + k1 : 9 + k1, :]
        re, im = back_re[k1 * LINE : k1 * LINE + LINE], back_im[k1 * LINE : k1 * LINE + LINE]
        lines_re.append(re * turn_re - im * turn_im)
        lines_im.append(im * turn_re + re * turn_im)
    for a, value in enumerate(eight_back(lines_re, lines_im)):
        corr_out[a * LINE : a * LINE + LINE, :] = value
    for d in FAR_FIRST:
        to = lax.rem(pitch + d, PITCH)
        send(
            corr_out.at[rows(to * LINE, SENT)], corr_in.at[rows(pitch * LINE, SENT)],
            back_s, back_r, at_pitch(d),
        )
    corr_in[rows(pitch * LINE, LINE), :] = corr_out[rows(pitch * LINE, LINE), :]

    place = lax.broadcasted_iota(jnp.int32, (8, LANES), 0)

    def tiles(ref, n, which):
        start = n * MAPS + which
        return [ref[start + V * j : start + V * j + 8, :] for j in range(V)]

    def spread_rows(vector):
        return [jnp.broadcast_to(vector[..., j : j + 1, :], vector.shape) for j in range(V)]

    def mix(matrix, parts):
        total = matrix[0] * parts[0]
        for j in range(1, V):
            total = total + matrix[j] * parts[j]
        return total

    finish(gm_r, (GROUP - 1) * USED)
    forward = jnp.stack(tiles(maps_in, 0, A))
    across = [jnp.stack(tiles(maps_in, 0, C))]
    for n in range(1, GROUP):
        parts = spread_rows(forward)
        forward = mix(tiles(maps_in, n, A), parts)
        across.append(mix(tiles(maps_in, n, C), parts))
    backward = jnp.concatenate([jnp.stack(tiles(maps_in, GROUP - 1, B)), across[GROUP - 1]], 0)
    for n in range(GROUP - 2, -1, -1):
        backward = mix(tiles(maps_in, n, B), spread_rows(backward))
        backward = jnp.concatenate([backward[:V], backward[V:] + across[n]], 0)
    columns = jnp.concatenate([forward, backward], 0)
    for n in range(3 * V):
        start = A + V * n if n < V else V * n - 25
        packed[start : start + 8, :] = columns[n]
    layer_maps[rows(layer * MAPS, MAPS), :] = packed[...]
    pl.semaphore_wait(ready, len(near))
    for t in range(LAYERS):
        single = to_layer(
            layer_maps.at[rows(layer * MAPS + A, SINGLE)], layer_maps.at[rows(layer * MAPS + A, SINGLE)], zm_s, zm_r, t,
        )
        pl.when(layer != t)(single.start)
        pair = to_layer(
            layer_maps.at[rows(layer * MAPS, PAIR)], layer_maps.at[rows(layer * MAPS, PAIR)], zt_s, zt_r, t,
        )
        pl.when(layer > t)(pair.start)

    finish(side_r, 16)
    own = prior[...]
    below, above = [], []
    for i in range(V):
        low_tiles, high_tiles = [], []
        for a in range(GROUP):
            n = i * GROUP + a
            tile = prior[i, a * 8 : a * 8 + 8, :]
            edge = pltpu.roll(lower[...], LANES - n, 1) if n else lower[...]
            low_tiles.append(jnp.where(column == 0, edge, pltpu.roll(tile, 1, 1)))
            edge = pltpu.roll(upper[...], LANES - 1 - n, 1)
            high_tiles.append(jnp.where(column == LANES - 1, edge, pltpu.roll(tile, LANES - 1, 1)))
        below.append(jnp.concatenate(low_tiles, 0))
        above.append(jnp.concatenate(high_tiles, 0))
    zero_row = jnp.zeros((8, LANES), jnp.float32)
    for i in range(V):
        total = residual[i]
        before = after = None
        for j in range(V):
            total = total - coupling[i, 2, j] * below[j] - coupling[i, 3, j] * above[j]
            low_term = coupling[i, 4, j] * own[j]
            high_term = coupling[i, 5, j] * own[j]
            before = low_term if before is None else before + low_term
            after = high_term if after is None else after + high_term
        total = total - jnp.concatenate([zero_row, before[:24]], 0) - jnp.concatenate([after[8:], zero_row], 0)
        source[i] = total

    def sweep(offsets, parity):
        star = None
        for s in range(4):
            block = inverse[:, :, every(s, 4), :]
            rhs = source[:, every(s, 4), :]
            value = block[:, 0] * rhs[0][None]
            for j in range(1, V):
                value = value + block[:, j] * rhs[j][None]
            star = value if s == 0 else value + apply(down[s], star)
            base[s] = star
        update = star
        for s in (2, 1, 0):
            update = base[s] + apply(up[s], update)
            base[s] = update
        ahead = pltpu.roll(star, 7, 1) + apply(next_reach, star)
        behind = update + apply(third[0], pltpu.roll(update, 7, 1) + apply(next_both, star))
        for i in range(V):
            offsets[every(i, VECS), :] = ahead[i]
            offsets[every(V + i, VECS), :] = behind[i]
        for d in MEMBERS:
            to = lax.rem(member + d, GROUP)
            copy = pltpu.make_async_remote_copy(
                src_ref=offsets.at[rows(cell(to) * 2 * VECS, SENT)], dst_ref=vecs_in.at[rows(member * VECS, SENT)],
                send_sem=gv_s, recv_sem=gv_r,
                device_id=at_member(d), device_id_type=pl.DeviceIdType.MESH,
            )
            pl.when(lax.rem(to, 2) == parity)(copy.start)

    sweep(vecs_early, 0)

    finish(back_r, (PITCH - 1) * SENT)
    for j in range(V):
        source[j, 0:8, :] = source[j, 0:8, :] + corr_in[every(j, LINE), :]
        source[j, 24:32, :] = source[j, 24:32, :] + corr_in[every(V + j, LINE), :]
    sweep(vecs_out, 1)
    vecs_in[rows(member * VECS, VECS), :] = vecs_out[rows(cell(member) * 2 * VECS, VECS), :]

    def chain(count, maps_ref, vecs_ref, x, y):
        entering_x, entering_y, crossing = [], [None] * count, []
        for n in range(count):
            entering_x.append(x)
            offset = vecs_ref[n * VECS : n * VECS + 8, :]
            if x is None:
                crossing.append(vecs_ref[n * VECS + V : n * VECS + V + 8, :])
                x = offset
            else:
                parts = spread_rows(x)
                ahead = mix(tiles(maps_ref, n, A), parts)
                crossing.append(mix(tiles(maps_ref, n, C), parts) + vecs_ref[n * VECS + V : n * VECS + V + 8, :])
                x = ahead + offset
        for n in range(count - 1, -1, -1):
            entering_y[n] = y
            y = crossing[n] if y is None else mix(tiles(maps_ref, n, B), spread_rows(y)) + crossing[n]
        return entering_x, entering_y, x, y

    finish(gv_r, (GROUP - 1) * SENT)
    _, _, x, y = chain(GROUP, maps_in, vecs_in, None, None)
    tail = pltpu.roll(y, V, 0)
    layer_vecs[rows(layer * VECS, 8), :] = jnp.where(place < V, x, tail)
    layer_vecs[rows(layer * VECS + 8, 8), :] = tail
    for t in range(LAYERS):
        pl.when(layer != t)(to_layer(
            layer_vecs.at[rows(layer * VECS, SENT)], layer_vecs.at[rows(layer * VECS, SENT)], zv_s, zv_r, t,
        ).start)
    finish(zm_r, (LAYERS - 1) * SINGLE)
    for t in range(LAYERS - 1):
        pl.when(layer == t)(functools.partial(finish, zt_r, (LAYERS - 1 - t) * PAIR))
    finish(zv_r, (LAYERS - 1) * SENT)
    entering_x, entering_y, _, _ = chain(LAYERS, layer_maps, layer_vecs, None, None)
    x = jnp.zeros((8, LANES), jnp.float32)
    y = jnp.zeros((8, LANES), jnp.float32)
    for n in range(8):
        if entering_x[n] is not None:
            x = jnp.where(layer == n, entering_x[n], x)
        if entering_y[n] is not None:
            y = jnp.where(layer == n, entering_y[n], y)
    entering_x, entering_y, _, _ = chain(GROUP, maps_in, vecs_in, x, y)
    for n in range(GROUP):
        tail = pltpu.roll(entering_y[n], V, 0)
        entry_out[n * VECS : n * VECS + 8, :] = jnp.where(place < V, entering_x[n], tail)
        entry_out[n * VECS + 8 : n * VECS + 16, :] = tail
    for d in MEMBERS:
        to = lax.rem(member + d, GROUP)
        send(
            entry_out.at[rows(to * VECS, SENT)], entry_in.at[rows(cell(member) * 2 * VECS, SENT)],
            ge_s, ge_r, at_member(d),
        )
    entry_in[rows(cell(member) * 2 * VECS, VECS), :] = entry_out[rows(member * VECS, VECS), :]
    finish(ge_r, (GROUP - 1) * SENT)
    x = jnp.stack([entry_in[every(i, VECS), :] for i in range(V)])
    y = jnp.stack([entry_in[every(V + i, VECS), :] for i in range(V)])
    odd = place % 2 == 1
    x = jnp.where(odd, pltpu.roll(apply(first[3], x) + base[3], 1, 1), x)
    y = jnp.where(odd, pltpu.roll(y, 1, 1), y)
    y = jnp.where(odd, y, pltpu.roll(apply(third[0], y) + apply(second[0], x) + base[0], 7, 1))
    for s in range(4):
        value = base[s]
        for j in range(V):
            value = value + second[s, j] * x[j][None] + third[s, j] * y[j][None]
        for i in range(V):
            out[i, every(s, 4), :] = value[i]

    finish(pitch_s, (PITCH - 1) * SENT)
    finish(side_s, 16)
    finish(gm_s, (GROUP - 1) * USED)
    finish(back_s, (PITCH - 1) * SENT)
    finish(gv_s, (GROUP - 1) * SENT)
    finish(zv_s, (LAYERS - 1) * SENT)
    finish(ge_s, (GROUP - 1) * SENT)
    finish(zm_s, (LAYERS - 1) * SINGLE)
    for t in range(1, LAYERS):
        pl.when(layer == t)(functools.partial(finish, zt_s, t * PAIR))


def body(residual, inverse_diagonal, prior_increment, coupling, characteristic, cutoffs):
    f32 = jnp.float32
    fields = (V, 32, LANES)
    matrices = pltpu.VMEM((4, V, V, 8, LANES), f32)

    def vmem(count):
        return pltpu.VMEM((count, LANES), f32)

    scratch = [
        pltpu.VMEM(fields, f32), pltpu.VMEM((V, V, 32, LANES), f32), pltpu.VMEM(fields, f32),
        pltpu.SMEM((V, 6, V), f32), pltpu.SMEM((2,), jnp.int32),
        pltpu.VMEM((50, 2, 512), f32), pltpu.VMEM((2 * LOW, LANES), jnp.bfloat16), vmem(16),
        pltpu.SemaphoreType.DMA((8,)),
        vmem(8), vmem(8), vmem(8), vmem(8),
        vmem(128), vmem(128), vmem(128), vmem(128), vmem(128),
        vmem(8 * MAPS), vmem(GROUP * MAPS), vmem(MAPS), vmem(LAYERS * MAPS),
        vmem(8 * VECS), vmem(8 * VECS), vmem(GROUP * VECS), vmem(LAYERS * VECS), vmem(GROUP * VECS), vmem(8 * VECS),
        matrices, matrices, matrices, matrices, matrices,
        pltpu.VMEM((V, V, 8, LANES), f32), pltpu.VMEM((V, V, 8, LANES), f32),
        pltpu.VMEM(fields, f32), pltpu.VMEM((4, V, 8, LANES), f32),
        pltpu.VMEM((104, 512), f32), vmem(104 * 8),
        *[pltpu.SemaphoreType.DMA] * 18,
        pltpu.SemaphoreType.REGULAR,
    ]
    inside = pl.BlockSpec(memory_space=pltpu.VMEM)
    outside = pl.BlockSpec(memory_space=pl.ANY)
    high_low, turns = table()
    result = pl.pallas_call(
        kernel,
        out_shape=pltpu.VMEM(fields, f32),
        in_specs=[outside] * 8,
        out_specs=inside,
        scratch_shapes=scratch,
        compiler_params=pltpu.CompilerParams(collective_id=0, has_side_effects=True),
    )(
        residual.reshape(fields),
        inverse_diagonal.reshape(V, V, 32, LANES),
        prior_increment.reshape(fields),
        coupling.transpose(1, 0, 2),
        characteristic.transpose(0, 3, 4, 1, 2).reshape(50, 2, 512),
        cutoffs,
        jnp.asarray(high_low),
        jnp.asarray(turns),
    )
    return result.reshape(V, GROUP, 8, LANES)


def solution(mesh):
    field = P(None, None, "span", "pitch")
    return jax.shard_map(
        body, mesh=mesh,
        in_specs=(field, P(None, None, None, "span", "pitch"), field, P(), P(), P()),
        out_specs=field, check_vma=False,
    )
```

```python
import functools

import jax
import jax.numpy as jnp
import numpy as np
from jax import lax
from jax.experimental import pallas as pl
from jax.experimental.pallas import tpu as pltpu
from jax.sharding import PartitionSpec as P

NP = 1024
PITCH = 8
GROUP = 4
LAYERS = 8
V = 5
LINE = 16
MAPS = 88
B, C, A = 0, 25, 56
PAIR, SINGLE, USED = 50, 25, 81
VECS = 16
SENT = 10
LANES = 128

FORWARD, BACK_RE, BACK_IM, ROWS = 0, 768, 1152, 1536
HALF = float(np.sqrt(0.5))


def table():
    two_pi = 2.0 * np.pi
    a = np.arange(8)
    b = np.arange(128)
    k2 = np.arange(64)
    twiddle = two_pi * np.outer(a, b) / NP
    lanes = two_pi * (np.outer(b, k2) % 128) / 128
    cos, sin = np.cos(lanes), np.sin(lanes)
    forward = np.block([[cos, -sin], [sin, cos]])
    back_re = np.concatenate([cos.T, -sin.T], 0)
    back_im = np.concatenate([sin.T, cos.T], 0)
    parts = [forward, back_re, back_im]
    pieces = []
    for part in parts:
        whole = part.astype(np.float32)
        high = whole.astype(jnp.bfloat16)
        pieces += [high, high, (whole - high.astype(np.float32)).astype(jnp.bfloat16)]
    turns = np.concatenate([np.cos(twiddle), np.sin(twiddle)], 0).astype(np.float32)
    return np.concatenate(pieces, 0), turns


FAR_FIRST = (4, 3, 5, 2, 6, 1, 7)
MEMBERS = (2, 1, 3)


def every(start, stride):
    return pl.ds(start, 8, stride=stride)


def rows(start, size):
    return pl.ds(pl.multiple_of(start, 8), size)


def product(later, earlier):
    total = later[0][None] * earlier[:, 0][:, None]
    for j in range(1, V):
        total = total + later[j][None] * earlier[:, j][:, None]
    return total


def apply(matrix, vector):
    total = matrix[0] * vector[0][None]
    for j in range(1, V):
        total = total + matrix[j] * vector[j][None]
    return total


def scaled(block, coupling, which):
    columns = []
    for k in range(V):
        total = block[:, 0] * (-coupling[0, which, k])
        for j in range(1, V):
            total = total + block[:, j] * (-coupling[j, which, k])
        columns.append(total)
    return jnp.stack(columns)


def times(data, const, start, size):
    data_high = data.astype(jnp.bfloat16)
    data_low = (data - data_high.astype(jnp.float32)).astype(jnp.bfloat16)
    thrice = jnp.concatenate([data_high, data_low, data_high], 1)
    return jnp.dot(thrice, const[start : start + 3 * size, :], preferred_element_type=jnp.float32)


def eight_forward(x):
    s0, d0, s2, d2 = x[0] + x[4], x[0] - x[4], x[2] + x[6], x[2] - x[6]
    s1, d1, s3, d3 = x[1] + x[5], x[1] - x[5], x[3] + x[7], x[3] - x[7]
    even, odd = s0 + s2, s1 + s3
    real, imag = s0 - s2, s3 - s1
    near, far = HALF * (d1 - d3), HALF * (d1 + d3)
    zero = jnp.zeros_like(even)
    first = (d0 + near, -(d2 + far))
    third = (d0 - near, d2 - far)
    return [
        (even + odd, zero), first, (real, imag), third,
        (even - odd, zero), (third[0], -third[1]), (real, -imag), (first[0], -first[1]),
    ]


def eight_back(re, im):
    p1, p2, p3 = re[1] + re[7], re[2] + re[6], re[3] + re[5]
    q1, q2, q3 = im[1] - im[7], im[2] - im[6], im[3] - im[5]
    total, gap = re[0] + re[4], re[0] - re[4]
    both, part = p1 + p3, HALF * (p1 - p3)
    cross, lean = q1 - q3, HALF * (q1 + q3)
    return [
        total + p2 + both, gap - q2 + part - lean, total - p2 - cross, gap + q2 - part - lean,
        total + p2 - both, gap - q2 - part + lean, total - p2 + cross, gap + q2 + part + lean,
    ]


def kernel(
    residual_in, inverse_in, prior_in, coupling_in, characteristic_in, cutoffs_in, const_in, turns_in, out,
    residual, inverse, prior, coupling, cutoffs, characteristic, const, turns, load_s,
    lower, upper, edge_low, edge_high, planes_out, planes_in, ordered, corr_out, corr_in,
    maps_out, maps_in, packed, layer_maps, vecs_early, vecs_out, vecs_in, layer_vecs, entry_out, entry_in,
    down, up, first, second, third, next_reach, next_both, source, base, flat, spectra,
    sent, pitch_r, back_r, side_r,
    gm_r, zm_r, gv_r, zv_r, ge_r, zt_s, zt_r, ready,
):
    pitch = lax.axis_index("pitch")
    span = lax.axis_index("span")
    layer = span // GROUP
    member = span % GROUP

    def cell(m):
        return (1 - m // 2) * (1 - m) + m // 2 * m

    def at_pitch(d):
        return {"pitch": lax.rem(pitch + d, PITCH), "span": span}

    def at_member(d):
        return {"pitch": pitch, "span": layer * GROUP + lax.rem(member + d, GROUP)}

    def at_layer(d):
        return {"pitch": pitch, "span": lax.rem(layer + d, LAYERS) * GROUP + member}

    peers = [at_pitch(d) for d in range(1, PITCH)]
    peers += [at_member(d) for d in range(1, GROUP)]
    near = [at_layer(d) for d in (1, 2, LAYERS - 2, LAYERS - 1)]
    peers += near
    loads = [pltpu.make_async_copy(residual_in, residual, load_s.at[0])]
    loads[0].start()
    barrier = pltpu.get_barrier_semaphore()
    for peer in peers:
        pl.semaphore_signal(barrier, inc=1, device_id=peer, device_id_type=pl.DeviceIdType.MESH)

    for n, (src, dst) in enumerate((
        (prior_in, prior), (inverse_in, inverse),
        (characteristic_in, characteristic), (const_in, const), (turns_in, turns),
        (coupling_in, coupling), (cutoffs_in, cutoffs),
    )):
        loads.append(pltpu.make_async_copy(src, dst, load_s.at[n + 1]))
        loads[-1].start()

    def send(src, dst, send_sem, recv_sem, peer):
        copy = pltpu.make_async_remote_copy(
            src_ref=src, dst_ref=dst, send_sem=send_sem, recv_sem=recv_sem,
            device_id=peer, device_id_type=pl.DeviceIdType.MESH,
        )
        copy.start()

    def to_layer(src, dst, send_sem, recv_sem, t):
        return pltpu.make_async_remote_copy(
            src_ref=src, dst_ref=dst, send_sem=send_sem, recv_sem=recv_sem,
            device_id={"pitch": pitch, "span": t * GROUP + member}, device_id_type=pl.DeviceIdType.MESH,
        )

    def finish(sem, count):
        area = maps_out.at[pl.ds(0, count)]
        pltpu.make_async_copy(area, area, sem).wait()

    loads[0].wait()
    for q, axial in enumerate((0, GROUP - 1)):
        for j in range(V):
            planes_out[every(q * V + j, LINE), :] = residual[j, axial * 8 : axial * 8 + 8, :]

    loads[2].wait()
    loads[6].wait()
    reach = None
    for s in range(4):
        block = inverse[:, :, every(s, 4), :]
        down[s] = scaled(block, coupling, 0)
        up[s] = scaled(block, coupling, 1)
        reach = down[s] if s == 0 else product(down[s], reach)
        first[s] = reach

    pl.semaphore_wait(barrier, len(peers))

    for d in FAR_FIRST:
        to = lax.rem(pitch + d, PITCH)
        send(
            planes_out.at[rows(to * LINE, SENT)], planes_in.at[rows(pitch * LINE, SENT)],
            sent, pitch_r, at_pitch(d),
        )
    reach = first[3]
    both = reach
    trail = up[3]
    second[3] = both
    third[3] = trail
    for s in (2, 1, 0):
        both = first[s] + product(up[s], both)
        trail = product(up[s], trail)
        second[s] = both
        third[s] = trail
    upper_reach = pltpu.roll(reach, 7, 2)
    upper_both = pltpu.roll(both, 7, 2)
    next_reach[...] = upper_reach
    next_both[...] = upper_both
    both = both + product(trail, product(upper_both, reach))
    trail = product(trail, pltpu.roll(trail, 7, 2))
    reach = product(upper_reach, reach)
    for k in range(V):
        for i in range(V):
            maps_out[every(A + V * k + i, MAPS), :] = reach[k, i]
            maps_out[every(B + V * k + i, MAPS), :] = trail[k, i]
            maps_out[every(C + V * k + i, MAPS), :] = both[k, i]
    for d in MEMBERS:
        to = lax.rem(member + d, GROUP)
        send(
            maps_out.at[rows(cell(to) * 2 * MAPS, USED)], maps_in.at[rows(member * MAPS, USED)],
            sent, gm_r, at_member(d),
        )
    for peer in near:
        pl.semaphore_signal(ready, inc=1, device_id=peer, device_id_type=pl.DeviceIdType.MESH)
    loads[1].wait()
    column = lax.broadcasted_iota(jnp.int32, (8, LANES), 1)
    last = initial = jnp.zeros((8, LANES), jnp.float32)
    for n in range(V * GROUP):
        tile = prior[n // GROUP, n % GROUP * 8 : n % GROUP * 8 + 8, :]
        last = jnp.where(column == n, pltpu.roll(tile, n + 1, 1), last)
        initial = jnp.where(column == n, pltpu.roll(tile, n, 1) if n else tile, initial)
    edge_high[...] = last
    edge_low[...] = initial
    send(edge_high, lower, sent, side_r, at_pitch(1))
    send(edge_low, upper, sent, side_r, at_pitch(PITCH - 1))

    planes_in[rows(pitch * LINE, LINE), :] = planes_out[rows(pitch * LINE, LINE), :]
    maps_in[rows(member * MAPS, MAPS), :] = maps_out[rows(cell(member) * 2 * MAPS, MAPS), :]

    loads[3].wait()
    flat[100:104, :] = jnp.zeros((4, 512), jnp.float32)
    for n in range(50):
        flat[2 * n : 2 * n + 2, :] = characteristic[n]
    whole = flat[...]
    high = whole.astype(jnp.bfloat16)
    rest = whole - high.astype(jnp.float32)
    middle = rest.astype(jnp.bfloat16)
    low = (rest - middle.astype(jnp.float32)).astype(jnp.bfloat16)
    harmonic = lax.broadcasted_iota(jnp.int32, (512, LANES), 0)
    lane = lax.broadcasted_iota(jnp.int32, (512, LANES), 1)
    apart = harmonic - 8 * (lane % 64)
    for k1 in range(8):
        pick = jnp.where(apart == k1, 1.0, 0.0).astype(jnp.bfloat16)
        part = jnp.dot(high, pick, preferred_element_type=jnp.float32)
        part = part + jnp.dot(middle, pick, preferred_element_type=jnp.float32)
        part = part + jnp.dot(low, pick, preferred_element_type=jnp.float32)
        spectra[pl.ds(k1, 104, stride=8), :] = part

    finish(pitch_r, (PITCH - 1) * SENT)
    for load in (loads[4], loads[5], loads[7]):
        load.wait()
    turned_re, turned_im = [], []
    parts = eight_forward([planes_in[a * LINE : a * LINE + LINE, :] for a in range(8)])
    for k1, (re, im) in enumerate(parts):
        turn_re, turn_im = turns[k1 : k1 + 1, :], turns[8 + k1 : 9 + k1, :]
        turned_re.append(re * turn_re + im * turn_im)
        turned_im.append(im * turn_re - re * turn_im)
    turned = jnp.concatenate([jnp.concatenate(turned_re, 0), jnp.concatenate(turned_im, 0)], 1)
    ordered[...] = times(turned, const, FORWARD, 256)
    spectrum = jnp.concatenate([ordered[every(line, LINE), :] for line in range(2 * V)], 0)
    number = lax.broadcasted_iota(jnp.int32, (8, LANES), 0) + 8 * (lax.broadcasted_iota(jnp.int32, (8, LANES), 1) % 64)
    weight = jnp.where(number == 0, 1.0, 2.0) / NP
    sign = jnp.where(lax.broadcasted_iota(jnp.int32, (80, LANES), 1) < 64, -1.0, 1.0)
    crossed = (pltpu.roll(spectrum, 64, 1) * sign).reshape(2, V, 8, LANES)
    spectrum = spectrum.reshape(2, V, 8, LANES)
    for q in range(2):
        factor = jnp.where(number < cutoffs[q], weight, 0.0)
        for i in range(V):
            total = None
            for j in range(V):
                row = (q * 25 + i * V + j) * 16
                term = spectra[row : row + 8, :] * spectrum[q, j] + spectra[row + 8 : row + 16, :] * crossed[q, j]
                total = term if total is None else total + term
            ordered[every(q * V + i, LINE), :] = total * factor
    corrected = ordered[...]
    back_re = times(corrected, const, BACK_RE, 128)
    back_im = times(corrected, const, BACK_IM, 128)
    lines_re, lines_im = [], []
    for k1 in range(8):
        turn_re, turn_im = turns[k1 : k1 + 1, :], turns[8 + k1 : 9 + k1, :]
        re, im = back_re[k1 * LINE : k1 * LINE + LINE], back_im[k1 * LINE : k1 * LINE + LINE]
        lines_re.append(re * turn_re - im * turn_im)
        lines_im.append(im * turn_re + re * turn_im)
    for a, value in enumerate(eight_back(lines_re, lines_im)):
        corr_out[a * LINE : a * LINE + LINE, :] = value
    for d in FAR_FIRST:
        to = lax.rem(pitch + d, PITCH)
        send(
            corr_out.at[rows(to * LINE, SENT)], corr_in.at[rows(pitch * LINE, SENT)],
            sent, back_r, at_pitch(d),
        )
    corr_in[rows(pitch * LINE, LINE), :] = corr_out[rows(pitch * LINE, LINE), :]

    place = lax.broadcasted_iota(jnp.int32, (8, LANES), 0)

    def tiles(ref, n, which):
        start = n * MAPS + which
        return [ref[start + V * j : start + V * j + 8, :] for j in range(V)]

    def spread_rows(vector):
        return [jnp.broadcast_to(vector[..., j : j + 1, :], vector.shape) for j in range(V)]

    def mix(matrix, parts):
        total = matrix[0] * parts[0]
        for j in range(1, V):
            total = total + matrix[j] * parts[j]
        return total

    finish(gm_r, (GROUP - 1) * USED)
    forward = jnp.stack(tiles(maps_in, 0, A))
    across = [jnp.stack(tiles(maps_in, 0, C))]
    for n in range(1, GROUP):
        parts = spread_rows(forward)
        forward = mix(tiles(maps_in, n, A), parts)
        across.append(mix(tiles(maps_in, n, C), parts))
    backward = jnp.concatenate([jnp.stack(tiles(maps_in, GROUP - 1, B)), across[GROUP - 1]], 0)
    for n in range(GROUP - 2, -1, -1):
        backward = mix(tiles(maps_in, n, B), spread_rows(backward))
        backward = jnp.concatenate([backward[:V], backward[V:] + across[n]], 0)
    columns = jnp.concatenate([forward, backward], 0)
    for n in range(3 * V):
        start = A + V * n if n < V else V * n - 25
        packed[start : start + 8, :] = columns[n]
    layer_maps[rows(layer * MAPS, MAPS), :] = packed[...]
    pl.semaphore_wait(ready, len(near))
    for t in range(LAYERS):
        single = to_layer(
            layer_maps.at[rows(layer * MAPS + A, SINGLE)], layer_maps.at[rows(layer * MAPS + A, SINGLE)], sent, zm_r, t,
        )
        pl.when(layer != t)(single.start)
        pair = to_layer(
            layer_maps.at[rows(layer * MAPS, PAIR)], layer_maps.at[rows(layer * MAPS, PAIR)], zt_s, zt_r, t,
        )
        pl.when(layer > t)(pair.start)

    finish(side_r, 16)
    own = prior[...]
    below, above = [], []
    for i in range(V):
        low_tiles, high_tiles = [], []
        for a in range(GROUP):
            n = i * GROUP + a
            tile = prior[i, a * 8 : a * 8 + 8, :]
            edge = pltpu.roll(lower[...], LANES - n, 1) if n else lower[...]
            low_tiles.append(jnp.where(column == 0, edge, pltpu.roll(tile, 1, 1)))
            edge = pltpu.roll(upper[...], LANES - 1 - n, 1)
            high_tiles.append(jnp.where(column == LANES - 1, edge, pltpu.roll(tile, LANES - 1, 1)))
        below.append(jnp.concatenate(low_tiles, 0))
        above.append(jnp.concatenate(high_tiles, 0))
    zero_row = jnp.zeros((8, LANES), jnp.float32)
    for i in range(V):
        total = residual[i]
        before = after = None
        for j in range(V):
            total = total - coupling[i, 2, j] * below[j] - coupling[i, 3, j] * above[j]
            low_term = coupling[i, 4, j] * own[j]
            high_term = coupling[i, 5, j] * own[j]
            before = low_term if before is None else before + low_term
            after = high_term if after is None else after + high_term
        total = total - jnp.concatenate([zero_row, before[:24]], 0) - jnp.concatenate([after[8:], zero_row], 0)
        source[i] = total

    def sweep(offsets, parity):
        star = None
        for s in range(4):
            block = inverse[:, :, every(s, 4), :]
            rhs = source[:, every(s, 4), :]
            value = block[:, 0] * rhs[0][None]
            for j in range(1, V):
                value = value + block[:, j] * rhs[j][None]
            star = value if s == 0 else value + apply(down[s], star)
            base[s] = star
        update = star
        for s in (2, 1, 0):
            update = base[s] + apply(up[s], update)
            base[s] = update
        ahead = pltpu.roll(star, 7, 1) + apply(next_reach, star)
        behind = update + apply(third[0], pltpu.roll(update, 7, 1) + apply(next_both, star))
        for i in range(V):
            offsets[every(i, VECS), :] = ahead[i]
            offsets[every(V + i, VECS), :] = behind[i]
        for d in MEMBERS:
            to = lax.rem(member + d, GROUP)
            copy = pltpu.make_async_remote_copy(
                src_ref=offsets.at[rows(cell(to) * 2 * VECS, SENT)], dst_ref=vecs_in.at[rows(member * VECS, SENT)],
                send_sem=sent, recv_sem=gv_r,
                device_id=at_member(d), device_id_type=pl.DeviceIdType.MESH,
            )
            pl.when(lax.rem(to, 2) == parity)(copy.start)

    sweep(vecs_early, 0)

    finish(back_r, (PITCH - 1) * SENT)
    for j in range(V):
        source[j, 0:8, :] = source[j, 0:8, :] + corr_in[every(j, LINE), :]
        source[j, 24:32, :] = source[j, 24:32, :] + corr_in[every(V + j, LINE), :]
    sweep(vecs_out, 1)
    vecs_in[rows(member * VECS, VECS), :] = vecs_out[rows(cell(member) * 2 * VECS, VECS), :]

    def chain(count, maps_ref, vecs_ref, x, y):
        entering_x, entering_y, crossing = [], [None] * count, []
        for n in range(count):
            entering_x.append(x)
            offset = vecs_ref[n * VECS : n * VECS + 8, :]
            if x is None:
                crossing.append(vecs_ref[n * VECS + V : n * VECS + V + 8, :])
                x = offset
            else:
                parts = spread_rows(x)
                ahead = mix(tiles(maps_ref, n, A), parts)
                crossing.append(mix(tiles(maps_ref, n, C), parts) + vecs_ref[n * VECS + V : n * VECS + V + 8, :])
                x = ahead + offset
        for n in range(count - 1, -1, -1):
            entering_y[n] = y
            y = crossing[n] if y is None else mix(tiles(maps_ref, n, B), spread_rows(y)) + crossing[n]
        return entering_x, entering_y, x, y

    finish(gv_r, (GROUP - 1) * SENT)
    _, _, x, y = chain(GROUP, maps_in, vecs_in, None, None)
    tail = pltpu.roll(y, V, 0)
    layer_vecs[rows(layer * VECS, 8), :] = jnp.where(place < V, x, tail)
    layer_vecs[rows(layer * VECS + 8, 8), :] = tail
    for t in range(LAYERS):
        pl.when(layer != t)(to_layer(
            layer_vecs.at[rows(layer * VECS, SENT)], layer_vecs.at[rows(layer * VECS, SENT)], sent, zv_r, t,
        ).start)
    finish(zm_r, (LAYERS - 1) * SINGLE)
    for t in range(LAYERS - 1):
        pl.when(layer == t)(functools.partial(finish, zt_r, (LAYERS - 1 - t) * PAIR))
    finish(zv_r, (LAYERS - 1) * SENT)
    entering_x, entering_y, _, _ = chain(LAYERS, layer_maps, layer_vecs, None, None)
    x = jnp.zeros((8, LANES), jnp.float32)
    y = jnp.zeros((8, LANES), jnp.float32)
    for n in range(8):
        if entering_x[n] is not None:
            x = jnp.where(layer == n, entering_x[n], x)
        if entering_y[n] is not None:
            y = jnp.where(layer == n, entering_y[n], y)
    entering_x, entering_y, _, _ = chain(GROUP, maps_in, vecs_in, x, y)
    for n in range(GROUP):
        tail = pltpu.roll(entering_y[n], V, 0)
        entry_out[n * VECS : n * VECS + 8, :] = jnp.where(place < V, entering_x[n], tail)
        entry_out[n * VECS + 8 : n * VECS + 16, :] = tail
    for d in MEMBERS:
        to = lax.rem(member + d, GROUP)
        send(
            entry_out.at[rows(to * VECS, SENT)], entry_in.at[rows(cell(member) * 2 * VECS, SENT)],
            sent, ge_r, at_member(d),
        )
    entry_in[rows(cell(member) * 2 * VECS, VECS), :] = entry_out[rows(member * VECS, VECS), :]
    finish(ge_r, (GROUP - 1) * SENT)
    x = jnp.stack([entry_in[every(i, VECS), :] for i in range(V)])
    y = jnp.stack([entry_in[every(V + i, VECS), :] for i in range(V)])
    odd = place % 2 == 1
    x = jnp.where(odd, pltpu.roll(apply(first[3], x) + base[3], 1, 1), x)
    y = jnp.where(odd, pltpu.roll(y, 1, 1), y)
    y = jnp.where(odd, y, pltpu.roll(apply(third[0], y) + apply(second[0], x) + base[0], 7, 1))
    for s in range(4):
        value = base[s]
        for j in range(V):
            value = value + second[s, j] * x[j][None] + third[s, j] * y[j][None]
        for i in range(V):
            out[i, every(s, 4), :] = value[i]

    total = 16 + (2 * PITCH - 2) * SENT + (GROUP - 1) * (USED + 2 * SENT) + (LAYERS - 1) * (SINGLE + SENT)
    finish(sent, total)
    for t in range(1, LAYERS):
        pl.when(layer == t)(functools.partial(finish, zt_s, t * PAIR))


def body(residual, inverse_diagonal, prior_increment, coupling, characteristic, cutoffs):
    f32 = jnp.float32
    fields = (V, 32, LANES)
    matrices = pltpu.VMEM((4, V, V, 8, LANES), f32)

    def vmem(count):
        return pltpu.VMEM((count, LANES), f32)

    scratch = [
        pltpu.VMEM(fields, f32), pltpu.VMEM((V, V, 32, LANES), f32), pltpu.VMEM(fields, f32),
        pltpu.SMEM((V, 6, V), f32), pltpu.SMEM((2,), jnp.int32),
        pltpu.VMEM((50, 2, 512), f32), pltpu.VMEM((ROWS, LANES), jnp.bfloat16), vmem(16),
        pltpu.SemaphoreType.DMA((8,)),
        vmem(8), vmem(8), vmem(8), vmem(8),
        vmem(128), vmem(128), vmem(128), vmem(128), vmem(128),
        vmem(8 * MAPS), vmem(GROUP * MAPS), vmem(MAPS), vmem(LAYERS * MAPS),
        vmem(8 * VECS), vmem(8 * VECS), vmem(GROUP * VECS), vmem(LAYERS * VECS), vmem(GROUP * VECS), vmem(8 * VECS),
        matrices, matrices, matrices, matrices, matrices,
        pltpu.VMEM((V, V, 8, LANES), f32), pltpu.VMEM((V, V, 8, LANES), f32),
        pltpu.VMEM(fields, f32), pltpu.VMEM((4, V, 8, LANES), f32),
        pltpu.VMEM((104, 512), f32), vmem(104 * 8),
        *[pltpu.SemaphoreType.DMA] * 11,
        pltpu.SemaphoreType.REGULAR,
    ]
    inside = pl.BlockSpec(memory_space=pltpu.VMEM)
    outside = pl.BlockSpec(memory_space=pl.ANY)
    high_low, turns = table()
    result = pl.pallas_call(
        kernel,
        out_shape=pltpu.VMEM(fields, f32),
        in_specs=[outside] * 8,
        out_specs=inside,
        scratch_shapes=scratch,
        compiler_params=pltpu.CompilerParams(collective_id=0, has_side_effects=True),
    )(
        residual.reshape(fields),
        inverse_diagonal.reshape(V, V, 32, LANES),
        prior_increment.reshape(fields),
        coupling.transpose(1, 0, 2),
        characteristic.transpose(0, 3, 4, 1, 2).reshape(50, 2, 512),
        cutoffs,
        jnp.asarray(high_low),
        jnp.asarray(turns),
    )
    return result.reshape(V, GROUP, 8, LANES)


def solution(mesh):
    field = P(None, None, "span", "pitch")
    return jax.shard_map(
        body, mesh=mesh,
        in_specs=(field, P(None, None, None, "span", "pitch"), field, P(), P(), P()),
        out_specs=field, check_vma=False,
    )
```

```python
import functools

import jax
import jax.numpy as jnp
import numpy as np
from jax import lax
from jax.experimental import pallas as pl
from jax.experimental.pallas import tpu as pltpu
from jax.sharding import PartitionSpec as P

NP = 1024
PITCH = 8
GROUP = 4
LAYERS = 8
V = 5
LINE = 16
MAPS = 88
B, C, A = 0, 25, 56
PAIR, SINGLE, USED = 50, 25, 81
VECS = 16
SENT = 10
LANES = 128

FORWARD, BACK_RE, BACK_IM, LOW = 0, 256, 384, 512
HALF = float(np.sqrt(0.5))


def table():
    two_pi = 2.0 * np.pi
    a = np.arange(8)
    b = np.arange(128)
    k2 = np.arange(64)
    twiddle = two_pi * np.outer(a, b) / NP
    lanes = two_pi * (np.outer(b, k2) % 128) / 128
    cos, sin = np.cos(lanes), np.sin(lanes)
    forward = np.block([[cos, -sin], [sin, cos]])
    back_re = np.concatenate([cos.T, -sin.T], 0)
    back_im = np.concatenate([sin.T, cos.T], 0)
    parts = [forward, back_re, back_im]
    whole = np.concatenate(parts, 0).astype(np.float32)
    high = whole.astype(jnp.bfloat16)
    low = (whole - high.astype(np.float32)).astype(jnp.bfloat16)
    turns = np.concatenate([np.cos(twiddle), np.sin(twiddle)], 0).astype(np.float32)
    return np.concatenate([high, low], 0), turns


FAR_FIRST = (4, 3, 5, 2, 6, 1, 7)
MEMBERS = (2, 1, 3)


def every(start, stride):
    return pl.ds(start, 8, stride=stride)


def rows(start, size):
    return pl.ds(pl.multiple_of(start, 8), size)


def product(later, earlier):
    total = later[0][None] * earlier[:, 0][:, None]
    for j in range(1, V):
        total = total + later[j][None] * earlier[:, j][:, None]
    return total


def apply(matrix, vector):
    total = matrix[0] * vector[0][None]
    for j in range(1, V):
        total = total + matrix[j] * vector[j][None]
    return total


def scaled(block, coupling, which):
    columns = []
    for k in range(V):
        total = block[:, 0] * (-coupling[0, which, k])
        for j in range(1, V):
            total = total + block[:, j] * (-coupling[j, which, k])
        columns.append(total)
    return jnp.stack(columns)


def times(data, const, start, size):
    data_high = data.astype(jnp.bfloat16)
    data_low = (data - data_high.astype(jnp.float32)).astype(jnp.bfloat16)
    high = const[start : start + size, :]
    low = const[LOW + start : LOW + start + size, :]
    total = jnp.dot(data_high, high, preferred_element_type=jnp.float32)
    total = total + jnp.dot(data_low, high, preferred_element_type=jnp.float32)
    return total + jnp.dot(data_high, low, preferred_element_type=jnp.float32)


def eight_forward(x):
    s0, d0, s2, d2 = x[0] + x[4], x[0] - x[4], x[2] + x[6], x[2] - x[6]
    s1, d1, s3, d3 = x[1] + x[5], x[1] - x[5], x[3] + x[7], x[3] - x[7]
    even, odd = s0 + s2, s1 + s3
    real, imag = s0 - s2, s3 - s1
    near, far = HALF * (d1 - d3), HALF * (d1 + d3)
    zero = jnp.zeros_like(even)
    first = (d0 + near, -(d2 + far))
    third = (d0 - near, d2 - far)
    return [
        (even + odd, zero), first, (real, imag), third,
        (even - odd, zero), (third[0], -third[1]), (real, -imag), (first[0], -first[1]),
    ]


def eight_back(re, im):
    p1, p2, p3 = re[1] + re[7], re[2] + re[6], re[3] + re[5]
    q1, q2, q3 = im[1] - im[7], im[2] - im[6], im[3] - im[5]
    total, gap = re[0] + re[4], re[0] - re[4]
    both, part = p1 + p3, HALF * (p1 - p3)
    cross, lean = q1 - q3, HALF * (q1 + q3)
    return [
        total + p2 + both, gap - q2 + part - lean, total - p2 - cross, gap + q2 - part - lean,
        total + p2 - both, gap - q2 - part + lean, total - p2 + cross, gap + q2 + part + lean,
    ]


def kernel(
    residual_in, inverse_in, prior_in, coupling_in, characteristic_in, cutoffs_in, const_in, turns_in, out,
    residual, inverse, prior, coupling, cutoffs, characteristic, const, turns, load_s,
    lower, upper, edge_low, edge_high, planes_out, planes_in, ordered, corr_out, corr_in,
    maps_out, maps_in, packed, layer_maps, vecs_early, vecs_out, vecs_in, layer_vecs, entry_out, entry_in,
    down, up, first, second, third, next_reach, next_both, source, base, flat, spectra,
    pitch_s, pitch_r, back_s, back_r, side_s, side_r,
    gm_s, gm_r, zm_s, zm_r, gv_s, gv_r, zv_s, zv_r, ge_s, ge_r, zt_s, zt_r, ready,
):
    pitch = lax.axis_index("pitch")
    span = lax.axis_index("span")
    layer = span // GROUP
    member = span % GROUP

    def cell(m):
        return (1 - m // 2) * (1 - m) + m // 2 * m

    def at_pitch(d):
        return {"pitch": lax.rem(pitch + d, PITCH), "span": span}

    def at_member(d):
        return {"pitch": pitch, "span": layer * GROUP + lax.rem(member + d, GROUP)}

    def at_layer(d):
        return {"pitch": pitch, "span": lax.rem(layer + d, LAYERS) * GROUP + member}

    peers = [at_pitch(d) for d in range(1, PITCH)]
    peers += [at_member(d) for d in range(1, GROUP)]
    near = [at_layer(d) for d in (1, 2, LAYERS - 2, LAYERS - 1)]
    peers += near
    loads = [pltpu.make_async_copy(residual_in, residual, load_s.at[0])]
    loads[0].start()
    barrier = pltpu.get_barrier_semaphore()
    for peer in peers:
        pl.semaphore_signal(barrier, inc=1, device_id=peer, device_id_type=pl.DeviceIdType.MESH)

    for n, (src, dst) in enumerate((
        (prior_in, prior), (inverse_in, inverse),
        (characteristic_in, characteristic), (const_in, const), (turns_in, turns),
        (coupling_in, coupling), (cutoffs_in, cutoffs),
    )):
        loads.append(pltpu.make_async_copy(src, dst, load_s.at[n + 1]))
        loads[-1].start()

    def send(src, dst, send_sem, recv_sem, peer):
        copy = pltpu.make_async_remote_copy(
            src_ref=src, dst_ref=dst, send_sem=send_sem, recv_sem=recv_sem,
            device_id=peer, device_id_type=pl.DeviceIdType.MESH,
        )
        copy.start()

    def to_layer(src, dst, send_sem, recv_sem, t):
        return pltpu.make_async_remote_copy(
            src_ref=src, dst_ref=dst, send_sem=send_sem, recv_sem=recv_sem,
            device_id={"pitch": pitch, "span": t * GROUP + member}, device_id_type=pl.DeviceIdType.MESH,
        )

    def finish(sem, count):
        area = maps_out.at[pl.ds(0, count)]
        pltpu.make_async_copy(area, area, sem).wait()

    loads[0].wait()
    for q, axial in enumerate((0, GROUP - 1)):
        for j in range(V):
            planes_out[every(q * V + j, LINE), :] = residual[j, axial * 8 : axial * 8 + 8, :]

    loads[2].wait()
    loads[6].wait()
    reach = None
    for s in range(2):
        block = inverse[:, :, every(s, 4), :]
        down[s] = scaled(block, coupling, 0)
        up[s] = scaled(block, coupling, 1)
        reach = down[s] if s == 0 else product(down[s], reach)
        first[s] = reach

    pl.semaphore_wait(barrier, len(peers))

    for d in FAR_FIRST:
        to = lax.rem(pitch + d, PITCH)
        send(
            planes_out.at[rows(to * LINE, SENT)], planes_in.at[rows(pitch * LINE, SENT)],
            pitch_s, pitch_r, at_pitch(d),
        )
    reach = first[1]
    for s in (2, 3):
        block = inverse[:, :, every(s, 4), :]
        down[s] = scaled(block, coupling, 0)
        up[s] = scaled(block, coupling, 1)
        reach = product(down[s], reach)
        first[s] = reach
    both = reach
    trail = up[3]
    second[3] = both
    third[3] = trail
    for s in (2, 1, 0):
        both = first[s] + product(up[s], both)
        trail = product(up[s], trail)
        second[s] = both
        third[s] = trail
    upper_reach = pltpu.roll(reach, 7, 2)
    upper_both = pltpu.roll(both, 7, 2)
    next_reach[...] = upper_reach
    next_both[...] = upper_both
    both = both + product(trail, product(upper_both, reach))
    trail = product(trail, pltpu.roll(trail, 7, 2))
    reach = product(upper_reach, reach)
    for k in range(V):
        for i in range(V):
            maps_out[every(A + V * k + i, MAPS), :] = reach[k, i]
            maps_out[every(B + V * k + i, MAPS), :] = trail[k, i]
            maps_out[every(C + V * k + i, MAPS), :] = both[k, i]
    for d in MEMBERS:
        to = lax.rem(member + d, GROUP)
        send(
            maps_out.at[rows(cell(to) * 2 * MAPS, USED)], maps_in.at[rows(member * MAPS, USED)],
            gm_s, gm_r, at_member(d),
        )
    for peer in near:
        pl.semaphore_signal(ready, inc=1, device_id=peer, device_id_type=pl.DeviceIdType.MESH)
    loads[1].wait()
    column = lax.broadcasted_iota(jnp.int32, (8, LANES), 1)
    last = initial = jnp.zeros((8, LANES), jnp.float32)
    for n in range(V * GROUP):
        tile = prior[n // GROUP, n % GROUP * 8 : n % GROUP * 8 + 8, :]
        last = jnp.where(column == n, pltpu.roll(tile, n + 1, 1), last)
        initial = jnp.where(column == n, pltpu.roll(tile, n, 1) if n else tile, initial)
    edge_high[...] = last
    edge_low[...] = initial
    send(edge_high, lower, side_s, side_r, at_pitch(1))
    send(edge_low, upper, side_s, side_r, at_pitch(PITCH - 1))

    planes_in[rows(pitch * LINE, LINE), :] = planes_out[rows(pitch * LINE, LINE), :]
    maps_in[rows(member * MAPS, MAPS), :] = maps_out[rows(cell(member) * 2 * MAPS, MAPS), :]

    loads[3].wait()
    flat[100:104, :] = jnp.zeros((4, 512), jnp.float32)
    for n in range(50):
        flat[2 * n : 2 * n + 2, :] = characteristic[n]
    whole = flat[...]
    high = whole.astype(jnp.bfloat16)
    rest = whole - high.astype(jnp.float32)
    middle = rest.astype(jnp.bfloat16)
    low = (rest - middle.astype(jnp.float32)).astype(jnp.bfloat16)
    harmonic = lax.broadcasted_iota(jnp.int32, (512, LANES), 0)
    lane = lax.broadcasted_iota(jnp.int32, (512, LANES), 1)
    apart = harmonic - 8 * (lane % 64)
    for k1 in range(8):
        pick = jnp.where(apart == k1, 1.0, 0.0).astype(jnp.bfloat16)
        part = jnp.dot(high, pick, preferred_element_type=jnp.float32)
        part = part + jnp.dot(middle, pick, preferred_element_type=jnp.float32)
        part = part + jnp.dot(low, pick, preferred_element_type=jnp.float32)
        spectra[pl.ds(k1, 104, stride=8), :] = part

    finish(pitch_r, (PITCH - 1) * SENT)
    for load in (loads[4], loads[5], loads[7]):
        load.wait()
    turned_re, turned_im = [], []
    parts = eight_forward([planes_in[a * LINE : a * LINE + LINE, :] for a in range(8)])
    for k1, (re, im) in enumerate(parts):
        turn_re, turn_im = turns[k1 : k1 + 1, :], turns[8 + k1 : 9 + k1, :]
        turned_re.append(re * turn_re + im * turn_im)
        turned_im.append(im * turn_re - re * turn_im)
    turned = jnp.concatenate([jnp.concatenate(turned_re, 0), jnp.concatenate(turned_im, 0)], 1)
    ordered[...] = times(turned, const, FORWARD, 256)
    spectrum = jnp.concatenate([ordered[every(line, LINE), :] for line in range(2 * V)], 0)
    number = lax.broadcasted_iota(jnp.int32, (8, LANES), 0) + 8 * (lax.broadcasted_iota(jnp.int32, (8, LANES), 1) % 64)
    weight = jnp.where(number == 0, 1.0, 2.0) / NP
    sign = jnp.where(lax.broadcasted_iota(jnp.int32, (80, LANES), 1) < 64, -1.0, 1.0)
    crossed = (pltpu.roll(spectrum, 64, 1) * sign).reshape(2, V, 8, LANES)
    spectrum = spectrum.reshape(2, V, 8, LANES)
    for q in range(2):
        factor = jnp.where(number < cutoffs[q], weight, 0.0)
        for i in range(V):
            total = None
            for j in range(V):
                row = (q * 25 + i * V + j) * 16
                term = spectra[row : row + 8, :] * spectrum[q, j] + spectra[row + 8 : row + 16, :] * crossed[q, j]
                total = term if total is None else total + term
            ordered[every(q * V + i, LINE), :] = total * factor
    corrected = ordered[...]
    back_re = times(corrected, const, BACK_RE, 128)
    back_im = times(corrected, const, BACK_IM, 128)
    lines_re, lines_im = [], []
    for k1 in range(8):
        turn_re, turn_im = turns[k1 : k1 + 1, :], turns[8 + k1 : 9 + k1, :]
        re, im = back_re[k1 * LINE : k1 * LINE + LINE], back_im[k1 * LINE : k1 * LINE + LINE]
        lines_re.append(re * turn_re - im * turn_im)
        lines_im.append(im * turn_re + re * turn_im)
    for a, value in enumerate(eight_back(lines_re, lines_im)):
        corr_out[a * LINE : a * LINE + LINE, :] = value
    for d in FAR_FIRST:
        to = lax.rem(pitch + d, PITCH)
        send(
            corr_out.at[rows(to * LINE, SENT)], corr_in.at[rows(pitch * LINE, SENT)],
            back_s, back_r, at_pitch(d),
        )
    corr_in[rows(pitch * LINE, LINE), :] = corr_out[rows(pitch * LINE, LINE), :]

    place = lax.broadcasted_iota(jnp.int32, (8, LANES), 0)

    def tiles(ref, n, which):
        start = n * MAPS + which
        return [ref[start + V * j : start + V * j + 8, :] for j in range(V)]

    def spread_rows(vector):
        return [jnp.broadcast_to(vector[..., j : j + 1, :], vector.shape) for j in range(V)]

    def mix(matrix, parts):
        total = matrix[0] * parts[0]
        for j in range(1, V):
            total = total + matrix[j] * parts[j]
        return total

    finish(gm_r, (GROUP - 1) * USED)
    forward = jnp.stack(tiles(maps_in, 0, A))
    across = [jnp.stack(tiles(maps_in, 0, C))]
    for n in range(1, GROUP):
        parts = spread_rows(forward)
        forward = mix(tiles(maps_in, n, A), parts)
        across.append(mix(tiles(maps_in, n, C), parts))
    backward = jnp.concatenate([jnp.stack(tiles(maps_in, GROUP - 1, B)), across[GROUP - 1]], 0)
    for n in range(GROUP - 2, -1, -1):
        backward = mix(tiles(maps_in, n, B), spread_rows(backward))
        backward = jnp.concatenate([backward[:V], backward[V:] + across[n]], 0)
    columns = jnp.concatenate([forward, backward], 0)
    for n in range(3 * V):
        start = A + V * n if n < V else V * n - 25
        packed[start : start + 8, :] = columns[n]
    layer_maps[rows(layer * MAPS, MAPS), :] = packed[...]
    pl.semaphore_wait(ready, len(near))
    for t in range(LAYERS):
        single = to_layer(
            layer_maps.at[rows(layer * MAPS + A, SINGLE)], layer_maps.at[rows(layer * MAPS + A, SINGLE)], zm_s, zm_r, t,
        )
        pl.when(layer != t)(single.start)
        pair = to_layer(
            layer_maps.at[rows(layer * MAPS, PAIR)], layer_maps.at[rows(layer * MAPS, PAIR)], zt_s, zt_r, t,
        )
        pl.when(layer > t)(pair.start)

    finish(side_r, 16)
    own = prior[...]
    below, above = [], []
    for i in range(V):
        low_tiles, high_tiles = [], []
        for a in range(GROUP):
            n = i * GROUP + a
            tile = prior[i, a * 8 : a * 8 + 8, :]
            edge = pltpu.roll(lower[...], LANES - n, 1) if n else lower[...]
            low_tiles.append(jnp.where(column == 0, edge, pltpu.roll(tile, 1, 1)))
            edge = pltpu.roll(upper[...], LANES - 1 - n, 1)
            high_tiles.append(jnp.where(column == LANES - 1, edge, pltpu.roll(tile, LANES - 1, 1)))
        below.append(jnp.concatenate(low_tiles, 0))
        above.append(jnp.concatenate(high_tiles, 0))
    zero_row = jnp.zeros((8, LANES), jnp.float32)
    for i in range(V):
        total = residual[i]
        before = after = None
        for j in range(V):
            total = total - coupling[i, 2, j] * below[j] - coupling[i, 3, j] * above[j]
            low_term = coupling[i, 4, j] * own[j]
            high_term = coupling[i, 5, j] * own[j]
            before = low_term if before is None else before + low_term
            after = high_term if after is None else after + high_term
        total = total - jnp.concatenate([zero_row, before[:24]], 0) - jnp.concatenate([after[8:], zero_row], 0)
        source[i] = total

    def sweep(offsets, parity):
        star = None
        for s in range(4):
            block = inverse[:, :, every(s, 4), :]
            rhs = source[:, every(s, 4), :]
            value = block[:, 0] * rhs[0][None]
            for j in range(1, V):
                value = value + block[:, j] * rhs[j][None]
            star = value if s == 0 else value + apply(down[s], star)
            base[s] = star
        update = star
        for s in (2, 1, 0):
            update = base[s] + apply(up[s], update)
            base[s] = update
        ahead = pltpu.roll(star, 7, 1) + apply(next_reach, star)
        behind = update + apply(third[0], pltpu.roll(update, 7, 1) + apply(next_both, star))
        for i in range(V):
            offsets[every(i, VECS), :] = ahead[i]
            offsets[every(V + i, VECS), :] = behind[i]
        for d in MEMBERS:
            to = lax.rem(member + d, GROUP)
            copy = pltpu.make_async_remote_copy(
                src_ref=offsets.at[rows(cell(to) * 2 * VECS, SENT)], dst_ref=vecs_in.at[rows(member * VECS, SENT)],
                send_sem=gv_s, recv_sem=gv_r,
                device_id=at_member(d), device_id_type=pl.DeviceIdType.MESH,
            )
            pl.when(lax.rem(to, 2) == parity)(copy.start)

    sweep(vecs_early, 0)

    finish(back_r, (PITCH - 1) * SENT)
    for j in range(V):
        source[j, 0:8, :] = source[j, 0:8, :] + corr_in[every(j, LINE), :]
        source[j, 24:32, :] = source[j, 24:32, :] + corr_in[every(V + j, LINE), :]
    sweep(vecs_out, 1)
    vecs_in[rows(member * VECS, VECS), :] = vecs_out[rows(cell(member) * 2 * VECS, VECS), :]

    def chain(count, maps_ref, vecs_ref, x, y):
        entering_x, entering_y, crossing = [], [None] * count, []
        for n in range(count):
            entering_x.append(x)
            offset = vecs_ref[n * VECS : n * VECS + 8, :]
            if x is None:
                crossing.append(vecs_ref[n * VECS + V : n * VECS + V + 8, :])
                x = offset
            else:
                parts = spread_rows(x)
                ahead = mix(tiles(maps_ref, n, A), parts)
                crossing.append(mix(tiles(maps_ref, n, C), parts) + vecs_ref[n * VECS + V : n * VECS + V + 8, :])
                x = ahead + offset
        for n in range(count - 1, -1, -1):
            entering_y[n] = y
            y = crossing[n] if y is None else mix(tiles(maps_ref, n, B), spread_rows(y)) + crossing[n]
        return entering_x, entering_y, x, y

    finish(gv_r, (GROUP - 1) * SENT)
    _, _, x, y = chain(GROUP, maps_in, vecs_in, None, None)
    tail = pltpu.roll(y, V, 0)
    layer_vecs[rows(layer * VECS, 8), :] = jnp.where(place < V, x, tail)
    layer_vecs[rows(layer * VECS + 8, 8), :] = tail
    for t in range(LAYERS):
        pl.when(layer != t)(to_layer(
            layer_vecs.at[rows(layer * VECS, SENT)], layer_vecs.at[rows(layer * VECS, SENT)], zv_s, zv_r, t,
        ).start)
    finish(zm_r, (LAYERS - 1) * SINGLE)
    for t in range(LAYERS - 1):
        pl.when(layer == t)(functools.partial(finish, zt_r, (LAYERS - 1 - t) * PAIR))
    finish(zv_r, (LAYERS - 1) * SENT)
    entering_x, entering_y, _, _ = chain(LAYERS, layer_maps, layer_vecs, None, None)
    x = jnp.zeros((8, LANES), jnp.float32)
    y = jnp.zeros((8, LANES), jnp.float32)
    for n in range(8):
        if entering_x[n] is not None:
            x = jnp.where(layer == n, entering_x[n], x)
        if entering_y[n] is not None:
            y = jnp.where(layer == n, entering_y[n], y)
    entering_x, entering_y, _, _ = chain(GROUP, maps_in, vecs_in, x, y)
    for n in range(GROUP):
        tail = pltpu.roll(entering_y[n], V, 0)
        entry_out[n * VECS : n * VECS + 8, :] = jnp.where(place < V, entering_x[n], tail)
        entry_out[n * VECS + 8 : n * VECS + 16, :] = tail
    for d in MEMBERS:
        to = lax.rem(member + d, GROUP)
        send(
            entry_out.at[rows(to * VECS, SENT)], entry_in.at[rows(cell(member) * 2 * VECS, SENT)],
            ge_s, ge_r, at_member(d),
        )
    entry_in[rows(cell(member) * 2 * VECS, VECS), :] = entry_out[rows(member * VECS, VECS), :]
    finish(ge_r, (GROUP - 1) * SENT)
    x = jnp.stack([entry_in[every(i, VECS), :] for i in range(V)])
    y = jnp.stack([entry_in[every(V + i, VECS), :] for i in range(V)])
    odd = place % 2 == 1
    x = jnp.where(odd, pltpu.roll(apply(first[3], x) + base[3], 1, 1), x)
    y = jnp.where(odd, pltpu.roll(y, 1, 1), y)
    y = jnp.where(odd, y, pltpu.roll(apply(third[0], y) + apply(second[0], x) + base[0], 7, 1))
    for s in range(4):
        value = base[s]
        for j in range(V):
            value = value + second[s, j] * x[j][None] + third[s, j] * y[j][None]
        for i in range(V):
            out[i, every(s, 4), :] = value[i]

    finish(pitch_s, (PITCH - 1) * SENT)
    finish(side_s, 16)
    finish(gm_s, (GROUP - 1) * USED)
    finish(back_s, (PITCH - 1) * SENT)
    finish(gv_s, (GROUP - 1) * SENT)
    finish(zv_s, (LAYERS - 1) * SENT)
    finish(ge_s, (GROUP - 1) * SENT)
    finish(zm_s, (LAYERS - 1) * SINGLE)
    for t in range(1, LAYERS):
        pl.when(layer == t)(functools.partial(finish, zt_s, t * PAIR))


def body(residual, inverse_diagonal, prior_increment, coupling, characteristic, cutoffs):
    f32 = jnp.float32
    fields = (V, 32, LANES)
    matrices = pltpu.VMEM((4, V, V, 8, LANES), f32)

    def vmem(count):
        return pltpu.VMEM((count, LANES), f32)

    scratch = [
        pltpu.VMEM(fields, f32), pltpu.VMEM((V, V, 32, LANES), f32), pltpu.VMEM(fields, f32),
        pltpu.SMEM((V, 6, V), f32), pltpu.SMEM((2,), jnp.int32),
        pltpu.VMEM((50, 2, 512), f32), pltpu.VMEM((2 * LOW, LANES), jnp.bfloat16), vmem(16),
        pltpu.SemaphoreType.DMA((8,)),
        vmem(8), vmem(8), vmem(8), vmem(8),
        vmem(128), vmem(128), vmem(128), vmem(128), vmem(128),
        vmem(8 * MAPS), vmem(GROUP * MAPS), vmem(MAPS), vmem(LAYERS * MAPS),
        vmem(8 * VECS), vmem(8 * VECS), vmem(GROUP * VECS), vmem(LAYERS * VECS), vmem(GROUP * VECS), vmem(8 * VECS),
        matrices, matrices, matrices, matrices, matrices,
        pltpu.VMEM((V, V, 8, LANES), f32), pltpu.VMEM((V, V, 8, LANES), f32),
        pltpu.VMEM(fields, f32), pltpu.VMEM((4, V, 8, LANES), f32),
        pltpu.VMEM((104, 512), f32), vmem(104 * 8),
        *[pltpu.SemaphoreType.DMA] * 18,
        pltpu.SemaphoreType.REGULAR,
    ]
    inside = pl.BlockSpec(memory_space=pltpu.VMEM)
    outside = pl.BlockSpec(memory_space=pl.ANY)
    high_low, turns = table()
    result = pl.pallas_call(
        kernel,
        out_shape=pltpu.VMEM(fields, f32),
        in_specs=[outside] * 8,
        out_specs=inside,
        scratch_shapes=scratch,
        compiler_params=pltpu.CompilerParams(collective_id=0, has_side_effects=True),
    )(
        residual.reshape(fields),
        inverse_diagonal.reshape(V, V, 32, LANES),
        prior_increment.reshape(fields),
        coupling.transpose(1, 0, 2),
        characteristic.transpose(0, 3, 4, 1, 2).reshape(50, 2, 512),
        cutoffs,
        jnp.asarray(high_low),
        jnp.asarray(turns),
    )
    return result.reshape(V, GROUP, 8, LANES)


def solution(mesh):
    field = P(None, None, "span", "pitch")
    return jax.shard_map(
        body, mesh=mesh,
        in_specs=(field, P(None, None, None, "span", "pitch"), field, P(), P(), P()),
        out_specs=field, check_vma=False,
    )
```

```python
import functools

import jax
import jax.numpy as jnp
import numpy as np
from jax import lax
from jax.experimental import pallas as pl
from jax.experimental.pallas import tpu as pltpu
from jax.sharding import PartitionSpec as P

NP = 1024
PITCH = 8
GROUP = 4
LAYERS = 8
V = 5
LINE = 16
MAPS = 88
B, C, A = 0, 25, 56
PAIR, SINGLE, USED = 50, 25, 81
VECS = 16
SENT = 10
LANES = 128

FORWARD, BACK_RE, BACK_IM, LOW = 0, 256, 384, 512
HALF = float(np.sqrt(0.5))


def table():
    two_pi = 2.0 * np.pi
    a = np.arange(8)
    b = np.arange(128)
    k2 = np.arange(64)
    twiddle = two_pi * np.outer(a, b) / NP
    lanes = two_pi * (np.outer(b, k2) % 128) / 128
    cos, sin = np.cos(lanes), np.sin(lanes)
    forward = np.block([[cos, -sin], [sin, cos]])
    back_re = np.concatenate([cos.T, -sin.T], 0)
    back_im = np.concatenate([sin.T, cos.T], 0)
    parts = [forward, back_re, back_im]
    whole = np.concatenate(parts, 0).astype(np.float32)
    high = whole.astype(jnp.bfloat16)
    low = (whole - high.astype(np.float32)).astype(jnp.bfloat16)
    turns = np.concatenate([np.cos(twiddle), np.sin(twiddle)], 0).astype(np.float32)
    return np.concatenate([high, low], 0), turns


FAR_FIRST = (4, 3, 5, 2, 6, 1, 7)
MEMBERS = (1, 3, 2)


def every(start, stride):
    return pl.ds(start, 8, stride=stride)


def rows(start, size):
    return pl.ds(pl.multiple_of(start, 8), size)


def product(later, earlier):
    total = later[0][None] * earlier[:, 0][:, None]
    for j in range(1, V):
        total = total + later[j][None] * earlier[:, j][:, None]
    return total


def apply(matrix, vector):
    total = matrix[0] * vector[0][None]
    for j in range(1, V):
        total = total + matrix[j] * vector[j][None]
    return total


def scaled(block, coupling, which):
    columns = []
    for k in range(V):
        total = block[:, 0] * (-coupling[0, which, k])
        for j in range(1, V):
            total = total + block[:, j] * (-coupling[j, which, k])
        columns.append(total)
    return jnp.stack(columns)


def times(data, const, start, size):
    data_high = data.astype(jnp.bfloat16)
    data_low = (data - data_high.astype(jnp.float32)).astype(jnp.bfloat16)
    high = const[start : start + size, :]
    low = const[LOW + start : LOW + start + size, :]
    total = jnp.dot(data_high, high, preferred_element_type=jnp.float32)
    total = total + jnp.dot(data_low, high, preferred_element_type=jnp.float32)
    return total + jnp.dot(data_high, low, preferred_element_type=jnp.float32)


def eight_forward(x):
    s0, d0, s2, d2 = x[0] + x[4], x[0] - x[4], x[2] + x[6], x[2] - x[6]
    s1, d1, s3, d3 = x[1] + x[5], x[1] - x[5], x[3] + x[7], x[3] - x[7]
    even, odd = s0 + s2, s1 + s3
    real, imag = s0 - s2, s3 - s1
    near, far = HALF * (d1 - d3), HALF * (d1 + d3)
    zero = jnp.zeros_like(even)
    first = (d0 + near, -(d2 + far))
    third = (d0 - near, d2 - far)
    return [
        (even + odd, zero), first, (real, imag), third,
        (even - odd, zero), (third[0], -third[1]), (real, -imag), (first[0], -first[1]),
    ]


def eight_back(re, im):
    p1, p2, p3 = re[1] + re[7], re[2] + re[6], re[3] + re[5]
    q1, q2, q3 = im[1] - im[7], im[2] - im[6], im[3] - im[5]
    total, gap = re[0] + re[4], re[0] - re[4]
    both, part = p1 + p3, HALF * (p1 - p3)
    cross, lean = q1 - q3, HALF * (q1 + q3)
    return [
        total + p2 + both, gap - q2 + part - lean, total - p2 - cross, gap + q2 - part - lean,
        total + p2 - both, gap - q2 - part + lean, total - p2 + cross, gap + q2 + part + lean,
    ]


def kernel(
    residual_in, inverse_in, prior_in, coupling_in, characteristic_in, cutoffs_in, const_in, turns_in, out,
    residual, inverse, prior, coupling, cutoffs, characteristic, const, turns, load_s,
    lower, upper, edge_low, edge_high, planes_out, planes_in, ordered, corr_out, corr_in,
    maps_out, maps_in, packed, layer_maps, vecs_early, vecs_out, vecs_in, layer_vecs, entry_out, entry_in,
    down, up, first, second, third, next_reach, next_both, source, base, flat, spectra,
    pitch_s, pitch_r, back_s, back_r, side_s, side_r,
    gm_s, gm_r, zm_s, zm_r, gv_s, gv_r, zv_s, zv_r, ge_s, ge_r, zt_s, zt_r, ready,
):
    pitch = lax.axis_index("pitch")
    span = lax.axis_index("span")
    layer = span // GROUP
    member = span % GROUP

    def cell(m):
        return (1 - m // 2) * (1 - m) + m // 2 * m

    def at_pitch(d):
        return {"pitch": lax.rem(pitch + d, PITCH), "span": span}

    def at_member(d):
        return {"pitch": pitch, "span": layer * GROUP + lax.rem(member + d, GROUP)}

    def at_layer(d):
        return {"pitch": pitch, "span": lax.rem(layer + d, LAYERS) * GROUP + member}

    peers = [at_pitch(d) for d in range(1, PITCH)]
    peers += [at_member(d) for d in range(1, GROUP)]
    near = [at_layer(d) for d in (1, 2, LAYERS - 2, LAYERS - 1)]
    peers += near
    loads = [pltpu.make_async_copy(residual_in, residual, load_s.at[0])]
    loads[0].start()
    barrier = pltpu.get_barrier_semaphore()
    for peer in peers:
        pl.semaphore_signal(barrier, inc=1, device_id=peer, device_id_type=pl.DeviceIdType.MESH)

    for n, (src, dst) in enumerate((
        (prior_in, prior), (inverse_in, inverse),
        (characteristic_in, characteristic), (const_in, const), (turns_in, turns),
        (coupling_in, coupling), (cutoffs_in, cutoffs),
    )):
        loads.append(pltpu.make_async_copy(src, dst, load_s.at[n + 1]))
        loads[-1].start()

    def send(src, dst, send_sem, recv_sem, peer):
        copy = pltpu.make_async_remote_copy(
            src_ref=src, dst_ref=dst, send_sem=send_sem, recv_sem=recv_sem,
            device_id=peer, device_id_type=pl.DeviceIdType.MESH,
        )
        copy.start()

    def to_layer(src, dst, send_sem, recv_sem, t):
        return pltpu.make_async_remote_copy(
            src_ref=src, dst_ref=dst, send_sem=send_sem, recv_sem=recv_sem,
            device_id={"pitch": pitch, "span": t * GROUP + member}, device_id_type=pl.DeviceIdType.MESH,
        )

    def finish(sem, count):
        area = maps_out.at[pl.ds(0, count)]
        pltpu.make_async_copy(area, area, sem).wait()

    loads[0].wait()
    for q, axial in enumerate((0, GROUP - 1)):
        for j in range(V):
            planes_out[every(q * V + j, LINE), :] = residual[j, axial * 8 : axial * 8 + 8, :]

    loads[2].wait()
    loads[6].wait()
    reach = None
    for s in range(4):
        block = inverse[:, :, every(s, 4), :]
        down[s] = scaled(block, coupling, 0)
        up[s] = scaled(block, coupling, 1)
        reach = down[s] if s == 0 else product(down[s], reach)
        first[s] = reach

    pl.semaphore_wait(barrier, len(peers))

    for d in FAR_FIRST:
        to = lax.rem(pitch + d, PITCH)
        send(
            planes_out.at[rows(to * LINE, SENT)], planes_in.at[rows(pitch * LINE, SENT)],
            pitch_s, pitch_r, at_pitch(d),
        )
    reach = first[3]
    both = reach
    trail = up[3]
    second[3] = both
    third[3] = trail
    for s in (2, 1, 0):
        both = first[s] + product(up[s], both)
        trail = product(up[s], trail)
        second[s] = both
        third[s] = trail
    upper_reach = pltpu.roll(reach, 7, 2)
    upper_both = pltpu.roll(both, 7, 2)
    next_reach[...] = upper_reach
    next_both[...] = upper_both
    both = both + product(trail, product(upper_both, reach))
    trail = product(trail, pltpu.roll(trail, 7, 2))
    reach = product(upper_reach, reach)
    for k in range(V):
        for i in range(V):
            maps_out[every(A + V * k + i, MAPS), :] = reach[k, i]
            maps_out[every(B + V * k + i, MAPS), :] = trail[k, i]
            maps_out[every(C + V * k + i, MAPS), :] = both[k, i]
    for d in MEMBERS:
        to = lax.rem(member + d, GROUP)
        send(
            maps_out.at[rows(cell(to) * 2 * MAPS, USED)], maps_in.at[rows(member * MAPS, USED)],
            gm_s, gm_r, at_member(d),
        )
    for peer in near:
        pl.semaphore_signal(ready, inc=1, device_id=peer, device_id_type=pl.DeviceIdType.MESH)
    loads[1].wait()
    column = lax.broadcasted_iota(jnp.int32, (8, LANES), 1)
    last = initial = jnp.zeros((8, LANES), jnp.float32)
    for n in range(V * GROUP):
        tile = prior[n // GROUP, n % GROUP * 8 : n % GROUP * 8 + 8, :]
        last = jnp.where(column == n, pltpu.roll(tile, n + 1, 1), last)
        initial = jnp.where(column == n, pltpu.roll(tile, n, 1) if n else tile, initial)
    edge_high[...] = last
    edge_low[...] = initial
    send(edge_high, lower, side_s, side_r, at_pitch(1))
    send(edge_low, upper, side_s, side_r, at_pitch(PITCH - 1))

    planes_in[rows(pitch * LINE, LINE), :] = planes_out[rows(pitch * LINE, LINE), :]
    maps_in[rows(member * MAPS, MAPS), :] = maps_out[rows(cell(member) * 2 * MAPS, MAPS), :]

    loads[3].wait()
    flat[100:104, :] = jnp.zeros((4, 512), jnp.float32)
    for n in range(50):
        flat[2 * n : 2 * n + 2, :] = characteristic[n]
    whole = flat[...]
    high = whole.astype(jnp.bfloat16)
    rest = whole - high.astype(jnp.float32)
    middle = rest.astype(jnp.bfloat16)
    low = (rest - middle.astype(jnp.float32)).astype(jnp.bfloat16)
    harmonic = lax.broadcasted_iota(jnp.int32, (512, LANES), 0)
    lane = lax.broadcasted_iota(jnp.int32, (512, LANES), 1)
    apart = harmonic - 8 * (lane % 64)
    for k1 in range(8):
        pick = jnp.where(apart == k1, 1.0, 0.0).astype(jnp.bfloat16)
        part = jnp.dot(high, pick, preferred_element_type=jnp.float32)
        part = part + jnp.dot(middle, pick, preferred_element_type=jnp.float32)
        part = part + jnp.dot(low, pick, preferred_element_type=jnp.float32)
        spectra[pl.ds(k1, 104, stride=8), :] = part

    finish(pitch_r, (PITCH - 1) * SENT)
    for load in (loads[4], loads[5], loads[7]):
        load.wait()
    turned_re, turned_im = [], []
    parts = eight_forward([planes_in[a * LINE : a * LINE + LINE, :] for a in range(8)])
    for k1, (re, im) in enumerate(parts):
        turn_re, turn_im = turns[k1 : k1 + 1, :], turns[8 + k1 : 9 + k1, :]
        turned_re.append(re * turn_re + im * turn_im)
        turned_im.append(im * turn_re - re * turn_im)
    turned = jnp.concatenate([jnp.concatenate(turned_re, 0), jnp.concatenate(turned_im, 0)], 1)
    ordered[...] = times(turned, const, FORWARD, 256)
    spectrum = jnp.concatenate([ordered[every(line, LINE), :] for line in range(2 * V)], 0)
    number = lax.broadcasted_iota(jnp.int32, (8, LANES), 0) + 8 * (lax.broadcasted_iota(jnp.int32, (8, LANES), 1) % 64)
    weight = jnp.where(number == 0, 1.0, 2.0) / NP
    sign = jnp.where(lax.broadcasted_iota(jnp.int32, (80, LANES), 1) < 64, -1.0, 1.0)
    crossed = (pltpu.roll(spectrum, 64, 1) * sign).reshape(2, V, 8, LANES)
    spectrum = spectrum.reshape(2, V, 8, LANES)
    for q in range(2):
        factor = jnp.where(number < cutoffs[q], weight, 0.0)
        for i in range(V):
            total = None
            for j in range(V):
                row = (q * 25 + i * V + j) * 16
                term = spectra[row : row + 8, :] * spectrum[q, j] + spectra[row + 8 : row + 16, :] * crossed[q, j]
                total = term if total is None else total + term
            ordered[every(q * V + i, LINE), :] = total * factor
    corrected = ordered[...]
    back_re = times(corrected, const, BACK_RE, 128)
    back_im = times(corrected, const, BACK_IM, 128)
    lines_re, lines_im = [], []
    for k1 in range(8):
        turn_re, turn_im = turns[k1 : k1 + 1, :], turns[8 + k1 : 9 + k1, :]
        re, im = back_re[k1 * LINE : k1 * LINE + LINE], back_im[k1 * LINE : k1 * LINE + LINE]
        lines_re.append(re * turn_re - im * turn_im)
        lines_im.append(im * turn_re + re * turn_im)
    for a, value in enumerate(eight_back(lines_re, lines_im)):
        corr_out[a * LINE : a * LINE + LINE, :] = value
    for d in FAR_FIRST:
        to = lax.rem(pitch + d, PITCH)
        send(
            corr_out.at[rows(to * LINE, SENT)], corr_in.at[rows(pitch * LINE, SENT)],
            back_s, back_r, at_pitch(d),
        )
    corr_in[rows(pitch * LINE, LINE), :] = corr_out[rows(pitch * LINE, LINE), :]

    place = lax.broadcasted_iota(jnp.int32, (8, LANES), 0)

    def tiles(ref, n, which):
        start = n * MAPS + which
        return [ref[start + V * j : start + V * j + 8, :] for j in range(V)]

    def spread_rows(vector):
        return [jnp.broadcast_to(vector[..., j : j + 1, :], vector.shape) for j in range(V)]

    def mix(matrix, parts):
        total = matrix[0] * parts[0]
        for j in range(1, V):
            total = total + matrix[j] * parts[j]
        return total

    finish(gm_r, (GROUP - 1) * USED)
    forward = jnp.stack(tiles(maps_in, 0, A))
    across = [jnp.stack(tiles(maps_in, 0, C))]
    for n in range(1, GROUP):
        parts = spread_rows(forward)
        forward = mix(tiles(maps_in, n, A), parts)
        across.append(mix(tiles(maps_in, n, C), parts))
    backward = jnp.concatenate([jnp.stack(tiles(maps_in, GROUP - 1, B)), across[GROUP - 1]], 0)
    for n in range(GROUP - 2, -1, -1):
        backward = mix(tiles(maps_in, n, B), spread_rows(backward))
        backward = jnp.concatenate([backward[:V], backward[V:] + across[n]], 0)
    columns = jnp.concatenate([forward, backward], 0)
    for n in range(3 * V):
        start = A + V * n if n < V else V * n - 25
        packed[start : start + 8, :] = columns[n]
    layer_maps[rows(layer * MAPS, MAPS), :] = packed[...]
    pl.semaphore_wait(ready, len(near))
    for t in range(LAYERS):
        single = to_layer(
            layer_maps.at[rows(layer * MAPS + A, SINGLE)], layer_maps.at[rows(layer * MAPS + A, SINGLE)], zm_s, zm_r, t,
        )
        pl.when(layer != t)(single.start)
        pair = to_layer(
            layer_maps.at[rows(layer * MAPS, PAIR)], layer_maps.at[rows(layer * MAPS, PAIR)], zt_s, zt_r, t,
        )
        pl.when(layer > t)(pair.start)

    finish(side_r, 16)
    own = prior[...]
    below, above = [], []
    for i in range(V):
        low_tiles, high_tiles = [], []
        for a in range(GROUP):
            n = i * GROUP + a
            tile = prior[i, a * 8 : a * 8 + 8, :]
            edge = pltpu.roll(lower[...], LANES - n, 1) if n else lower[...]
            low_tiles.append(jnp.where(column == 0, edge, pltpu.roll(tile, 1, 1)))
            edge = pltpu.roll(upper[...], LANES - 1 - n, 1)
            high_tiles.append(jnp.where(column == LANES - 1, edge, pltpu.roll(tile, LANES - 1, 1)))
        below.append(jnp.concatenate(low_tiles, 0))
        above.append(jnp.concatenate(high_tiles, 0))
    zero_row = jnp.zeros((8, LANES), jnp.float32)
    for i in range(V):
        total = residual[i]
        before = after = None
        for j in range(V):
            total = total - coupling[i, 2, j] * below[j] - coupling[i, 3, j] * above[j]
            low_term = coupling[i, 4, j] * own[j]
            high_term = coupling[i, 5, j] * own[j]
            before = low_term if before is None else before + low_term
            after = high_term if after is None else after + high_term
        total = total - jnp.concatenate([zero_row, before[:24]], 0) - jnp.concatenate([after[8:], zero_row], 0)
        source[i] = total

    def sweep(offsets, parity):
        star = None
        for s in range(4):
            block = inverse[:, :, every(s, 4), :]
            rhs = source[:, every(s, 4), :]
            value = block[:, 0] * rhs[0][None]
            for j in range(1, V):
                value = value + block[:, j] * rhs[j][None]
            star = value if s == 0 else value + apply(down[s], star)
            base[s] = star
        update = star
        for s in (2, 1, 0):
            update = base[s] + apply(up[s], update)
            base[s] = update
        ahead = pltpu.roll(star, 7, 1) + apply(next_reach, star)
        behind = update + apply(third[0], pltpu.roll(update, 7, 1) + apply(next_both, star))
        for i in range(V):
            offsets[every(i, VECS), :] = ahead[i]
            offsets[every(V + i, VECS), :] = behind[i]
        for d in MEMBERS:
            to = lax.rem(member + d, GROUP)
            copy = pltpu.make_async_remote_copy(
                src_ref=offsets.at[rows(cell(to) * 2 * VECS, SENT)], dst_ref=vecs_in.at[rows(member * VECS, SENT)],
                send_sem=gv_s, recv_sem=gv_r,
                device_id=at_member(d), device_id_type=pl.DeviceIdType.MESH,
            )
            pl.when(lax.rem(to, 2) == parity)(copy.start)

    sweep(vecs_early, 0)

    finish(back_r, (PITCH - 1) * SENT)
    for j in range(V):
        source[j, 0:8, :] = source[j, 0:8, :] + corr_in[every(j, LINE), :]
        source[j, 24:32, :] = source[j, 24:32, :] + corr_in[every(V + j, LINE), :]
    sweep(vecs_out, 1)
    vecs_in[rows(member * VECS, VECS), :] = vecs_out[rows(cell(member) * 2 * VECS, VECS), :]

    def chain(count, maps_ref, vecs_ref, x, y):
        entering_x, entering_y, crossing = [], [None] * count, []
        for n in range(count):
            entering_x.append(x)
            offset = vecs_ref[n * VECS : n * VECS + 8, :]
            if x is None:
                crossing.append(vecs_ref[n * VECS + V : n * VECS + V + 8, :])
                x = offset
            else:
                parts = spread_rows(x)
                ahead = mix(tiles(maps_ref, n, A), parts)
                crossing.append(mix(tiles(maps_ref, n, C), parts) + vecs_ref[n * VECS + V : n * VECS + V + 8, :])
                x = ahead + offset
        for n in range(count - 1, -1, -1):
            entering_y[n] = y
            y = crossing[n] if y is None else mix(tiles(maps_ref, n, B), spread_rows(y)) + crossing[n]
        return entering_x, entering_y, x, y

    finish(gv_r, (GROUP - 1) * SENT)
    _, _, x, y = chain(GROUP, maps_in, vecs_in, None, None)
    tail = pltpu.roll(y, V, 0)
    layer_vecs[rows(layer * VECS, 8), :] = jnp.where(place < V, x, tail)
    layer_vecs[rows(layer * VECS + 8, 8), :] = tail
    for t in range(LAYERS):
        pl.when(layer != t)(to_layer(
            layer_vecs.at[rows(layer * VECS, SENT)], layer_vecs.at[rows(layer * VECS, SENT)], zv_s, zv_r, t,
        ).start)
    finish(zm_r, (LAYERS - 1) * SINGLE)
    for t in range(LAYERS - 1):
        pl.when(layer == t)(functools.partial(finish, zt_r, (LAYERS - 1 - t) * PAIR))
    finish(zv_r, (LAYERS - 1) * SENT)
    entering_x, entering_y, _, _ = chain(LAYERS, layer_maps, layer_vecs, None, None)
    x = jnp.zeros((8, LANES), jnp.float32)
    y = jnp.zeros((8, LANES), jnp.float32)
    for n in range(8):
        if entering_x[n] is not None:
            x = jnp.where(layer == n, entering_x[n], x)
        if entering_y[n] is not None:
            y = jnp.where(layer == n, entering_y[n], y)
    entering_x, entering_y, _, _ = chain(GROUP, maps_in, vecs_in, x, y)
    for n in range(GROUP):
        tail = pltpu.roll(entering_y[n], V, 0)
        entry_out[n * VECS : n * VECS + 8, :] = jnp.where(place < V, entering_x[n], tail)
        entry_out[n * VECS + 8 : n * VECS + 16, :] = tail
    for d in MEMBERS:
        to = lax.rem(member + d, GROUP)
        send(
            entry_out.at[rows(to * VECS, SENT)], entry_in.at[rows(cell(member) * 2 * VECS, SENT)],
            ge_s, ge_r, at_member(d),
        )
    entry_in[rows(cell(member) * 2 * VECS, VECS), :] = entry_out[rows(member * VECS, VECS), :]
    finish(ge_r, (GROUP - 1) * SENT)
    x = jnp.stack([entry_in[every(i, VECS), :] for i in range(V)])
    y = jnp.stack([entry_in[every(V + i, VECS), :] for i in range(V)])
    odd = place % 2 == 1
    x = jnp.where(odd, pltpu.roll(apply(first[3], x) + base[3], 1, 1), x)
    y = jnp.where(odd, pltpu.roll(y, 1, 1), y)
    y = jnp.where(odd, y, pltpu.roll(apply(third[0], y) + apply(second[0], x) + base[0], 7, 1))
    for s in range(4):
        value = base[s]
        for j in range(V):
            value = value + second[s, j] * x[j][None] + third[s, j] * y[j][None]
        for i in range(V):
            out[i, every(s, 4), :] = value[i]

    finish(pitch_s, (PITCH - 1) * SENT)
    finish(side_s, 16)
    finish(gm_s, (GROUP - 1) * USED)
    finish(back_s, (PITCH - 1) * SENT)
    finish(gv_s, (GROUP - 1) * SENT)
    finish(zv_s, (LAYERS - 1) * SENT)
    finish(ge_s, (GROUP - 1) * SENT)
    finish(zm_s, (LAYERS - 1) * SINGLE)
    for t in range(1, LAYERS):
        pl.when(layer == t)(functools.partial(finish, zt_s, t * PAIR))


def body(residual, inverse_diagonal, prior_increment, coupling, characteristic, cutoffs):
    f32 = jnp.float32
    fields = (V, 32, LANES)
    matrices = pltpu.VMEM((4, V, V, 8, LANES), f32)

    def vmem(count):
        return pltpu.VMEM((count, LANES), f32)

    scratch = [
        pltpu.VMEM(fields, f32), pltpu.VMEM((V, V, 32, LANES), f32), pltpu.VMEM(fields, f32),
        pltpu.SMEM((V, 6, V), f32), pltpu.SMEM((2,), jnp.int32),
        pltpu.VMEM((50, 2, 512), f32), pltpu.VMEM((2 * LOW, LANES), jnp.bfloat16), vmem(16),
        pltpu.SemaphoreType.DMA((8,)),
        vmem(8), vmem(8), vmem(8), vmem(8),
        vmem(128), vmem(128), vmem(128), vmem(128), vmem(128),
        vmem(8 * MAPS), vmem(GROUP * MAPS), vmem(MAPS), vmem(LAYERS * MAPS),
        vmem(8 * VECS), vmem(8 * VECS), vmem(GROUP * VECS), vmem(LAYERS * VECS), vmem(GROUP * VECS), vmem(8 * VECS),
        matrices, matrices, matrices, matrices, matrices,
        pltpu.VMEM((V, V, 8, LANES), f32), pltpu.VMEM((V, V, 8, LANES), f32),
        pltpu.VMEM(fields, f32), pltpu.VMEM((4, V, 8, LANES), f32),
        pltpu.VMEM((104, 512), f32), vmem(104 * 8),
        *[pltpu.SemaphoreType.DMA] * 18,
        pltpu.SemaphoreType.REGULAR,
    ]
    inside = pl.BlockSpec(memory_space=pltpu.VMEM)
    outside = pl.BlockSpec(memory_space=pl.ANY)
    high_low, turns = table()
    result = pl.pallas_call(
        kernel,
        out_shape=pltpu.VMEM(fields, f32),
        in_specs=[outside] * 8,
        out_specs=inside,
        scratch_shapes=scratch,
        compiler_params=pltpu.CompilerParams(collective_id=0, has_side_effects=True),
    )(
        residual.reshape(fields),
        inverse_diagonal.reshape(V, V, 32, LANES),
        prior_increment.reshape(fields),
        coupling.transpose(1, 0, 2),
        characteristic.transpose(0, 3, 4, 1, 2).reshape(50, 2, 512),
        cutoffs,
        jnp.asarray(high_low),
        jnp.asarray(turns),
    )
    return result.reshape(V, GROUP, 8, LANES)


def solution(mesh):
    field = P(None, None, "span", "pitch")
    return jax.shard_map(
        body, mesh=mesh,
        in_specs=(field, P(None, None, None, "span", "pitch"), field, P(), P(), P()),
        out_specs=field, check_vma=False,
    )
```
